32 devices in a mesh: data: 1 (over z), seq: 32 (over y, x, core).
Axes of the slice: x: 4, y: 4, z: 1, core: 2. Of those that a mesh axis runs over, the one named last changes fastest.
The devices are a block of a 4x4x8 slice.
Arguments:
- tokens: bfloat16 [16, 4096, 768], P('data', 'seq')
- lengths: int32 [16], P('data')
- slot_params: bfloat16 [768, 128], replicated
- logit_scale: float32 [1], replicated
- w_in: bfloat16 [128, 768, 3072], P('seq')
- w_out: bfloat16 [128, 3072, 768], P('seq')
Outputs:
- output: bfloat16 [16, 4096, 768], P('data', 'seq')
All inputs are finite; a program needn't handle non-finite values.
Results may differ from the reference program's by a relative error of at most 0.0156646.
Values are sent between devices in bfloat16 or wider.
A program may use at most 768 MiB of HBM per device.

```python
import jax
import jax.numpy as jnp
from jax import lax

BATCH = 16
TOKENS = 4096
D_MODEL = 768
FF_DIM = 3072
EXPERTS = 128
SLOTS = 1
NUM_SLOTS = EXPERTS * SLOTS


def setup_inputs(seed: int = 0, part: int = 0) -> dict:
    base_key = jax.random.key(seed)
    k_phi, k_win, k_wout, k_gain = jax.random.split(base_key, 4)
    part_key = jax.random.fold_in(base_key, part)
    k_sel, k_noise, k_len = jax.random.split(part_key, 3)
    slot_params = jax.random.normal(k_phi, (D_MODEL, NUM_SLOTS), jnp.float32)
    chosen = jax.random.randint(k_sel, (BATCH, TOKENS), 0, NUM_SLOTS)
    noise = jax.random.normal(k_noise, (BATCH, TOKENS, D_MODEL), jnp.float32)
    tokens = jnp.take(slot_params.T, chosen, axis=0) + noise
    lengths = jax.random.randint(k_len, (BATCH,), 1, TOKENS + 1)
    logit_scale = jax.random.uniform(k_gain, (1,), jnp.float32, 6.0, 9.0)
    w_in = jax.random.normal(k_win, (EXPERTS, D_MODEL, FF_DIM), jnp.float32) * D_MODEL ** -0.5
    w_out = jax.random.normal(k_wout, (EXPERTS, FF_DIM, D_MODEL), jnp.float32) * FF_DIM ** -0.5
    return {
        "tokens": tokens.astype(jnp.bfloat16),
        "lengths": lengths.astype(jnp.int32),
        "slot_params": slot_params.astype(jnp.bfloat16),
        "logit_scale": logit_scale,
        "w_in": w_in.astype(jnp.bfloat16),
        "w_out": w_out.astype(jnp.bfloat16),
    }


def reference(tokens, lengths, slot_params, logit_scale, w_in, w_out):
    params_f32 = slot_params.astype(jnp.float32)
    col_inv = lax.rsqrt(jnp.sum(params_f32 * params_f32, axis=0, keepdims=True) + 1e-6)
    phi_norm = (params_f32 * (logit_scale[0] * col_inv)).astype(jnp.bfloat16)
    positions = jnp.arange(TOKENS)

    def row_logits(row_tokens):
        tok_f32 = row_tokens.astype(jnp.float32)
        tok_norm = (tok_f32 * lax.rsqrt(jnp.sum(tok_f32 * tok_f32, axis=-1, keepdims=True) + 1e-6)).astype(jnp.bfloat16)
        return jnp.dot(tok_norm, phi_norm, preferred_element_type=jnp.float32)

    def dispatch_row(row_args):
        row_tokens, row_len = row_args
        logits = row_logits(row_tokens)
        is_valid = (positions < row_len)[:, None]
        col_max = jnp.max(jnp.where(is_valid, logits, -jnp.inf), axis=0)
        disp_w = jnp.where(is_valid, jnp.exp(logits - col_max[None, :]), 0.0)
        col_sum = jnp.sum(disp_w, axis=0)
        slot_sum = jnp.dot(disp_w.astype(jnp.bfloat16).T, row_tokens, preferred_element_type=jnp.float32)
        return (slot_sum / col_sum[:, None]).astype(jnp.bfloat16)

    slot_in = lax.map(dispatch_row, (tokens, lengths))
    by_expert = slot_in.reshape(BATCH, EXPERTS, SLOTS, D_MODEL).transpose(1, 0, 2, 3).reshape(EXPERTS, BATCH * SLOTS, D_MODEL)

    def expert_ffn(exp_args):
        exp_in, exp_w_in, exp_w_out = exp_args
        hidden = jax.nn.gelu(jnp.dot(exp_in, exp_w_in, preferred_element_type=jnp.float32)).astype(jnp.bfloat16)
        return jnp.dot(hidden, exp_w_out, preferred_element_type=jnp.float32).astype(jnp.bfloat16)

    expert_out = lax.map(expert_ffn, (by_expert, w_in, w_out))
    slot_out = expert_out.reshape(EXPERTS, BATCH, SLOTS, D_MODEL).transpose(1, 0, 2, 3).reshape(BATCH, NUM_SLOTS, D_MODEL)

    def combine_row(row_args):
        row_tokens, row_len, row_slots = row_args
        logits = row_logits(row_tokens)
        is_valid = (positions < row_len)[:, None]
        combine_w = jax.nn.softmax(logits, axis=-1).astype(jnp.bfloat16)
        mixed = jnp.dot(combine_w, row_slots, preferred_element_type=jnp.float32).astype(jnp.bfloat16)
        return jnp.where(is_valid, mixed, jnp.zeros_like(mixed))

    return lax.map(combine_row, (tokens, lengths, slot_out))
```

```python
import functools

import jax
import jax.numpy as jnp
from jax import lax
from jax.experimental import pallas as pl
from jax.experimental.pallas import tpu as pltpu
from jax.sharding import PartitionSpec as P

CHUNK = 256
NDIM = 4
F32 = jnp.float32
BF16 = jnp.bfloat16
MESH = pl.DeviceIdType.MESH


def _nt(a, b):
    return lax.dot_general(a, b, (((1,), (1,)), ((), ())), preferred_element_type=F32)


def _nn(a, b):
    return jnp.dot(a, b, preferred_element_type=F32)


def _kernel(len_ref, gain_ref, tok_hbm, phi_hbm, wi_hbm, wo_hbm, y_hbm,
            x_v, phi_v, phit_v, wi_v, wo_v, ct_v, c_v, part, half_in, r0, r1, r2, r3,
            z_part, z_half, z0, z1, z2, z3, xs, xs_f, hid, hid_b, ys_f, yx, yx_in, gath,
            tok_sem, phi_sem, wi_sem, wo_sem, out_sem,
            hs_sem, hr_sem, zhs_sem, zhr_sem, zs_sem, zr_sem, rs_sem, rr_sem,
            xss_sem, xsr_sem, yxs_sem, yxr_sem, gs_sem, gr_sem, gds_sem, gdr_sem):
    rows, tok_count, width = x_v.shape
    experts = wi_v.shape[0]
    nk = width // CHUNK
    hrows = rows // 2
    gsz = hrows // NDIM
    nslots = phit_v.shape[0]
    chip_rows = 2 * experts
    me = lax.axis_index("seq")
    core = lax.rem(me, 2)
    chip = me // 2
    x = lax.rem(chip, 4)
    y = chip // 4
    xb = x // 2
    xa = lax.rem(x + xb, 2)
    yb = y // 2
    ya = lax.rem(y + yb, 2)
    bits = (yb, ya, xb, xa)

    def dev(yy, xx, cc):
        return {"seq": (yy * 4 + xx) * 2 + cc}

    mate = dev(y, x, 1 - core)
    flips = (
        dev(3 - y, x, core),
        dev(y + 1 - 2 * lax.rem(y, 2), x, core),
        dev(y, 3 - x, core),
        dev(y, x + 1 - 2 * lax.rem(x, 2), core),
    )
    orders = ((3, 1, 2, 0), (1, 2, 0, 3), (2, 0, 3, 1), (0, 3, 1, 2))
    own0 = core * hrows
    oth0 = (1 - core) * hrows

    barrier = pltpu.get_barrier_semaphore()
    for d in flips + (mate,):
        pl.semaphore_signal(barrier, inc=1, device_id=d, device_id_type=MESH)

    def tok_copy(b):
        return pltpu.make_async_copy(tok_hbm.at[b], x_v.at[b], tok_sem.at[b])

    phi_copy = pltpu.make_async_copy(phi_hbm, phi_v, phi_sem)
    phi_copy.start()
    for j in range(rows):
        tok_copy(lax.rem(oth0 + j, rows)).start()
    wi_copies = [pltpu.make_async_copy(wi_hbm.at[e], wi_v.at[e], wi_sem.at[e]) for e in range(experts)]
    wo_copies = [pltpu.make_async_copy(wo_hbm.at[e], wo_v.at[e], wo_sem.at[e]) for e in range(experts)]

    z_part[...] = jnp.zeros_like(z_part)
    ys_f[...] = jnp.zeros_like(ys_f)

    gain = gain_ref[0]
    shift = gain * (1.0 + 2.0 ** -7)
    phi_copy.wait()
    pf = phi_v[...].astype(F32)
    pn = (pf * (gain * lax.rsqrt(jnp.sum(pf * pf, axis=0, keepdims=True) + 1e-6))).astype(BF16)
    new = lax.broadcasted_iota(jnp.int32, (nslots, nslots), 0)
    old = lax.broadcasted_iota(jnp.int32, (nslots, nslots), 1)
    nchip = new // chip_rows
    nxa, nxb, nya, nyb = nchip & 1, (nchip >> 1) & 1, (nchip >> 2) & 1, (nchip >> 3) & 1
    src = ((2 * nyb + (nya ^ nyb)) * 4 + 2 * nxb + (nxa ^ nxb)) * chip_rows + (new & (chip_rows - 1))
    perm = jnp.where(src == old, 1.0, 0.0).astype(BF16)
    phit_v[...] = _nt(perm, pn).astype(BF16)

    lane = lax.broadcasted_iota(jnp.int32, (nslots, tok_count), 1)
    pos = me * tok_count + lane

    def front(b0):
        zs = []
        for u in range(gsz):
            b = b0 + u
            tok_copy(b).wait()
            xv = x_v[b]
            xf = xv.astype(F32)
            xn = (xf * lax.rsqrt(jnp.sum(xf * xf, axis=1, keepdims=True) + 1e-6)).astype(BF16)
            ex = jnp.exp(_nt(phit_v[...], xn) - shift)
            ct_v[b] = (ex * (1.0 / jnp.sum(ex, axis=0, keepdims=True))).astype(BF16)
            exm = jnp.where(pos < len_ref[b], ex, 0.0)
            zs.append(jnp.where(lane == b, jnp.sum(exm, axis=1, keepdims=True), 0.0))
            w = exm.astype(BF16)
            for k in range(nk):
                pk = _nn(w, xv[:, k * CHUNK:(k + 1) * CHUNK])
                part[k, b] = pk.reshape(2, 2, 2, 2, chip_rows, CHUNK).astype(BF16)
        z_part[...] += functools.reduce(jnp.add, zs).reshape(z_part.shape)

    def half_copy(q):
        return pltpu.make_async_remote_copy(
            part.at[:, pl.ds(oth0 + q * gsz, gsz)], half_in.at[:, pl.ds(q * gsz, gsz)],
            hs_sem.at[q], hr_sem.at[q], device_id=mate, device_id_type=MESH)

    def where_(order, s, flip):
        idx = [slice(None)] * NDIM
        for t in range(s):
            idx[order[t]] = bits[order[t]]
        if flip:
            idx[order[s]] = 1 - bits[order[s]]
        return tuple(idx)

    rbuf = (r0, r1, r2, r3)
    zbuf = (z0, z1, z2, z3)

    def rs_copy(k, q, s):
        order = orders[q]
        i = (k * NDIM + q) * NDIM + s
        return pltpu.make_async_remote_copy(
            part.at[(k, pl.ds(own0 + q * gsz, gsz)) + where_(order, s, True)],
            rbuf[s].at[k, pl.ds(q * gsz, gsz)],
            rs_sem.at[i], rr_sem.at[i], device_id=flips[order[s]], device_id_type=MESH)

    def z_copy(s):
        order = orders[0]
        return pltpu.make_async_remote_copy(
            z_part.at[where_(order, s, True)], zbuf[s],
            zs_sem.at[s], zr_sem.at[s], device_id=flips[order[s]], device_id_type=MESH)

    zh_copy = pltpu.make_async_remote_copy(
        z_part, z_half, zhs_sem, zhr_sem, device_id=mate, device_id_type=MESH)

    pl.semaphore_wait(barrier, NDIM + 1)

    def far(q, carry):
        front(oth0 + q * gsz)
        half_copy(q).start()
        return carry

    lax.fori_loop(0, NDIM, far, 0)
    for cp in wi_copies + wo_copies:
        cp.start()

    for q in range(NDIM):
        front(own0 + q * gsz)
        half_copy(q).wait_recv()
        for k in range(nk):
            for u in range(gsz):
                b = own0 + q * gsz + u
                part[k, b] = (part[k, b].astype(F32) + half_in[k, q * gsz + u].astype(F32)).astype(BF16)
            rs_copy(k, q, 0).start()

    zh_copy.start()
    zh_copy.wait()
    z_part[...] += z_half[...]
    z_copy(0).start()

    def flip_c(b, carry):
        c_v[b] = ct_v[b].astype(F32).T.astype(BF16)
        return carry

    lax.fori_loop(0, rows, flip_c, 0)

    def rs_add(k, q, s):
        order = orders[q]
        rs_copy(k, q, s).wait()
        for u in range(gsz):
            at = (k, own0 + q * gsz + u) + where_(order, s + 1, False)
            part[at] = (part[at].astype(F32) + rbuf[s][k, q * gsz + u].astype(F32)).astype(BF16)

    for s in range(NDIM - 1):
        for k in range(nk):
            for q in range(NDIM):
                rs_add(k, q, s)
                rs_copy(k, q, s + 1).start()
        z_copy(s).wait()
        at = where_(orders[0], s + 1, False)
        z_part[at] = z_part[at] + zbuf[s][...]
        z_copy(s + 1).start()

    z_copy(3).wait()
    z_own = z_part[bits] + z3[...]
    z_lane = lax.broadcasted_iota(jnp.int32, z_own.shape, 1)
    z_inv = [
        1.0 / jnp.sum(jnp.where(z_lane == own0 + j, z_own, 0.0), axis=1, keepdims=True)
        for j in range(hrows)
    ]

    def xs_copy(k):
        ref = xs.at[k, pl.ds(own0, hrows)]
        return pltpu.make_async_remote_copy(
            ref, ref, xss_sem.at[k], xsr_sem.at[k], device_id=mate, device_id_type=MESH)

    def ffn_in(k):
        xs_copy(k).wait()
        for t in range(CHUNK // 128):
            xs_f[t] = xs[k, :, :, t * 128:(t + 1) * 128].astype(F32).reshape(rows * chip_rows, 128)
        for e in range(experts):
            if k == 0:
                wi_copies[e].wait()
            pick = pl.ds(core * experts + e, rows, stride=chip_rows)
            xe = jnp.concatenate([xs_f[t, pick, :] for t in range(CHUNK // 128)], axis=1).astype(BF16)
            h = _nn(xe, wi_v[e, k * CHUNK:(k + 1) * CHUNK, :])
            hid[e] = h if k == 0 else hid[e] + h

    for k in range(nk):
        for q in range(NDIM):
            rs_copy(k, q, 3).wait()
            for u in range(gsz):
                j = q * gsz + u
                s_own = part[(k, own0 + j) + bits].astype(F32) + r3[k, j].astype(F32)
                xs[k, own0 + j] = (s_own * z_inv[j]).astype(BF16)
        xs_copy(k).start()
        if k > 0:
            ffn_in(k - 1)
    ffn_in(nk - 1)
    for e in range(experts):
        hid_b[e] = jax.nn.gelu(hid[e], approximate=True).astype(BF16)

    row8 = lax.broadcasted_iota(jnp.int32, (hrows, chip_rows, CHUNK), 1)
    mine8 = (row8 // experts) == core

    def yx_copy(k):
        return pltpu.make_async_remote_copy(
            yx.at[k, pl.ds(oth0, hrows)], yx_in.at[k],
            yxs_sem.at[k], yxr_sem.at[k], device_id=mate, device_id_type=MESH)

    def g_copy(k, q, s):
        order = orders[q]
        i = (k * NDIM + q) * NDIM + s
        ref = gath.at[(k, pl.ds(own0 + q * gsz, gsz)) + where_(order, s + 1, False)]
        return pltpu.make_async_remote_copy(
            ref, ref, gs_sem.at[i], gr_sem.at[i], device_id=flips[order[s]], device_id_type=MESH)

    def gd_copy(k, q):
        ref = gath.at[k, pl.ds(own0 + q * gsz, gsz)]
        i = k * NDIM + q
        return pltpu.make_async_remote_copy(
            ref, ref, gds_sem.at[i], gdr_sem.at[i], device_id=mate, device_id_type=MESH)

    def ffn_out(k):
        for e in range(experts):
            if k == 0:
                wo_copies[e].wait()
            ye = _nn(hid_b[e], wo_v[e, :, k * CHUNK:(k + 1) * CHUNK])
            for t in range(CHUNK // 128):
                ys_f[t, pl.ds(core * experts + e, rows, stride=chip_rows), :] = ye[:, t * 128:(t + 1) * 128]
        for t in range(CHUNK // 128):
            yx[k, :, :, t * 128:(t + 1) * 128] = ys_f[t].reshape(rows, chip_rows, 128).astype(BF16)
        yx_copy(k).start()

    def merge(k):
        yx_copy(k).wait()
        own = yx[k, pl.ds(own0, hrows)].astype(F32)
        merged = jnp.where(mine8, own, yx_in[k].astype(F32)).astype(BF16)
        gath[(k, pl.ds(own0, hrows)) + bits] = merged
        for q in range(NDIM):
            g_copy(k, q, NDIM - 1).start()

    for k in range(nk):
        ffn_out(k)
        if k > 0:
            merge(k - 1)
    merge(nk - 1)

    for s in range(NDIM - 1, 0, -1):
        for k in range(nk):
            for q in range(NDIM):
                g_copy(k, q, s).wait()
                g_copy(k, q, s - 1).start()

    row_pos = me * tok_count + lax.broadcasted_iota(jnp.int32, (tok_count, CHUNK), 0)

    def mix(k, b0):
        for u in range(gsz):
            b = b0 + u
            gb = gath[k, b].astype(F32).reshape(nslots, CHUNK).astype(BF16)
            yk = jnp.where(row_pos < len_ref[b], _nn(c_v[b], gb), 0.0)
            x_v[b, :, k * CHUNK:(k + 1) * CHUNK] = yk.astype(BF16)

    def out_copy(b):
        return pltpu.make_async_copy(x_v.at[b], y_hbm.at[b], out_sem.at[b])

    for k in range(nk):
        for q in range(NDIM):
            g_copy(k, q, 0).wait()
            gd_copy(k, q).start()
            mix(k, own0 + q * gsz)
            if k == nk - 1:
                for u in range(gsz):
                    out_copy(own0 + q * gsz + u).start()
    for k in range(nk):
        for q in range(NDIM):
            gd_copy(k, q).wait()
            mix(k, oth0 + q * gsz)
            if k == nk - 1:
                for u in range(gsz):
                    out_copy(oth0 + q * gsz + u).start()
    for q in range(NDIM):
        half_copy(q).wait_send()
    for b in range(rows):
        out_copy(b).wait()


def solution(mesh):
    def shard_body(tok, lens, phi, gain, w_in, w_out):
        rows, tok_count, width = tok.shape
        experts, _, ff = w_in.shape
        nslots = phi.shape[1]
        nk = width // CHUNK
        hrows = rows // 2
        cr = 2 * experts
        cube = (2, 2, 2, 2)
        vm = pltpu.VMEM
        dma = pltpu.SemaphoreType.DMA
        anyspace = pl.BlockSpec(memory_space=pl.ANY)
        smem = pl.BlockSpec(memory_space=pltpu.SMEM)
        scratch = [
            vm((rows, tok_count, width), BF16),
            vm((width, nslots), BF16),
            vm((nslots, width), BF16),
            vm(w_in.shape, BF16),
            vm(w_out.shape, BF16),
            vm((rows, nslots, tok_count), BF16),
            vm((rows, tok_count, nslots), BF16),
            vm((nk, rows) + cube + (cr, CHUNK), BF16),
            vm((nk, hrows) + cube + (cr, CHUNK), BF16),
            vm((nk, hrows, 2, 2, 2, cr, CHUNK), BF16),
            vm((nk, hrows, 2, 2, cr, CHUNK), BF16),
            vm((nk, hrows, 2, cr, CHUNK), BF16),
            vm((nk, hrows, cr, CHUNK), BF16),
            vm(cube + (cr, tok_count), F32),
            vm(cube + (cr, tok_count), F32),
            vm((2, 2, 2, cr, tok_count), F32),
            vm((2, 2, cr, tok_count), F32),
            vm((2, cr, tok_count), F32),
            vm((cr, tok_count), F32),
            vm((nk, rows, cr, CHUNK), BF16),
            vm((CHUNK // 128, rows * cr, 128), F32),
            vm((experts, rows, ff), F32),
            vm((experts, rows, ff), BF16),
            vm((CHUNK // 128, rows * cr, 128), F32),
            vm((nk, rows, cr, CHUNK), BF16),
            vm((nk, hrows, cr, CHUNK), BF16),
            vm((nk, rows) + cube + (cr, CHUNK), BF16),
            dma((rows,)), dma, dma((experts,)), dma((experts,)), dma((rows,)),
            dma((NDIM,)), dma((NDIM,)), dma, dma, dma((NDIM,)), dma((NDIM,)),
            dma((nk * NDIM * NDIM,)), dma((nk * NDIM * NDIM,)),
            dma((nk,)), dma((nk,)), dma((nk,)), dma((nk,)),
            dma((nk * NDIM * NDIM,)), dma((nk * NDIM * NDIM,)),
            dma((nk * NDIM,)), dma((nk * NDIM,)),
        ]
        return pl.pallas_call(
            _kernel,
            out_shape=jax.ShapeDtypeStruct(tok.shape, BF16),
            in_specs=[smem, smem, anyspace, anyspace, anyspace, anyspace],
            out_specs=anyspace,
            scratch_shapes=scratch,
            compiler_params=pltpu.CompilerParams(
                collective_id=0, has_side_effects=True, vmem_limit_bytes=67043328),
        )(lens, gain, tok, phi, w_in, w_out)

    return jax.shard_map(
        shard_body,
        mesh=mesh,
        in_specs=(P("data", "seq", None), P("data"), P(None, None), P(None), P("seq", None, None), P("seq", None, None)),
        out_specs=P("data", "seq", None),
        check_vma=False,
    )
```

```python
import functools

import jax
import jax.numpy as jnp
from jax import lax
from jax.experimental import pallas as pl
from jax.experimental.pallas import tpu as pltpu
from jax.sharding import PartitionSpec as P

CHUNK = 256
GROUPS = 4
F32 = jnp.float32
BF16 = jnp.bfloat16
MESH = pl.DeviceIdType.MESH
ORDERS = ((3, 1, 2, 0), (1, 2, 3, 0), (2, 0, 3, 1), (0, 3, 2, 1))
FLIPS = tuple((f & 1, (f >> 1) & 1, (f >> 2) & 1) for f in range(1, 8))


def _nt(a, b):
    return lax.dot_general(a, b, (((1,), (1,)), ((), ())), preferred_element_type=F32)


def _nn(a, b):
    return jnp.dot(a, b, preferred_element_type=F32)


def _exchange_kernel(len_ref, gain_ref, tok_hbm, phi_hbm, wi_hbm, wo_hbm, g_hbm, c_hbm,
                     x_v, xn_v, w_v, phi_v, phit_v, wi_v, wo_v, ct_v, c_v, part, half_in, r0, r1, q_out, q_in,
                     z_part, z_half, z0, z1, zq, xs_f, hid, hid_b, ys_f, yx, g_in, gath,
                     phi_sem, tok_sem, wi_sem, wo_sem, c_sem,
                     hs_sem, hr_sem, zhs_sem, zhr_sem, zs_sem, zr_sem, rs_sem, rr_sem,
                     qs_sem, qr_sem, ys_sem, yr_sem, gs_sem, gr_sem, gds_sem, gdr_sem, go_sem):
    rows, tok_count, width = x_v.shape
    experts = wi_v.shape[0]
    nk = width // CHUNK
    hrows = rows // 2
    gsz = hrows // GROUPS
    nslots = phit_v.shape[0]
    chip_rows = 2 * experts
    me = lax.axis_index("seq")
    core = lax.rem(me, 2)
    chip = me // 2
    x = lax.rem(chip, 4)
    y = chip // 4
    xb = x // 2
    xa = lax.rem(x + xb, 2)
    yb = y // 2
    ya = lax.rem(y + yb, 2)
    bits = (yb, ya, xb, xa)

    def peer(dims, flip_core=0):
        b = [1 - v if d in dims else v for d, v in enumerate(bits)]
        yy = 2 * b[0] + lax.rem(b[0] + b[1], 2)
        xx = 2 * b[2] + lax.rem(b[2] + b[3], 2)
        return {"seq": (yy * 4 + xx) * 2 + (1 - core if flip_core else core)}

    def group_peer(q, f):
        fu, fv, fc = FLIPS[f]
        dims = tuple(d for d, on in zip(ORDERS[q][2:], (fu, fv)) if on)
        return peer(dims, fc)

    mate = peer((), 1)
    steps = tuple(peer((d,)) for d in range(4))
    own0 = core * hrows
    oth0 = (1 - core) * hrows

    pairs = sorted({dims for q in range(GROUPS) for dims in (tuple(sorted(ORDERS[q][2:])),)})
    greet = []
    for fc in (0, 1):
        greet += [peer((d,), fc) for d in range(4)]
        greet += [peer(dims, fc) for dims in pairs]
    greet.append(mate)
    barrier = pltpu.get_barrier_semaphore()
    for d in greet:
        pl.semaphore_signal(barrier, inc=1, device_id=d, device_id_type=MESH)

    def tok_copy(h):
        at = pl.ds(oth0 if h == 0 else own0, hrows)
        return pltpu.make_async_copy(tok_hbm.at[at], x_v.at[at], tok_sem.at[h])

    phi_copy = pltpu.make_async_copy(phi_hbm, phi_v, phi_sem)
    wi_copies = [pltpu.make_async_copy(wi_hbm.at[e], wi_v.at[e], wi_sem.at[e]) for e in range(experts)]
    wo_copies = [pltpu.make_async_copy(wo_hbm.at[e], wo_v.at[e], wo_sem.at[e]) for e in range(experts)]
    phi_copy.start()
    tok_copy(0).start()
    tok_copy(1).start()

    z_part[...] = jnp.zeros_like(z_part)
    gain = gain_ref[0]
    shift = gain * (1.0 + 2.0 ** -7)
    lane = lax.broadcasted_iota(jnp.int32, (nslots, tok_count), 1)
    pos = me * tok_count + lane

    def batch(i):
        return oth0 + i if i < hrows else own0 + i - hrows

    def normalise(i):
        xf = x_v[batch(i)].astype(F32)
        xn_v[i] = (xf * lax.rsqrt(jnp.sum(xf * xf, axis=1, keepdims=True) + 1e-6)).astype(BF16)

    def weigh(i):
        b = batch(i)
        ex = jnp.exp(_nt(phit_v[...], xn_v[i]) - shift)
        ct_v[b] = (ex * (1.0 / jnp.sum(ex, axis=0, keepdims=True))).astype(BF16)
        exm = jnp.where(pos < len_ref[b], ex, 0.0)
        w_v[i] = exm.astype(BF16)
        zs = jnp.where(lane == b, jnp.sum(exm, axis=1, keepdims=True), 0.0)
        z_part[...] += zs.reshape(z_part.shape)

    def collect(i):
        b = batch(i)
        for k in range(nk):
            pk = _nn(w_v[i], x_v[b, :, k * CHUNK:(k + 1) * CHUNK])
            part[k, b] = pk.reshape(2, 2, 2, 2, chip_rows, CHUNK).astype(BF16)

    def half_copy(q):
        return pltpu.make_async_remote_copy(
            part.at[:, pl.ds(oth0 + q * gsz, gsz)], half_in.at[:, pl.ds(q * gsz, gsz)],
            hs_sem.at[q], hr_sem.at[q], device_id=mate, device_id_type=MESH)

    def region(order, fixed, flip=None):
        idx = [slice(None)] * 4
        for t in range(fixed):
            idx[order[t]] = bits[order[t]]
        if flip is not None:
            idx[flip] = 1 - bits[flip]
        return tuple(idx)

    rbuf = (r0, r1)
    zbuf = (z0, z1)

    def rs_copy(k, q, s):
        order = ORDERS[q]
        i = (k * GROUPS + q) * 2 + s
        return pltpu.make_async_remote_copy(
            part.at[(k, pl.ds(own0 + q * gsz, gsz)) + region(order, s, order[s])],
            rbuf[s].at[k, pl.ds(q * gsz, gsz)],
            rs_sem.at[i], rr_sem.at[i], device_id=steps[order[s]], device_id_type=MESH)

    def z_copy(s):
        order = ORDERS[0]
        return pltpu.make_async_remote_copy(
            z_part.at[region(order, s, order[s])], zbuf[s],
            zs_sem.at[s], zr_sem.at[s], device_id=steps[order[s]], device_id_type=MESH)

    def zq_copy(f):
        fu, fv, _ = FLIPS[f]
        order = ORDERS[0]
        idx = list(bits)
        for d, on in zip(order[2:], (fu, fv)):
            if on:
                idx[d] = 1 - idx[d]
        return pltpu.make_async_remote_copy(
            z_part.at[tuple(idx)], zq.at[f], zs_sem.at[2 + f], zr_sem.at[2 + f],
            device_id=group_peer(0, f), device_id_type=MESH)

    zh_copy = pltpu.make_async_remote_copy(
        z_part, z_half, zhs_sem, zhr_sem, device_id=mate, device_id_type=MESH)

    phi_copy.wait()
    pf = phi_v[...].astype(F32)
    pn = (pf * (gain * lax.rsqrt(jnp.sum(pf * pf, axis=0, keepdims=True) + 1e-6))).astype(BF16)
    new = lax.broadcasted_iota(jnp.int32, (nslots, nslots), 0)
    old = lax.broadcasted_iota(jnp.int32, (nslots, nslots), 1)
    nchip = new // chip_rows
    nxa, nxb, nya, nyb = nchip & 1, (nchip >> 1) & 1, (nchip >> 2) & 1, (nchip >> 3) & 1
    src = ((2 * nyb + (nya ^ nyb)) * 4 + 2 * nxb + (nxa ^ nxb)) * chip_rows + (new & (chip_rows - 1))
    perm = jnp.where(src == old, 1.0, 0.0).astype(BF16)
    phit_v[...] = _nt(perm, pn).astype(BF16)

    tok_copy(0).wait()
    for cp in wi_copies + wo_copies:
        cp.start()
    for i in range(hrows + 2):
        if i < hrows:
            normalise(i)
        if 1 <= i < hrows + 1:
            weigh(i - 1)
        if i >= 2:
            collect(i - 2)
    pl.semaphore_wait(barrier, len(greet))
    for q in range(GROUPS):
        half_copy(q).start()
    tok_copy(1).wait()
    for i in range(hrows, rows + 2):
        if i < rows:
            normalise(i)
        if hrows + 1 <= i < rows + 1:
            weigh(i - 1)
        if i >= hrows + 2:
            collect(i - 2)
    zh_copy.start()

    for q in range(GROUPS):
        half_copy(q).wait_recv()
        for k in range(nk):
            for u in range(gsz):
                b = own0 + q * gsz + u
                part[k, b] = (part[k, b].astype(F32) + half_in[k, q * gsz + u].astype(F32)).astype(BF16)
            rs_copy(k, q, 0).start()

    zh_copy.wait()
    z_part[...] += z_half[...]
    z_copy(0).start()


    def flip_c(i, carry):
        for u in range(4):
            c_v[4 * i + u] = ct_v[4 * i + u].astype(F32).T.astype(BF16)
        return carry

    lax.fori_loop(0, rows // 4, flip_c, 0)
    c_copy = pltpu.make_async_copy(c_v, c_hbm, c_sem)
    c_copy.start()

    def q_copy(k, q, f):
        fu, fv, fc = FLIPS[f]
        o = ORDERS[q]
        mu, mv = bits[o[2]], bits[o[3]]
        du = 1 - mu if fu else mu
        dv = 1 - mv if fv else mv
        dc = 1 - core if fc else core
        i = (k * GROUPS + q) * 7 + f
        return pltpu.make_async_remote_copy(
            q_out.at[k, q, dc, du, dv], q_in.at[k, q, core, mu, mv],
            qs_sem.at[i], qr_sem.at[i], device_id=group_peer(q, f), device_id_type=MESH)

    row8 = lax.broadcasted_iota(jnp.int32, (chip_rows, CHUNK), 0)
    low = row8 < experts

    def at_rest(q, u, v):
        o = ORDERS[q]
        idx = list(bits)
        idx[o[2]] = u
        idx[o[3]] = v
        return tuple(idx)

    def at_recv(q, u, v):
        o = ORDERS[q]
        free = sorted(o[2:])
        val = {o[2]: u, o[3]: v}
        return tuple(val[d] for d in free)

    for k in range(nk):
        for q in range(GROUPS):
            o = ORDERS[q]
            rs_copy(k, q, 0).wait()
            for u in range(gsz):
                at = (k, own0 + q * gsz + u) + region(o, 1)
                part[at] = (part[at].astype(F32) + r0[k, q * gsz + u].astype(F32)).astype(BF16)
            rs_copy(k, q, 1).start()
    z_copy(0).wait()
    at = region(ORDERS[0], 1)
    z_part[at] = z_part[at] + z0[...]
    z_copy(1).start()
    for k in range(nk):
        for q in range(GROUPS):
            o = ORDERS[q]
            mu, mv = bits[o[2]], bits[o[3]]
            rs_copy(k, q, 1).wait()
            for u in range(2):
                for v in range(2):
                    ev, od = [
                        part[(k, own0 + q * gsz + w) + at_rest(q, u, v)].astype(F32)
                        + r1[(k, q * gsz + w) + at_recv(q, u, v)].astype(F32)
                        for w in range(gsz)
                    ]
                    q_out[k, q, 0, u, v] = jnp.where(low, ev, pltpu.roll(od, experts, 0)).astype(BF16)
                    q_out[k, q, 1, u, v] = jnp.where(low, pltpu.roll(ev, experts, 0), od).astype(BF16)
            for f in range(7):
                q_copy(k, q, f).start()
            q_in[k, q, core, mu, mv] = q_out[k, q, core, mu, mv]
    z_copy(1).wait()
    at = region(ORDERS[0], 2)
    z_part[at] = z_part[at] + z1[...]
    for f in range(3):
        zq_copy(f).start()
    for f in range(3):
        zq_copy(f).wait()
    z_own = z_part[bits] + (zq[0] + (zq[1] + zq[2]))
    zrow = lax.broadcasted_iota(jnp.int32, z_own.shape, 0)
    eye = lax.broadcasted_iota(jnp.int32, (rows, z_own.shape[1]), 0) == lax.broadcasted_iota(
        jnp.int32, (rows, z_own.shape[1]), 1)
    z_inv = []
    for e in range(experts):
        zr = jnp.sum(jnp.where(zrow == core * experts + e, z_own, 0.0), axis=0, keepdims=True)
        z_inv.append(1.0 / jnp.sum(jnp.where(eye, zr, 0.0), axis=1, keepdims=True))

    lanes = CHUNK // 128
    for cp in wi_copies:
        cp.wait()
    for k in range(nk):
        for q in range(GROUPS):
            for f in range(7):
                q_copy(k, q, f).wait()
        for cs in range(2):
            for q in range(GROUPS):
                p = cs * GROUPS + q
                s = [q_in[k, q, cs, u, v].astype(F32) for u in range(2) for v in range(2)]
                s = (s[0] + s[1]) + (s[2] + s[3])
                for t in range(lanes):
                    xs_f[t, p * chip_rows:(p + 1) * chip_rows, :] = s[:, t * 128:(t + 1) * 128]
        for e in range(experts):
            pick = pl.ds(e, rows, stride=experts)
            xe = jnp.concatenate([xs_f[t, pick, :] for t in range(lanes)], axis=1)
            h = _nn((xe * z_inv[e]).astype(BF16), wi_v[e, k * CHUNK:(k + 1) * CHUNK, :])
            hid[e] = h if k == 0 else hid[e] + h
    for cp in wo_copies:
        cp.wait()
    for e in range(experts):
        hid_b[e] = jax.nn.gelu(hid[e], approximate=True).astype(BF16)

    def y_copy(k, q, f):
        _, _, fc = FLIPS[f]
        o = ORDERS[q]
        dc = 1 - core if fc else core
        i = (k * GROUPS + q) * 7 + f
        return pltpu.make_async_remote_copy(
            yx.at[k, dc * GROUPS + q], g_in.at[k, q, core, bits[o[2]], bits[o[3]]],
            ys_sem.at[i], yr_sem.at[i], device_id=group_peer(q, f), device_id_type=MESH)

    def g_copy(k, q, s):
        i = (k * GROUPS + q) * 2 + s
        ref = gath.at[(k, pl.ds(own0 + q * gsz, gsz)) + region(ORDERS[q], s + 1)]
        return pltpu.make_async_remote_copy(
            ref, ref, gs_sem.at[i], gr_sem.at[i], device_id=steps[ORDERS[q][s]], device_id_type=MESH)

    def gd_copy(k, q):
        at = (k, pl.ds(own0 + q * gsz, gsz))
        i = k * GROUPS + q
        return pltpu.make_async_remote_copy(
            gath.at[at], g_hbm.at[at], gds_sem.at[i], gdr_sem.at[i], device_id=mate, device_id_type=MESH)

    def go_copy(k, q):
        at = (k, pl.ds(own0 + q * gsz, gsz))
        return pltpu.make_async_copy(gath.at[at], g_hbm.at[at], go_sem.at[k * GROUPS + q])

    for k in range(nk):
        for e in range(experts):
            ye = _nn(hid_b[e], wo_v[e, :, k * CHUNK:(k + 1) * CHUNK])
            for t in range(lanes):
                ys_f[t, pl.ds(e, rows, stride=experts), :] = ye[:, t * 128:(t + 1) * 128]
        for t in range(lanes):
            yx[k, :, :, t * 128:(t + 1) * 128] = ys_f[t].reshape(rows // 2, chip_rows, 128).astype(BF16)
        for q in range(GROUPS):
            o = ORDERS[q]
            for f in range(7):
                y_copy(k, q, f).start()
            g_in[k, q, core, bits[o[2]], bits[o[3]]] = yx[k, core * GROUPS + q]

    for k in range(nk):
        for q in range(GROUPS):
            for f in range(7):
                y_copy(k, q, f).wait()
            for u in range(2):
                for v in range(2):
                    s0 = g_in[k, q, 0, u, v].astype(F32)
                    s1 = g_in[k, q, 1, u, v].astype(F32)
                    at = at_rest(q, u, v)
                    gath[(k, own0 + q * gsz) + at] = jnp.where(low, s0, pltpu.roll(s1, experts, 0)).astype(BF16)
                    gath[(k, own0 + q * gsz + 1) + at] = jnp.where(low, pltpu.roll(s0, experts, 0), s1).astype(BF16)
            g_copy(k, q, 1).start()
    for k in range(nk):
        for q in range(GROUPS):
            g_copy(k, q, 1).wait()
            g_copy(k, q, 0).start()
    for k in range(nk):
        for q in range(GROUPS):
            g_copy(k, q, 0).wait()
            gd_copy(k, q).start()
            go_copy(k, q).start()
    for k in range(nk):
        for q in range(GROUPS):
            gd_copy(k, q).wait()
            go_copy(k, q).wait()
    for q in range(GROUPS):
        half_copy(q).wait_send()
    c_copy.wait()


def _mix_kernel(len_ref, g_hbm, c_hbm, y_hbm, g_v, c_v, y_v, g_sem, c_sem, y_sem):
    rows, tok_count, width = y_v.shape
    nk = g_v.shape[0]
    nslots = c_v.shape[2]

    def c_copy(b):
        return pltpu.make_async_copy(c_hbm.at[b], c_v.at[b], c_sem.at[b])

    def g_copy(b):
        return pltpu.make_async_copy(g_hbm.at[:, b], g_v.at[:, b], g_sem.at[b])

    def y_copy(b):
        return pltpu.make_async_copy(y_v.at[b], y_hbm.at[b], y_sem.at[b])

    for b in range(rows):
        c_copy(b).start()
        g_copy(b).start()
    row_pos = lax.axis_index("seq") * tok_count + lax.broadcasted_iota(jnp.int32, (tok_count, CHUNK), 0)
    for b0 in range(0, rows, 2):
        for b in (b0, b0 + 1):
            c_copy(b).wait()
            g_copy(b).wait()
        for b in (b0, b0 + 1):
            for k in range(nk):
                gb = g_v[k, b].astype(F32).reshape(nslots, CHUNK).astype(BF16)
                yk = jnp.where(row_pos < len_ref[b], _nn(c_v[b], gb), 0.0)
                y_v[b, :, k * CHUNK:(k + 1) * CHUNK] = yk.astype(BF16)
        for b in (b0, b0 + 1):
            y_copy(b).start()
    for b in range(rows):
        y_copy(b).wait()


def solution(mesh):
    def shard_body(tok, lens, phi, gain, w_in, w_out):
        rows, tok_count, width = tok.shape
        experts, _, ff = w_in.shape
        nslots = phi.shape[1]
        nk = width // CHUNK
        hrows = rows // 2
        cr = 2 * experts
        cube = (2, 2, 2, 2)
        tile = (cr, CHUNK)
        lanes = CHUNK // 128
        vm = pltpu.VMEM
        dma = pltpu.SemaphoreType.DMA
        anyspace = pl.BlockSpec(memory_space=pl.ANY)
        smem = pl.BlockSpec(memory_space=pltpu.SMEM)
        gshape = (nk, rows) + cube + tile
        scratch = [
            vm((rows, tok_count, width), BF16),
            vm((rows, tok_count, width), BF16),
            vm((rows, nslots, tok_count), BF16),
            vm((width, nslots), BF16),
            vm((nslots, width), BF16),
            vm(w_in.shape, BF16),
            vm(w_out.shape, BF16),
            vm((rows, nslots, tok_count), BF16),
            vm((rows, tok_count, nslots), BF16),
            vm(gshape, BF16),
            vm((nk, hrows) + cube + tile, BF16),
            vm((nk, hrows, 2, 2, 2) + tile, BF16),
            vm((nk, hrows, 2, 2) + tile, BF16),
            vm((nk, GROUPS, 2, 2, 2) + tile, BF16),
            vm((nk, GROUPS, 2, 2, 2) + tile, BF16),
            vm(cube + (cr, tok_count), F32),
            vm(cube + (cr, tok_count), F32),
            vm((2, 2, 2, cr, tok_count), F32),
            vm((2, 2, cr, tok_count), F32),
            vm((3, cr, tok_count), F32),
            vm((lanes, rows * experts, 128), F32),
            vm((experts, rows, ff), F32),
            vm((experts, rows, ff), BF16),
            vm((lanes, rows * experts, 128), F32),
            vm((nk, rows // 2) + tile, BF16),
            vm((nk, GROUPS, 2, 2, 2) + tile, BF16),
            vm(gshape, BF16),
            dma, dma((2,)), dma((experts,)), dma((experts,)), dma,
            dma((GROUPS,)), dma((GROUPS,)), dma, dma, dma((5,)), dma((5,)),
            dma((nk * GROUPS * 2,)), dma((nk * GROUPS * 2,)),
            dma((nk * GROUPS * 7,)), dma((nk * GROUPS * 7,)),
            dma((nk * GROUPS * 7,)), dma((nk * GROUPS * 7,)),
            dma((nk * GROUPS * 2,)), dma((nk * GROUPS * 2,)),
            dma((nk * GROUPS,)), dma((nk * GROUPS,)), dma((nk * GROUPS,)),
        ]
        gath, comb = pl.pallas_call(
            _exchange_kernel,
            out_shape=(
                jax.ShapeDtypeStruct(gshape, BF16),
                jax.ShapeDtypeStruct((rows, tok_count, nslots), BF16),
            ),
            in_specs=[smem, smem, anyspace, anyspace, anyspace, anyspace],
            out_specs=(anyspace, anyspace),
            scratch_shapes=scratch,
            compiler_params=pltpu.CompilerParams(
                collective_id=0, has_side_effects=True, vmem_limit_bytes=67043328),
        )(lens, gain, tok, phi, w_in, w_out)
        return pl.pallas_call(
            _mix_kernel,
            out_shape=jax.ShapeDtypeStruct(tok.shape, BF16),
            in_specs=[smem, anyspace, anyspace],
            out_specs=anyspace,
            scratch_shapes=[
                vm(gshape, BF16),
                vm((rows, tok_count, nslots), BF16),
                vm(tok.shape, BF16),
                dma((rows,)), dma((rows,)), dma((rows,)),
            ],
        )(lens, gath, comb)

    return jax.shard_map(
        shard_body,
        mesh=mesh,
        in_specs=(P("data", "seq", None), P("data"), P(None, None), P(None), P("seq", None, None), P("seq", None, None)),
        out_specs=P("data", "seq", None),
        check_vma=False,
    )
```

```python
import functools

import jax
import jax.numpy as jnp
from jax import lax
from jax.experimental import pallas as pl
from jax.experimental.pallas import tpu as pltpu
from jax.sharding import PartitionSpec as P

CHUNK = 256
GROUPS = 4
F32 = jnp.float32
BF16 = jnp.bfloat16
MESH = pl.DeviceIdType.MESH
ORDERS = ((3, 1, 2, 0), (1, 3, 2, 0), (2, 0, 3, 1), (0, 2, 3, 1))
FLIPS = tuple((f & 1, (f >> 1) & 1, (f >> 2) & 1) for f in range(1, 8))


def _nt(a, b):
    return lax.dot_general(a, b, (((1,), (1,)), ((), ())), preferred_element_type=F32)


def _nn(a, b):
    return jnp.dot(a, b, preferred_element_type=F32)


def _exchange_kernel(len_ref, gain_ref, tok_hbm, phi_hbm, wi_hbm, wo_hbm, g_hbm, c_hbm,
                     x_v, xn_v, w_v, phi_v, phit_v, wi_v, wo_v, ct_v, c_v, part, half_in, r0, r1, q_out, q_in,
                     z_part, z_half, z0, z1, zq, xs_f, hid, hid_b, ys_f, yx, g_in, gath,
                     phi_sem, tok_sem, wi_sem, wo_sem, c_sem,
                     hs_sem, hr_sem, zhs_sem, zhr_sem, zs_sem, zr_sem, rs_sem, rr_sem,
                     qs_sem, qr_sem, ys_sem, yr_sem, gs_sem, gr_sem, gds_sem, gdr_sem, go_sem):
    rows, tok_count, width = x_v.shape
    experts = wi_v.shape[0]
    nk = width // CHUNK
    hrows = rows // 2
    gsz = hrows // GROUPS
    nslots = phit_v.shape[0]
    chip_rows = 2 * experts
    me = lax.axis_index("seq")
    core = lax.rem(me, 2)
    chip = me // 2
    x = lax.rem(chip, 4)
    y = chip // 4
    xb = x // 2
    xa = lax.rem(x + xb, 2)
    yb = y // 2
    ya = lax.rem(y + yb, 2)
    bits = (yb, ya, xb, xa)

    def peer(dims, flip_core=0):
        b = [1 - v if d in dims else v for d, v in enumerate(bits)]
        yy = 2 * b[0] + lax.rem(b[0] + b[1], 2)
        xx = 2 * b[2] + lax.rem(b[2] + b[3], 2)
        return {"seq": (yy * 4 + xx) * 2 + (1 - core if flip_core else core)}

    def group_peer(q, f):
        fu, fv, fc = FLIPS[f]
        dims = tuple(d for d, on in zip(ORDERS[q][2:], (fu, fv)) if on)
        return peer(dims, fc)

    mate = peer((), 1)
    steps = tuple(peer((d,)) for d in range(4))
    own0 = core * hrows
    oth0 = (1 - core) * hrows

    pairs = sorted({dims for q in range(GROUPS) for dims in (tuple(sorted(ORDERS[q][2:])),)})
    greet = []
    for fc in (0, 1):
        greet += [peer((d,), fc) for d in range(4)]
        greet += [peer(dims, fc) for dims in pairs]
    greet.append(mate)
    barrier = pltpu.get_barrier_semaphore()
    for d in greet:
        pl.semaphore_signal(barrier, inc=1, device_id=d, device_id_type=MESH)

    def batch(i):
        q, r = divmod(i, 2 * gsz)
        return (oth0 if r < gsz else own0 - gsz) + q * gsz + r

    def tok_copy(i):
        at = pl.ds(batch(i), gsz)
        return pltpu.make_async_copy(tok_hbm.at[at], x_v.at[at], tok_sem.at[i // gsz])

    phi_copy = pltpu.make_async_copy(phi_hbm, phi_v, phi_sem)
    wi_copies = [pltpu.make_async_copy(wi_hbm.at[e], wi_v.at[e], wi_sem.at[e]) for e in range(experts)]
    wo_copies = [pltpu.make_async_copy(wo_hbm.at[e], wo_v.at[e], wo_sem.at[e]) for e in range(experts)]
    phi_copy.start()
    for i in range(0, rows, gsz):
        tok_copy(i).start()

    z_part[...] = jnp.zeros_like(z_part)
    gain = gain_ref[0]
    shift = gain * (1.0 + 2.0 ** -7)
    lane = lax.broadcasted_iota(jnp.int32, (nslots, tok_count), 1)
    pos = me * tok_count + lane

    def normalise(i):
        xf = x_v[batch(i)].astype(F32)
        xn_v[i] = (xf * lax.rsqrt(jnp.sum(xf * xf, axis=1, keepdims=True) + 1e-6)).astype(BF16)

    def weigh(i):
        b = batch(i)
        ex = jnp.exp(_nt(phit_v[...], xn_v[i]) - shift)
        ct_v[b] = (ex * (1.0 / jnp.sum(ex, axis=0, keepdims=True))).astype(BF16)
        exm = jnp.where(pos < len_ref[b], ex, 0.0)
        w_v[i] = exm.astype(BF16)
        zs = jnp.where(lane == b, jnp.sum(exm, axis=1, keepdims=True), 0.0)
        z_part[...] += zs.reshape(z_part.shape)

    def collect(i):
        b = batch(i)
        for k in range(nk):
            pk = _nn(w_v[i], x_v[b, :, k * CHUNK:(k + 1) * CHUNK])
            part[k, b] = pk.reshape(2, 2, 2, 2, chip_rows, CHUNK).astype(BF16)

    def half_copy(q):
        return pltpu.make_async_remote_copy(
            part.at[:, pl.ds(oth0 + q * gsz, gsz)], half_in.at[:, pl.ds(q * gsz, gsz)],
            hs_sem.at[q], hr_sem.at[q], device_id=mate, device_id_type=MESH)

    def region(order, fixed, flip=None):
        idx = [slice(None)] * 4
        for t in range(fixed):
            idx[order[t]] = bits[order[t]]
        if flip is not None:
            idx[flip] = 1 - bits[flip]
        return tuple(idx)

    rbuf = (r0, r1)
    zbuf = (z0, z1)

    def rs_copy(k, q, s):
        order = ORDERS[q]
        i = (k * GROUPS + q) * 2 + s
        return pltpu.make_async_remote_copy(
            part.at[(k, pl.ds(own0 + q * gsz, gsz)) + region(order, s, order[s])],
            rbuf[s].at[k, pl.ds(q * gsz, gsz)],
            rs_sem.at[i], rr_sem.at[i], device_id=steps[order[s]], device_id_type=MESH)

    def z_copy(s):
        order = ORDERS[0]
        return pltpu.make_async_remote_copy(
            z_part.at[region(order, s, order[s])], zbuf[s],
            zs_sem.at[s], zr_sem.at[s], device_id=steps[order[s]], device_id_type=MESH)

    def zq_copy(f):
        fu, fv, _ = FLIPS[f]
        order = ORDERS[0]
        idx = list(bits)
        for d, on in zip(order[2:], (fu, fv)):
            if on:
                idx[d] = 1 - idx[d]
        return pltpu.make_async_remote_copy(
            z_part.at[tuple(idx)], zq.at[f], zs_sem.at[2 + f], zr_sem.at[2 + f],
            device_id=group_peer(0, f), device_id_type=MESH)

    zh_copy = pltpu.make_async_remote_copy(
        z_part, z_half, zhs_sem, zhr_sem, device_id=mate, device_id_type=MESH)

    phi_copy.wait()
    pf = phi_v[...].astype(F32)
    pn = (pf * (gain * lax.rsqrt(jnp.sum(pf * pf, axis=0, keepdims=True) + 1e-6))).astype(BF16)
    new = lax.broadcasted_iota(jnp.int32, (nslots, nslots), 0)
    old = lax.broadcasted_iota(jnp.int32, (nslots, nslots), 1)
    nchip = new // chip_rows
    nxa, nxb, nya, nyb = nchip & 1, (nchip >> 1) & 1, (nchip >> 2) & 1, (nchip >> 3) & 1
    src = ((2 * nyb + (nya ^ nyb)) * 4 + 2 * nxb + (nxa ^ nxb)) * chip_rows + (new & (chip_rows - 1))
    perm = jnp.where(src == old, 1.0, 0.0).astype(BF16)
    phit_v[...] = _nt(perm, pn).astype(BF16)

    for cp in wi_copies + wo_copies:
        cp.start()

    def half_add(q):
        half_copy(q).wait_recv()
        for k in range(nk):
            for u in range(gsz):
                b = own0 + q * gsz + u
                part[k, b] = part[k, b] + half_in[k, q * gsz + u]
            rs_copy(k, q, 0).start()

    for i in range(rows + 2):
        if i < rows and i % gsz == 0:
            tok_copy(i).wait()
        if i < rows:
            normalise(i)
        if 1 <= i < rows + 1:
            weigh(i - 1)
        if i >= 2:
            collect(i - 2)
            q, r = divmod(i - 2, 2 * gsz)
            if r == gsz - 1:
                if q == 0:
                    pl.semaphore_wait(barrier, len(greet))
                half_copy(q).start()
                if q > 0:
                    half_add(q - 1)
    zh_copy.start()
    half_add(GROUPS - 1)

    zh_copy.wait()
    z_part[...] += z_half[...]
    z_copy(0).start()


    def flip_c(i, carry):
        for u in range(4):
            c_v[4 * i + u] = ct_v[4 * i + u].astype(F32).T.astype(BF16)
        return carry

    lax.fori_loop(0, rows // 4, flip_c, 0)
    c_copy = pltpu.make_async_copy(c_v, c_hbm, c_sem)
    c_copy.start()

    def q_copy(k, h, f):
        fu, fv, fc = FLIPS[f]
        o = ORDERS[2 * h]
        mu, mv = bits[o[2]], bits[o[3]]
        du = 1 - mu if fu else mu
        dv = 1 - mv if fv else mv
        dc = 1 - core if fc else core
        i = (k * 2 + h) * 7 + f
        return pltpu.make_async_remote_copy(
            q_out.at[k, h, dc, du, dv], q_in.at[k, h, core, mu, mv],
            qs_sem.at[i], qr_sem.at[i], device_id=group_peer(2 * h, f), device_id_type=MESH)

    row8 = lax.broadcasted_iota(jnp.int32, (chip_rows, CHUNK), 0)
    low = row8 < experts

    def at_rest(q, u, v):
        o = ORDERS[q]
        idx = list(bits)
        idx[o[2]] = u
        idx[o[3]] = v
        return tuple(idx)

    def at_recv(q, u, v):
        o = ORDERS[q]
        free = sorted(o[2:])
        val = {o[2]: u, o[3]: v}
        return tuple(val[d] for d in free)

    for k in range(nk):
        for q in range(GROUPS):
            o = ORDERS[q]
            rs_copy(k, q, 0).wait()
            for u in range(gsz):
                at = (k, own0 + q * gsz + u) + region(o, 1)
                part[at] = part[at] + r0[k, q * gsz + u]
            rs_copy(k, q, 1).start()
        if k == 0:
            z_copy(0).wait()
            at = region(ORDERS[0], 1)
            z_part[at] = z_part[at] + z0[...]
            z_copy(1).start()
    z_copy(1).wait()
    at = region(ORDERS[0], 2)
    z_part[at] = z_part[at] + z1[...]
    for f in range(3):
        zq_copy(f).start()
    for k in range(nk):
        for q in range(GROUPS):
            rs_copy(k, q, 1).wait()
        for q in range(GROUPS):
            h, g = divmod(q, 2)
            for u in range(2):
                for v in range(2):
                    ev, od = [
                        part[(k, own0 + q * gsz + w) + at_rest(q, u, v)].astype(F32)
                        + r1[(k, q * gsz + w) + at_recv(q, u, v)].astype(F32)
                        for w in range(gsz)
                    ]
                    q_out[k, h, 0, u, v, g] = jnp.where(low, ev, pltpu.roll(od, experts, 0)).astype(BF16)
                    q_out[k, h, 1, u, v, g] = jnp.where(low, pltpu.roll(ev, experts, 0), od).astype(BF16)
        for h in range(2):
            o = ORDERS[2 * h]
            mu, mv = bits[o[2]], bits[o[3]]
            for f in range(7):
                q_copy(k, h, f).start()
            q_in[k, h, core, mu, mv] = q_out[k, h, core, mu, mv]
    for f in range(3):
        zq_copy(f).wait()
    z_own = z_part[bits] + (zq[0] + (zq[1] + zq[2]))
    zrow = lax.broadcasted_iota(jnp.int32, z_own.shape, 0)
    eye = lax.broadcasted_iota(jnp.int32, (rows, z_own.shape[1]), 0) == lax.broadcasted_iota(
        jnp.int32, (rows, z_own.shape[1]), 1)
    z_inv = []
    for e in range(experts):
        zr = jnp.sum(jnp.where(zrow == core * experts + e, z_own, 0.0), axis=0, keepdims=True)
        z_inv.append(1.0 / jnp.sum(jnp.where(eye, zr, 0.0), axis=1, keepdims=True))

    lanes = CHUNK // 128
    for cp in wi_copies:
        cp.wait()
    for k in range(nk):
        for h in range(2):
            for f in range(7):
                q_copy(k, h, f).wait()
        for cs in range(2):
            for q in range(GROUPS):
                p = cs * GROUPS + q
                s = [q_in[k, q // 2, cs, u, v, q % 2].astype(F32) for u in range(2) for v in range(2)]
                s = (s[0] + s[1]) + (s[2] + s[3])
                for t in range(lanes):
                    xs_f[t, p * chip_rows:(p + 1) * chip_rows, :] = s[:, t * 128:(t + 1) * 128]
        for e in range(experts):
            pick = pl.ds(e, rows, stride=experts)
            xe = jnp.concatenate([xs_f[t, pick, :] for t in range(lanes)], axis=1)
            h = _nn((xe * z_inv[e]).astype(BF16), wi_v[e, k * CHUNK:(k + 1) * CHUNK, :])
            hid[e] = h if k == 0 else hid[e] + h
    for cp in wo_copies:
        cp.wait()
    for e in range(experts):
        hid_b[e] = jax.nn.gelu(hid[e], approximate=True).astype(BF16)

    def y_copy(k, h, f):
        _, _, fc = FLIPS[f]
        o = ORDERS[2 * h]
        dc = 1 - core if fc else core
        i = (k * 2 + h) * 7 + f
        return pltpu.make_async_remote_copy(
            yx.at[k, dc * 2 + h], g_in.at[k, h, core, bits[o[2]], bits[o[3]]],
            ys_sem.at[i], yr_sem.at[i], device_id=group_peer(2 * h, f), device_id_type=MESH)

    def g_copy(k, q, s):
        i = (k * GROUPS + q) * 2 + s
        ref = gath.at[(k, pl.ds(own0 + q * gsz, gsz)) + region(ORDERS[q], s + 1)]
        return pltpu.make_async_remote_copy(
            ref, ref, gs_sem.at[i], gr_sem.at[i], device_id=steps[ORDERS[q][s]], device_id_type=MESH)

    def gd_copy(k, q):
        at = (k, pl.ds(own0 + q * gsz, gsz))
        i = k * GROUPS + q
        return pltpu.make_async_remote_copy(
            gath.at[at], g_hbm.at[at], gds_sem.at[i], gdr_sem.at[i], device_id=mate, device_id_type=MESH)

    def go_copy(k, q):
        at = (k, pl.ds(own0 + q * gsz, gsz))
        return pltpu.make_async_copy(gath.at[at], g_hbm.at[at], go_sem.at[k * GROUPS + q])

    for k in range(nk):
        for e in range(experts):
            ye = _nn(hid_b[e], wo_v[e, :, k * CHUNK:(k + 1) * CHUNK])
            for t in range(lanes):
                ys_f[t, pl.ds(e, rows, stride=experts), :] = ye[:, t * 128:(t + 1) * 128]
        for t in range(lanes):
            yx[k, :, :, :, t * 128:(t + 1) * 128] = ys_f[t].reshape(4, 2, chip_rows, 128).astype(BF16)
        for h in range(2):
            o = ORDERS[2 * h]
            for f in range(7):
                y_copy(k, h, f).start()
            g_in[k, h, core, bits[o[2]], bits[o[3]]] = yx[k, core * 2 + h]

    for k in range(nk):
        for h in range(2):
            for f in range(7):
                y_copy(k, h, f).wait()
        for q in range(GROUPS):
            for u in range(2):
                for v in range(2):
                    s0 = g_in[k, q // 2, 0, u, v, q % 2].astype(F32)
                    s1 = g_in[k, q // 2, 1, u, v, q % 2].astype(F32)
                    at = at_rest(q, u, v)
                    gath[(k, own0 + q * gsz) + at] = jnp.where(low, s0, pltpu.roll(s1, experts, 0)).astype(BF16)
                    gath[(k, own0 + q * gsz + 1) + at] = jnp.where(low, pltpu.roll(s0, experts, 0), s1).astype(BF16)
        for q in range(GROUPS):
            g_copy(k, q, 1).start()
    for k in range(nk):
        for q in range(GROUPS):
            g_copy(k, q, 1).wait()
            g_copy(k, q, 0).start()
    for k in range(nk):
        for q in range(GROUPS):
            g_copy(k, q, 0).wait()
            gd_copy(k, q).start()
            go_copy(k, q).start()
    for k in range(nk):
        for q in range(GROUPS):
            gd_copy(k, q).wait()
            go_copy(k, q).wait()
    for q in range(GROUPS):
        half_copy(q).wait_send()
    c_copy.wait()


def _mix_kernel(len_ref, g_hbm, c_hbm, y_hbm, g_v, c_v, y_v, g_sem, c_sem, y_sem):
    rows, tok_count, width = y_v.shape
    nk = g_v.shape[0]

    def c_copy(b):
        return pltpu.make_async_copy(c_hbm.at[b], c_v.at[b], c_sem.at[b])

    def g_copy(b):
        return pltpu.make_async_copy(g_hbm.at[:, b], g_v.at[:, b], g_sem.at[b])

    def y_copy(b):
        return pltpu.make_async_copy(y_v.at[b], y_hbm.at[b], y_sem.at[b])

    for b in range(rows):
        c_copy(b).start()
        g_copy(b).start()
    row_pos = lax.axis_index("seq") * tok_count + lax.broadcasted_iota(jnp.int32, (tok_count, CHUNK), 0)
    for b0 in range(0, rows, 4):
        for b in range(b0, b0 + 4):
            c_copy(b).wait()
            g_copy(b).wait()
        for b in range(b0, b0 + 4):
            for k in range(nk):
                yk = jnp.where(row_pos < len_ref[b], _nn(c_v[b], g_v[k, b]), 0.0)
                y_v[b, :, k * CHUNK:(k + 1) * CHUNK] = yk.astype(BF16)
        for b in range(b0, b0 + 4):
            y_copy(b).start()
    for b in range(rows):
        y_copy(b).wait()


def solution(mesh):
    def shard_body(tok, lens, phi, gain, w_in, w_out):
        rows, tok_count, width = tok.shape
        experts, _, ff = w_in.shape
        nslots = phi.shape[1]
        nk = width // CHUNK
        hrows = rows // 2
        cr = 2 * experts
        cube = (2, 2, 2, 2)
        tile = (cr, CHUNK)
        lanes = CHUNK // 128
        vm = pltpu.VMEM
        dma = pltpu.SemaphoreType.DMA
        anyspace = pl.BlockSpec(memory_space=pl.ANY)
        smem = pl.BlockSpec(memory_space=pltpu.SMEM)
        gshape = (nk, rows) + cube + tile
        scratch = [
            vm((rows, tok_count, width), BF16),
            vm((rows, tok_count, width), BF16),
            vm((rows, nslots, tok_count), BF16),
            vm((width, nslots), BF16),
            vm((nslots, width), BF16),
            vm(w_in.shape, BF16),
            vm(w_out.shape, BF16),
            vm((rows, nslots, tok_count), BF16),
            vm((rows, tok_count, nslots), BF16),
            vm(gshape, BF16),
            vm((nk, hrows) + cube + tile, BF16),
            vm((nk, hrows, 2, 2, 2) + tile, BF16),
            vm((nk, hrows, 2, 2) + tile, BF16),
            vm((nk, 2, 2, 2, 2, 2) + tile, BF16),
            vm((nk, 2, 2, 2, 2, 2) + tile, BF16),
            vm(cube + (cr, tok_count), F32),
            vm(cube + (cr, tok_count), F32),
            vm((2, 2, 2, cr, tok_count), F32),
            vm((2, 2, cr, tok_count), F32),
            vm((3, cr, tok_count), F32),
            vm((lanes, rows * experts, 128), F32),
            vm((experts, rows, ff), F32),
            vm((experts, rows, ff), BF16),
            vm((lanes, rows * experts, 128), F32),
            vm((nk, 4, 2) + tile, BF16),
            vm((nk, 2, 2, 2, 2, 2) + tile, BF16),
            vm(gshape, BF16),
            dma, dma((2 * GROUPS,)), dma((experts,)), dma((experts,)), dma,
            dma((GROUPS,)), dma((GROUPS,)), dma, dma, dma((5,)), dma((5,)),
            dma((nk * GROUPS * 2,)), dma((nk * GROUPS * 2,)),
            dma((nk * 2 * 7,)), dma((nk * 2 * 7,)),
            dma((nk * 2 * 7,)), dma((nk * 2 * 7,)),
            dma((nk * GROUPS * 2,)), dma((nk * GROUPS * 2,)),
            dma((nk * GROUPS,)), dma((nk * GROUPS,)), dma((nk * GROUPS,)),
        ]
        gath, comb = pl.pallas_call(
            _exchange_kernel,
            out_shape=(
                jax.ShapeDtypeStruct(gshape, BF16),
                jax.ShapeDtypeStruct((rows, tok_count, nslots), BF16),
            ),
            in_specs=[smem, smem, anyspace, anyspace, anyspace, anyspace],
            out_specs=(anyspace, anyspace),
            scratch_shapes=scratch,
            compiler_params=pltpu.CompilerParams(
                collective_id=0, has_side_effects=True, vmem_limit_bytes=67043328),
        )(lens, gain, tok, phi, w_in, w_out)
        return pl.pallas_call(
            _mix_kernel,
            out_shape=jax.ShapeDtypeStruct(tok.shape, BF16),
            in_specs=[smem, anyspace, anyspace],
            out_specs=anyspace,
            scratch_shapes=[
                vm((nk, rows, nslots, CHUNK), BF16),
                vm((rows, tok_count, nslots), BF16),
                vm(tok.shape, BF16),
                dma((rows,)), dma((rows,)), dma((rows,)),
            ],
        )(lens, gath.reshape(nk, rows, nslots, CHUNK), comb)

    return jax.shard_map(
        shard_body,
        mesh=mesh,
        in_specs=(P("data", "seq", None), P("data"), P(None, None), P(None), P("seq", None, None), P("seq", None, None)),
        out_specs=P("data", "seq", None),
        check_vma=False,
    )
```

```python
import functools

import jax
import jax.numpy as jnp
from jax import lax
from jax.experimental import pallas as pl
from jax.experimental.pallas import tpu as pltpu
from jax.sharding import PartitionSpec as P

CHUNK = 256
GROUPS = 4
F32 = jnp.float32
BF16 = jnp.bfloat16
MESH = pl.DeviceIdType.MESH
ORDERS = ((3, 1, 2, 0), (1, 3, 2, 0), (2, 0, 3, 1), (0, 2, 3, 1))
FLIPS = tuple((f & 1, (f >> 1) & 1, (f >> 2) & 1) for f in range(1, 8))


def _nt(a, b):
    return lax.dot_general(a, b, (((1,), (1,)), ((), ())), preferred_element_type=F32)


def _nn(a, b):
    return jnp.dot(a, b, preferred_element_type=F32)


def _drain(ref, sem):
    pltpu.make_async_copy(ref, ref, sem).wait()


def _exchange_kernel(len_ref, gain_ref, tok_hbm, phi_hbm, wi_hbm, wo_hbm, g_hbm, c_hbm,
                     x_v, xn_v, w_v, phi_v, phit_v, wi_v, wo_v, ct_v, c_v, part, half_in, r0, r1, q_out, q_in,
                     z_part, z_half, z0, z1, zq, xs_f, hid, hid_b, ys_f, yx, g_in, gath,
                     phi_sem, tok_sem, wi_sem, wo_sem, c_sem,
                     hs_sem, hr_sem, zhs_sem, zhr_sem, zs_sem, zr_sem, rs_sem, rr_sem,
                     qs_sem, qr_sem, ys_sem, yr_sem, gs_sem, gr_sem, gds_sem, gdr_sem, go_sem):
    rows, tok_count, width = x_v.shape
    experts = wi_v.shape[0]
    nk = width // CHUNK
    hrows = rows // 2
    gsz = hrows // GROUPS
    nslots = phit_v.shape[0]
    chip_rows = 2 * experts
    me = lax.axis_index("seq")
    core = lax.rem(me, 2)
    chip = me // 2
    x = lax.rem(chip, 4)
    y = chip // 4
    xb = x // 2
    xa = lax.rem(x + xb, 2)
    yb = y // 2
    ya = lax.rem(y + yb, 2)
    bits = (yb, ya, xb, xa)

    def peer(dims, flip_core=0):
        b = [1 - v if d in dims else v for d, v in enumerate(bits)]
        yy = 2 * b[0] + lax.rem(b[0] + b[1], 2)
        xx = 2 * b[2] + lax.rem(b[2] + b[3], 2)
        return {"seq": (yy * 4 + xx) * 2 + (1 - core if flip_core else core)}

    def group_peer(q, f):
        fu, fv, fc = FLIPS[f]
        dims = tuple(d for d, on in zip(ORDERS[q][2:], (fu, fv)) if on)
        return peer(dims, fc)

    mate = peer((), 1)
    steps = tuple(peer((d,)) for d in range(4))
    own0 = core * hrows
    oth0 = (1 - core) * hrows

    pairs = sorted({dims for q in range(GROUPS) for dims in (tuple(sorted(ORDERS[q][2:])),)})
    greet = []
    for fc in (0, 1):
        greet += [peer((d,), fc) for d in range(4)]
        greet += [peer(dims, fc) for dims in pairs]
    greet.append(mate)
    barrier = pltpu.get_barrier_semaphore()
    for d in greet:
        pl.semaphore_signal(barrier, inc=1, device_id=d, device_id_type=MESH)

    def batch(i):
        return oth0 + i if i < hrows else own0 + i - hrows

    tok_step = rows // 4

    def tok_copy(i):
        at = pl.ds(batch(i), tok_step)
        return pltpu.make_async_copy(tok_hbm.at[at], x_v.at[at], tok_sem.at[i // tok_step])

    phi_copy = pltpu.make_async_copy(phi_hbm, phi_v, phi_sem)
    wi_copies = [pltpu.make_async_copy(wi_hbm.at[e], wi_v.at[e], wi_sem) for e in range(experts)]
    wo_copies = [pltpu.make_async_copy(wo_hbm.at[e], wo_v.at[e], wo_sem) for e in range(experts)]
    phi_copy.start()
    for i in range(0, rows, tok_step):
        tok_copy(i).start()

    z_part[...] = jnp.zeros_like(z_part)
    gain = gain_ref[0]
    shift = gain * (1.0 + 2.0 ** -7)
    lane = lax.broadcasted_iota(jnp.int32, (nslots, tok_count), 1)
    pos = me * tok_count + lane

    def normalise(i):
        xf = x_v[batch(i)].astype(F32)
        xn_v[i] = (xf * lax.rsqrt(jnp.sum(xf * xf, axis=1, keepdims=True) + 1e-6)).astype(BF16)

    def weigh(i):
        b = batch(i)
        ex = jnp.exp(_nt(phit_v[...], xn_v[i]) - shift)
        ct_v[b] = (ex * (1.0 / jnp.sum(ex, axis=0, keepdims=True))).astype(BF16)
        exm = jnp.where(pos < len_ref[b], ex, 0.0)
        w_v[i] = exm.astype(BF16)
        zs = jnp.where(lane == b, jnp.sum(exm, axis=1, keepdims=True), 0.0)
        z_part[...] += zs.reshape(z_part.shape)

    def collect(i):
        b = batch(i)
        for k in range(nk):
            pk = _nn(w_v[i], x_v[b, :, k * CHUNK:(k + 1) * CHUNK])
            part[k, b] = pk.reshape(2, 2, 2, 2, chip_rows, CHUNK).astype(BF16)

    def half_copy(q):
        return pltpu.make_async_remote_copy(
            part.at[:, pl.ds(oth0 + q * gsz, gsz)], half_in.at[:, pl.ds(q * gsz, gsz)],
            hs_sem, hr_sem.at[q], device_id=mate, device_id_type=MESH)

    def region(order, fixed, flip=None):
        idx = [slice(None)] * 4
        for t in range(fixed):
            idx[order[t]] = bits[order[t]]
        if flip is not None:
            idx[flip] = 1 - bits[flip]
        return tuple(idx)

    rbuf = (r0, r1)
    zbuf = (z0, z1)

    def rs_copy(k, q, s):
        order = ORDERS[q]
        return pltpu.make_async_remote_copy(
            part.at[(k, pl.ds(own0 + q * gsz, gsz)) + region(order, s, order[s])],
            rbuf[s].at[k, pl.ds(q * gsz, gsz)],
            rs_sem.at[s], rr_sem.at[2 * k + s], device_id=steps[order[s]], device_id_type=MESH)

    def z_copy(s):
        order = ORDERS[0]
        return pltpu.make_async_remote_copy(
            z_part.at[region(order, s, order[s])], zbuf[s],
            zs_sem.at[s], zr_sem.at[s], device_id=steps[order[s]], device_id_type=MESH)

    def zq_copy(f):
        fu, fv, _ = FLIPS[f]
        order = ORDERS[0]
        idx = list(bits)
        for d, on in zip(order[2:], (fu, fv)):
            if on:
                idx[d] = 1 - idx[d]
        return pltpu.make_async_remote_copy(
            z_part.at[tuple(idx)], zq.at[f], zs_sem.at[2], zr_sem.at[2],
            device_id=group_peer(0, f), device_id_type=MESH)

    zh_copy = pltpu.make_async_remote_copy(
        z_part, z_half, zhs_sem, zhr_sem, device_id=mate, device_id_type=MESH)

    ahead = 4
    tok_copy(0).wait()
    for i in range(ahead):
        normalise(i)
    phi_copy.wait()
    pf = phi_v[...].astype(F32)
    pn = (pf * (gain * lax.rsqrt(jnp.sum(pf * pf, axis=0, keepdims=True) + 1e-6))).astype(BF16)
    new = lax.broadcasted_iota(jnp.int32, (nslots, nslots), 0)
    old = lax.broadcasted_iota(jnp.int32, (nslots, nslots), 1)
    nchip = new // chip_rows
    nxa, nxb, nya, nyb = nchip & 1, (nchip >> 1) & 1, (nchip >> 2) & 1, (nchip >> 3) & 1
    src = ((2 * nyb + (nya ^ nyb)) * 4 + 2 * nxb + (nxa ^ nxb)) * chip_rows + (new & (chip_rows - 1))
    perm = jnp.where(src == old, 1.0, 0.0).astype(BF16)
    phit_v[...] = _nt(perm, pn).astype(BF16)

    for cp in wi_copies + wo_copies:
        cp.start()

    def half_add(q):
        half_copy(q).wait_recv()
        for k in range(nk):
            for u in range(gsz):
                b = own0 + q * gsz + u
                part[k, b] = part[k, b] + half_in[k, q * gsz + u]
            rs_copy(k, q, 0).start()

    for i in range(rows + 1):
        if i + ahead < rows:
            if (i + ahead) % tok_step == 0:
                tok_copy(i + ahead).wait()
            normalise(i + ahead)
        if i < rows:
            weigh(i)
        if i == rows - 1:
            zh_copy.start()
        if i >= 1:
            collect(i - 1)
            q, r = divmod(i - 1, gsz)
            if r == gsz - 1:
                if q == 0:
                    pl.semaphore_wait(barrier, len(greet))
                if q < GROUPS:
                    half_copy(q).start()
                else:
                    half_add(q - GROUPS)

    zh_copy.wait()
    z_part[...] += z_half[...]
    z_copy(0).start()


    def flip_c(i, carry):
        for u in range(4):
            c_v[4 * i + u] = ct_v[4 * i + u].astype(F32).T.astype(BF16)
        return carry

    lax.fori_loop(0, rows // 4, flip_c, 0)
    c_copy = pltpu.make_async_copy(c_v, c_hbm, c_sem)
    c_copy.start()

    def q_copy(k, h, f):
        fu, fv, fc = FLIPS[f]
        o = ORDERS[2 * h]
        mu, mv = bits[o[2]], bits[o[3]]
        du = 1 - mu if fu else mu
        dv = 1 - mv if fv else mv
        dc = 1 - core if fc else core
        return pltpu.make_async_remote_copy(
            q_out.at[k, h, dc, du, dv], q_in.at[k, 4 * core + 2 * mu + mv, h],
            qs_sem, qr_sem.at[k], device_id=group_peer(2 * h, f), device_id_type=MESH)

    row8 = lax.broadcasted_iota(jnp.int32, (chip_rows, CHUNK), 0)
    low = row8 < experts

    def at_rest(q, u, v):
        o = ORDERS[q]
        idx = list(bits)
        idx[o[2]] = u
        idx[o[3]] = v
        return tuple(idx)

    def at_recv(q, u, v):
        o = ORDERS[q]
        free = sorted(o[2:])
        val = {o[2]: u, o[3]: v}
        return tuple(val[d] for d in free)

    for k in range(nk):
        _drain(r0.at[k], rr_sem.at[2 * k])
        for q in range(GROUPS):
            for u in range(gsz):
                at = (k, own0 + q * gsz + u) + region(ORDERS[q], 1)
                part[at] = part[at] + r0[k, q * gsz + u]
            rs_copy(k, q, 1).start()
        if k == 0:
            z_copy(0).wait_recv()
            at = region(ORDERS[0], 1)
            z_part[at] = z_part[at] + z0[...]
            z_copy(1).start()
    z_copy(1).wait_recv()
    at = region(ORDERS[0], 2)
    z_part[at] = z_part[at] + z1[...]
    for f in range(3):
        zq_copy(f).start()
    for k in range(nk):
        _drain(r1.at[k], rr_sem.at[2 * k + 1])
        for q in range(GROUPS):
            h, g = divmod(q, 2)
            for u in range(2):
                for v in range(2):
                    ev, od = [
                        part[(k, own0 + q * gsz + w) + at_rest(q, u, v)].astype(F32)
                        + r1[(k, q * gsz + w) + at_recv(q, u, v)].astype(F32)
                        for w in range(gsz)
                    ]
                    q_out[k, h, 0, u, v, g] = jnp.where(low, ev, pltpu.roll(od, experts, 0)).astype(BF16)
                    q_out[k, h, 1, u, v, g] = jnp.where(low, pltpu.roll(ev, experts, 0), od).astype(BF16)
        for h in range(2):
            o = ORDERS[2 * h]
            mu, mv = bits[o[2]], bits[o[3]]
            for f in range(7):
                q_copy(k, h, f).start()
            q_in[k, 4 * core + 2 * mu + mv, h] = q_out[k, h, core, mu, mv]
    _drain(zq, zr_sem.at[2])
    z_own = z_part[bits] + (zq[0] + (zq[1] + zq[2]))
    zrow = lax.broadcasted_iota(jnp.int32, z_own.shape, 0)
    eye = lax.broadcasted_iota(jnp.int32, (rows, z_own.shape[1]), 0) == lax.broadcasted_iota(
        jnp.int32, (rows, z_own.shape[1]), 1)
    z_inv = []
    for e in range(experts):
        zr = jnp.sum(jnp.where(zrow == core * experts + e, z_own, 0.0), axis=0, keepdims=True)
        z_inv.append(1.0 / jnp.sum(jnp.where(eye, zr, 0.0), axis=1, keepdims=True))

    lanes = CHUNK // 128
    _drain(wi_v, wi_sem)
    for k in range(nk):
        _drain(q_in.at[k, pl.ds(0, 7)], qr_sem.at[k])
        for cs in range(2):
            for q in range(GROUPS):
                p = cs * GROUPS + q
                s = [q_in[k, 4 * cs + j, q // 2, q % 2].astype(F32) for j in range(4)]
                s = (s[0] + s[1]) + (s[2] + s[3])
                for t in range(lanes):
                    xs_f[t, p * chip_rows:(p + 1) * chip_rows, :] = s[:, t * 128:(t + 1) * 128]
        for e in range(experts):
            pick = pl.ds(e, rows, stride=experts)
            xe = jnp.concatenate([xs_f[t, pick, :] for t in range(lanes)], axis=1)
            h = _nn((xe * z_inv[e]).astype(BF16), wi_v[e, k * CHUNK:(k + 1) * CHUNK, :])
            hid[e] = h if k == 0 else hid[e] + h
    _drain(wo_v, wo_sem)
    for e in range(experts):
        hid_b[e] = jax.nn.gelu(hid[e], approximate=True).astype(BF16)

    def y_copy(k, h, f):
        _, _, fc = FLIPS[f]
        o = ORDERS[2 * h]
        dc = 1 - core if fc else core
        return pltpu.make_async_remote_copy(
            yx.at[k, dc * 2 + h], g_in.at[k, 4 * core + 2 * bits[o[2]] + bits[o[3]], h],
            ys_sem, yr_sem.at[k], device_id=group_peer(2 * h, f), device_id_type=MESH)

    def g_copy(k, q, s):
        ref = gath.at[(k, pl.ds(own0 + q * gsz, gsz)) + region(ORDERS[q], s + 1)]
        return pltpu.make_async_remote_copy(
            ref, ref, gs_sem.at[s], gr_sem.at[2 * k + s], device_id=steps[ORDERS[q][s]], device_id_type=MESH)

    def gd_copy(k, q):
        at = (k, pl.ds(own0 + q * gsz, gsz))
        return pltpu.make_async_remote_copy(
            gath.at[at], g_hbm.at[at], gds_sem, gdr_sem, device_id=mate, device_id_type=MESH)

    def go_copy(k, q):
        at = (k, pl.ds(own0 + q * gsz, gsz))
        return pltpu.make_async_copy(gath.at[at], g_hbm.at[at], go_sem)

    for k in range(nk):
        for e in range(experts):
            ye = _nn(hid_b[e], wo_v[e, :, k * CHUNK:(k + 1) * CHUNK])
            for t in range(lanes):
                ys_f[t, pl.ds(e, rows, stride=experts), :] = ye[:, t * 128:(t + 1) * 128]
        for t in range(lanes):
            yx[k, :, :, :, t * 128:(t + 1) * 128] = ys_f[t].reshape(4, 2, chip_rows, 128).astype(BF16)
        for h in range(2):
            o = ORDERS[2 * h]
            for f in range(7):
                y_copy(k, h, f).start()
            g_in[k, 4 * core + 2 * bits[o[2]] + bits[o[3]], h] = yx[k, core * 2 + h]

    for k in range(nk):
        _drain(g_in.at[k, pl.ds(0, 7)], yr_sem.at[k])
        for q in range(GROUPS):
            for u in range(2):
                for v in range(2):
                    s0 = g_in[k, 2 * u + v, q // 2, q % 2].astype(F32)
                    s1 = g_in[k, 4 + 2 * u + v, q // 2, q % 2].astype(F32)
                    at = at_rest(q, u, v)
                    gath[(k, own0 + q * gsz) + at] = jnp.where(low, s0, pltpu.roll(s1, experts, 0)).astype(BF16)
                    gath[(k, own0 + q * gsz + 1) + at] = jnp.where(low, pltpu.roll(s0, experts, 0), s1).astype(BF16)
        for q in range(GROUPS):
            g_copy(k, q, 1).start()
    for k in range(nk):
        _drain(r1.at[k], gr_sem.at[2 * k + 1])
        for q in range(GROUPS):
            g_copy(k, q, 0).start()
    for k in range(nk):
        _drain(r0.at[k], gr_sem.at[2 * k])
        for q in range(GROUPS):
            gd_copy(k, q).start()
            go_copy(k, q).start()
    z_copy(0).wait_send()
    z_copy(1).wait_send()
    _drain(half_in, hs_sem)
    _drain(zq, zs_sem.at[2])
    _drain(r0, rs_sem.at[0])
    _drain(r1, rs_sem.at[1])
    _drain(q_in.at[:, pl.ds(0, 7)], qs_sem)
    _drain(g_in.at[:, pl.ds(0, 7)], ys_sem)
    _drain(r0, gs_sem.at[0])
    _drain(r1, gs_sem.at[1])
    _drain(half_in, gds_sem)
    _drain(half_in, go_sem)
    _drain(half_in, gdr_sem)
    c_copy.wait()


def _mix_kernel(len_ref, g_hbm, c_hbm, y_hbm, g_v, c_v, y_v, g_sem, c_sem, y_sem):
    rows, tok_count, width = y_v.shape
    nk = g_v.shape[0]

    step = rows // 4

    def g_copy(b):
        at = pl.ds(b, step)
        return pltpu.make_async_copy(g_hbm.at[:, at], g_v.at[:, at], g_sem.at[b // step])

    def y_copy(b):
        at = pl.ds(b, step)
        return pltpu.make_async_copy(y_v.at[at], y_hbm.at[at], y_sem)

    c_copy = pltpu.make_async_copy(c_hbm, c_v, c_sem)
    c_copy.start()
    for b in range(0, rows, step):
        g_copy(b).start()
    row_pos = lax.axis_index("seq") * tok_count + lax.broadcasted_iota(jnp.int32, (tok_count, CHUNK), 0)
    c_copy.wait()
    for b0 in range(0, rows, step):
        g_copy(b0).wait()
        for b in range(b0, b0 + step):
            for k in range(nk):
                yk = jnp.where(row_pos < len_ref[b], _nn(c_v[b], g_v[k, b]), 0.0)
                y_v[b, :, k * CHUNK:(k + 1) * CHUNK] = yk.astype(BF16)
        y_copy(b0).start()
    _drain(y_v, y_sem)


def solution(mesh):
    def shard_body(tok, lens, phi, gain, w_in, w_out):
        rows, tok_count, width = tok.shape
        experts, _, ff = w_in.shape
        nslots = phi.shape[1]
        nk = width // CHUNK
        hrows = rows // 2
        cr = 2 * experts
        cube = (2, 2, 2, 2)
        tile = (cr, CHUNK)
        lanes = CHUNK // 128
        vm = pltpu.VMEM
        dma = pltpu.SemaphoreType.DMA
        anyspace = pl.BlockSpec(memory_space=pl.ANY)
        smem = pl.BlockSpec(memory_space=pltpu.SMEM)
        gshape = (nk, rows) + cube + tile
        scratch = [
            vm((rows, tok_count, width), BF16),
            vm((rows, tok_count, width), BF16),
            vm((rows, nslots, tok_count), BF16),
            vm((width, nslots), BF16),
            vm((nslots, width), BF16),
            vm(w_in.shape, BF16),
            vm(w_out.shape, BF16),
            vm((rows, nslots, tok_count), BF16),
            vm((rows, tok_count, nslots), BF16),
            vm(gshape, BF16),
            vm((nk, hrows) + cube + tile, BF16),
            vm((nk, hrows, 2, 2, 2) + tile, BF16),
            vm((nk, hrows, 2, 2) + tile, BF16),
            vm((nk, 2, 2, 2, 2, 2) + tile, BF16),
            vm((nk, 8, 2, 2) + tile, BF16),
            vm(cube + (cr, tok_count), F32),
            vm(cube + (cr, tok_count), F32),
            vm((2, 2, 2, cr, tok_count), F32),
            vm((2, 2, cr, tok_count), F32),
            vm((3, cr, tok_count), F32),
            vm((lanes, rows * experts, 128), F32),
            vm((experts, rows, ff), F32),
            vm((experts, rows, ff), BF16),
            vm((lanes, rows * experts, 128), F32),
            vm((nk, 4, 2) + tile, BF16),
            vm((nk, 8, 2, 2) + tile, BF16),
            vm(gshape, BF16),
            dma, dma((4,)), dma, dma, dma,
            dma, dma((GROUPS,)), dma, dma, dma((3,)), dma((3,)), dma((2,)), dma((2 * nk,)),
            dma, dma((nk,)), dma, dma((nk,)), dma((2,)), dma((2 * nk,)), dma, dma, dma,
        ]
        gath, comb = pl.pallas_call(
            _exchange_kernel,
            out_shape=(
                jax.ShapeDtypeStruct(gshape, BF16),
                jax.ShapeDtypeStruct((rows, tok_count, nslots), BF16),
            ),
            in_specs=[smem, smem, anyspace, anyspace, anyspace, anyspace],
            out_specs=(anyspace, anyspace),
            scratch_shapes=scratch,
            compiler_params=pltpu.CompilerParams(
                collective_id=0, has_side_effects=True, vmem_limit_bytes=67043328),
        )(lens, gain, tok, phi, w_in, w_out)
        return pl.pallas_call(
            _mix_kernel,
            out_shape=jax.ShapeDtypeStruct(tok.shape, BF16),
            in_specs=[smem, anyspace, anyspace],
            out_specs=anyspace,
            scratch_shapes=[
                vm((nk, rows, nslots, CHUNK), BF16),
                vm((rows, tok_count, nslots), BF16),
                vm(tok.shape, BF16),
                dma((4,)), dma, dma,
            ],
        )(lens, gath.reshape(nk, rows, nslots, CHUNK), comb)

    return jax.shard_map(
        shard_body,
        mesh=mesh,
        in_specs=(P("data", "seq", None), P("data"), P(None, None), P(None), P("seq", None, None), P("seq", None, None)),
        out_specs=P("data", "seq", None),
        check_vma=False,
    )
```

```python
import functools

import jax
import jax.numpy as jnp
from jax import lax
from jax.experimental import pallas as pl
from jax.experimental.pallas import tpu as pltpu
from jax.sharding import PartitionSpec as P

WIDE = 256
WIDTHS = (256, 256, 128, 128)
OFFS = tuple(sum(WIDTHS[:k]) for k in range(len(WIDTHS)))
NK = len(WIDTHS)
GROUPS = 4
F32 = jnp.float32
BF16 = jnp.bfloat16
MESH = pl.DeviceIdType.MESH
ORDERS = ((3, 1, 2, 0), (1, 3, 2, 0), (2, 0, 3, 1), (0, 2, 3, 1))
FLIPS = tuple((f & 1, (f >> 1) & 1, (f >> 2) & 1) for f in range(1, 8))


def _nt(a, b):
    return lax.dot_general(a, b, (((1,), (1,)), ((), ())), preferred_element_type=F32)


def _nn(a, b):
    return jnp.dot(a, b, preferred_element_type=F32)


def _drain(ref, sem):
    pltpu.make_async_copy(ref, ref, sem).wait()


def _exchange_kernel(*refs):
    it = iter(refs)

    def take(n=NK):
        return [next(it) for _ in range(n)]

    len_ref, gain_ref, tok_hbm, phi_hbm, wi_hbm, wo_hbm = take(6)
    g_hbm = take()
    c_hbm = next(it)
    x_v, xn_v, w_v, phi_v, phit_v, wi_v, wo_v, ct_v, c_v = take(9)
    part, half_in, r0, r1, q_out, q_in, yx, g_in, gath = [take() for _ in range(9)]
    z_part, z_half, z0, z1, zq, xs_f, hid, hid_b, ys_f = take(9)
    (phi_sem, tok_sem, wi_sem, wo_sem, c_sem, hs_sem, hr_sem, zhs_sem, zhr_sem, zs_sem, zr_sem,
     rs_sem, rr_sem, qs_sem, qr_sem, ys_sem, yr_sem, gs_sem, gr_sem, gds_sem, gdr_sem, go_sem) = take(22)
    rows, tok_count, width = x_v.shape
    experts = wi_v.shape[0]
    hrows = rows // 2
    gsz = hrows // GROUPS
    nslots = phit_v.shape[0]
    chip_rows = 2 * experts
    chunks = tuple(zip(range(NK), OFFS, WIDTHS))
    me = lax.axis_index("seq")
    core = lax.rem(me, 2)
    chip = me // 2
    x = lax.rem(chip, 4)
    y = chip // 4
    xb = x // 2
    xa = lax.rem(x + xb, 2)
    yb = y // 2
    ya = lax.rem(y + yb, 2)
    bits = (yb, ya, xb, xa)

    def peer(dims, flip_core=0):
        b = [1 - v if d in dims else v for d, v in enumerate(bits)]
        yy = 2 * b[0] + lax.rem(b[0] + b[1], 2)
        xx = 2 * b[2] + lax.rem(b[2] + b[3], 2)
        return {"seq": (yy * 4 + xx) * 2 + (1 - core if flip_core else core)}

    def group_peer(q, f):
        fu, fv, fc = FLIPS[f]
        dims = tuple(d for d, on in zip(ORDERS[q][2:], (fu, fv)) if on)
        return peer(dims, fc)

    mate = peer((), 1)
    steps = tuple(peer((d,)) for d in range(4))
    own0 = core * hrows
    oth0 = (1 - core) * hrows

    tok_step = rows // 4

    def batch(i):
        return oth0 + i if i < hrows else own0 + i - hrows

    def tok_copy(i):
        at = pl.ds(batch(i), tok_step)
        return pltpu.make_async_copy(tok_hbm.at[at], x_v.at[at], tok_sem.at[i // tok_step])

    phi_copy = pltpu.make_async_copy(phi_hbm, phi_v, phi_sem)
    wi_copies = [pltpu.make_async_copy(wi_hbm.at[e], wi_v.at[e], wi_sem) for e in range(experts)]
    wo_copies = [pltpu.make_async_copy(wo_hbm.at[e], wo_v.at[e], wo_sem) for e in range(experts)]
    tok_copy(0).start()
    phi_copy.start()
    tok_copy(tok_step).start()

    pairs = sorted({tuple(sorted(o[2:])) for o in ORDERS})
    greet = [mate]
    for fc in (0, 1):
        greet += [peer((d,), fc) for d in range(4)]
        greet += [peer(dims, fc) for dims in pairs]
    barrier = pltpu.get_barrier_semaphore()
    for d in greet:
        pl.semaphore_signal(barrier, inc=1, device_id=d, device_id_type=MESH)

    z_part[...] = jnp.zeros_like(z_part)
    gain = gain_ref[0]
    shift = gain * (1.0 + 2.0 ** -7)
    lane = lax.broadcasted_iota(jnp.int32, (nslots, tok_count), 1)
    pos = me * tok_count + lane

    def normalise(i):
        xf = x_v[batch(i)].astype(F32)
        xn_v[i] = (xf * lax.rsqrt(jnp.sum(xf * xf, axis=1, keepdims=True) + 1e-6)).astype(BF16)

    def weigh(i):
        b = batch(i)
        ex = jnp.exp(_nt(phit_v[...], xn_v[i]) - shift)
        ct_v[b] = (ex * (1.0 / jnp.sum(ex, axis=0, keepdims=True))).astype(BF16)
        exm = jnp.where(pos < len_ref[b], ex, 0.0)
        w_v[i] = exm.astype(BF16)
        zs = jnp.where(lane == b, jnp.sum(exm, axis=1, keepdims=True), 0.0)
        z_part[...] += zs.reshape(z_part.shape)

    def collect(i):
        b = batch(i)
        for base in range(0, width, WIDE):
            pk = _nn(w_v[i], x_v[b, :, base:base + WIDE])
            for k, off, wd in chunks:
                if base <= off < base + WIDE:
                    piece = pk[:, off - base:off - base + wd]
                    part[k][b] = piece.reshape(2, 2, 2, 2, chip_rows, wd).astype(BF16)

    def half_copy(k, h):
        n = hrows // 2
        return pltpu.make_async_remote_copy(
            part[k].at[pl.ds(oth0 + h * n, n)], half_in[k].at[pl.ds(h * n, n)],
            hs_sem, hr_sem.at[k], device_id=mate, device_id_type=MESH)

    def region(order, fixed, flip=None):
        idx = [slice(None)] * 4
        for t in range(fixed):
            idx[order[t]] = bits[order[t]]
        if flip is not None:
            idx[flip] = 1 - bits[flip]
        return tuple(idx)

    rbuf = (r0, r1)
    zbuf = (z0, z1)

    def rs_copy(k, q, s):
        order = ORDERS[q]
        return pltpu.make_async_remote_copy(
            part[k].at[(pl.ds(own0 + q * gsz, gsz),) + region(order, s, order[s])],
            rbuf[s][k].at[pl.ds(q * gsz, gsz)],
            rs_sem.at[s], rr_sem.at[2 * k + s], device_id=steps[order[s]], device_id_type=MESH)

    def z_copy(s):
        order = ORDERS[0]
        return pltpu.make_async_remote_copy(
            z_part.at[region(order, s, order[s])], zbuf[s],
            zs_sem.at[s], zr_sem.at[s], device_id=steps[order[s]], device_id_type=MESH)

    def zq_copy(f):
        fu, fv, _ = FLIPS[f]
        order = ORDERS[0]
        idx = list(bits)
        for d, on in zip(order[2:], (fu, fv)):
            if on:
                idx[d] = 1 - idx[d]
        return pltpu.make_async_remote_copy(
            z_part.at[tuple(idx)], zq.at[f], zs_sem.at[2], zr_sem.at[2],
            device_id=group_peer(0, f), device_id_type=MESH)

    zh_copy = pltpu.make_async_remote_copy(
        z_part, z_half, zhs_sem, zhr_sem, device_id=mate, device_id_type=MESH)

    tok_copy(0).wait()
    tok_copy(2 * tok_step).start()
    tok_copy(3 * tok_step).start()
    for i in range(tok_step):
        normalise(i)
    phi_copy.wait()
    pf = phi_v[...].astype(F32)
    pn = (pf * (gain * lax.rsqrt(jnp.sum(pf * pf, axis=0, keepdims=True) + 1e-6))).astype(BF16)
    new = lax.broadcasted_iota(jnp.int32, (nslots, nslots), 0)
    old = lax.broadcasted_iota(jnp.int32, (nslots, nslots), 1)
    nchip = new // chip_rows
    nxa, nxb, nya, nyb = nchip & 1, (nchip >> 1) & 1, (nchip >> 2) & 1, (nchip >> 3) & 1
    src = ((2 * nyb + (nya ^ nyb)) * 4 + 2 * nxb + (nxa ^ nxb)) * chip_rows + (new & (chip_rows - 1))
    perm = jnp.where(src == old, 1.0, 0.0).astype(BF16)
    phit_v[...] = _nt(perm, pn).astype(BF16)
    for cp in wi_copies + wo_copies:
        cp.start()

    def front(lo, hi, norm):
        norm = iter(norm)
        for i in range(lo, hi + 1):
            if i < hi:
                weigh(i)
            j = next(norm, None)
            if j is not None:
                normalise(j)
            if i > lo:
                collect(i - 1)

    tok_copy(tok_step).wait()
    front(0, tok_step, range(tok_step, 2 * tok_step))
    pl.semaphore_wait(barrier, len(greet))
    for k in range(NK):
        half_copy(k, 0).start()
    tok_copy(2 * tok_step).wait()
    front(tok_step, 2 * tok_step, range(2 * tok_step, 3 * tok_step))
    for k in range(NK):
        half_copy(k, 1).start()
    tok_copy(3 * tok_step).wait()
    front(2 * tok_step, rows, range(3 * tok_step, rows))
    zh_copy.start()

    for k in range(NK):
        _drain(half_in[k], hr_sem.at[k])
        for j in range(hrows):
            part[k][own0 + j] = part[k][own0 + j] + half_in[k][j]
        for q in range(GROUPS):
            rs_copy(k, q, 0).start()

    zh_copy.wait()
    z_part[...] += z_half[...]
    z_copy(0).start()


    def flip_c(i, carry):
        for u in range(4):
            c_v[4 * i + u] = ct_v[4 * i + u].astype(F32).T.astype(BF16)
        return carry

    lax.fori_loop(0, rows // 4, flip_c, 0)
    c_copy = pltpu.make_async_copy(c_v, c_hbm, c_sem)
    c_copy.start()

    def src_at(h):
        o = ORDERS[2 * h]
        return 4 * core + 2 * bits[o[2]] + bits[o[3]]

    def dst_at(h, f):
        fu, fv, fc = FLIPS[f]
        o = ORDERS[2 * h]
        mu, mv = bits[o[2]], bits[o[3]]
        return (1 - core if fc else core), (1 - mu if fu else mu), (1 - mv if fv else mv)

    def q_copy(k, h, f):
        dc, du, dv = dst_at(h, f)
        return pltpu.make_async_remote_copy(
            q_out[k].at[h, 4 * dc + 2 * du + dv], q_in[k].at[src_at(h), h],
            qs_sem, qr_sem.at[k], device_id=group_peer(2 * h, f), device_id_type=MESH)

    def low(wd):
        return lax.broadcasted_iota(jnp.int32, (chip_rows, wd), 0) < experts

    def at_rest(q, u, v):
        o = ORDERS[q]
        idx = list(bits)
        idx[o[2]] = u
        idx[o[3]] = v
        return tuple(idx)

    def at_recv(q, u, v):
        o = ORDERS[q]
        free = sorted(o[2:])
        val = {o[2]: u, o[3]: v}
        return tuple(val[d] for d in free)

    for k in range(NK):
        _drain(r0[k], rr_sem.at[2 * k])
        for q in range(GROUPS):
            for u in range(gsz):
                at = (own0 + q * gsz + u,) + region(ORDERS[q], 1)
                part[k][at] = part[k][at] + r0[k][q * gsz + u]
            rs_copy(k, q, 1).start()
        if k == 0:
            z_copy(0).wait_recv()
            at = region(ORDERS[0], 1)
            z_part[at] = z_part[at] + z0[...]
            z_copy(1).start()

    for k, _, wd in chunks:
        _drain(r1[k], rr_sem.at[2 * k + 1])
        for q in range(GROUPS):
            h, g = divmod(q, 2)
            for u in range(2):
                for v in range(2):
                    ev, od = [
                        part[k][(own0 + q * gsz + w,) + at_rest(q, u, v)].astype(F32)
                        + r1[k][(q * gsz + w,) + at_recv(q, u, v)].astype(F32)
                        for w in range(gsz)
                    ]
                    d = 2 * u + v
                    q_out[k][h, d, g] = jnp.where(low(wd), ev, pltpu.roll(od, experts, 0)).astype(BF16)
                    q_out[k][h, 4 + d, g] = jnp.where(low(wd), pltpu.roll(ev, experts, 0), od).astype(BF16)
        for h in range(2):
            for f in range(7):
                q_copy(k, h, f).start()
            q_in[k][src_at(h), h] = q_out[k][h, src_at(h)]
        if k == 0:
            z_copy(1).wait_recv()
            at = region(ORDERS[0], 2)
            z_part[at] = z_part[at] + z1[...]
            for f in range(3):
                zq_copy(f).start()
    _drain(zq, zr_sem.at[2])
    z_own = z_part[bits] + (zq[0] + (zq[1] + zq[2]))
    zrow = lax.broadcasted_iota(jnp.int32, z_own.shape, 0)
    eye = lax.broadcasted_iota(jnp.int32, (rows, z_own.shape[1]), 0) == lax.broadcasted_iota(
        jnp.int32, (rows, z_own.shape[1]), 1)
    z_inv = []
    for e in range(experts):
        zr = jnp.sum(jnp.where(zrow == core * experts + e, z_own, 0.0), axis=0, keepdims=True)
        z_inv.append(1.0 / jnp.sum(jnp.where(eye, zr, 0.0), axis=1, keepdims=True))

    _drain(wi_v, wi_sem)
    for k, off, wd in chunks:
        _drain(q_in[k].at[pl.ds(0, 7)], qr_sem.at[k])
        for cs in range(2):
            for q in range(GROUPS):
                p = cs * GROUPS + q
                s = [q_in[k][4 * cs + j, q // 2, q % 2].astype(F32) for j in range(4)]
                s = (s[0] + s[1]) + (s[2] + s[3])
                for t in range(wd // 128):
                    xs_f[t, p * chip_rows:(p + 1) * chip_rows, :] = s[:, t * 128:(t + 1) * 128]
        for e in range(experts):
            pick = pl.ds(e, rows, stride=experts)
            xe = [(xs_f[t, pick, :] * z_inv[e]).astype(BF16) for t in range(wd // 128)]
            xe = xe[0] if len(xe) == 1 else jnp.concatenate(xe, axis=1)
            h = _nn(xe, wi_v[e, off:off + wd, :])
            hid[e] = h if k == 0 else hid[e] + h
    _drain(wo_v, wo_sem)
    for e in range(experts):
        hid_b[e] = jax.nn.gelu(hid[e], approximate=True).astype(BF16)

    def y_copy(k, h, f):
        dc = dst_at(h, f)[0]
        return pltpu.make_async_remote_copy(
            yx[k].at[dc * 2 + h], g_in[k].at[src_at(h), h],
            ys_sem, yr_sem.at[k], device_id=group_peer(2 * h, f), device_id_type=MESH)

    def g_copy(k, q, s):
        ref = gath[k].at[(pl.ds(own0 + q * gsz, gsz),) + region(ORDERS[q], s + 1)]
        return pltpu.make_async_remote_copy(
            ref, ref, gs_sem.at[s], gr_sem.at[2 * k + s], device_id=steps[ORDERS[q][s]], device_id_type=MESH)

    def gd_copy(k):
        at = pl.ds(own0, hrows)
        return pltpu.make_async_remote_copy(
            gath[k].at[at], g_hbm[k].at[at], gds_sem, gdr_sem, device_id=mate, device_id_type=MESH)

    def go_copy(k):
        at = pl.ds(own0, hrows)
        return pltpu.make_async_copy(gath[k].at[at], g_hbm[k].at[at], go_sem)

    for base in range(0, width, WIDE):
        for e in range(experts):
            ye = _nn(hid_b[e], wo_v[e, :, base:base + WIDE])
            for t in range(WIDE // 128):
                ys_f[t, pl.ds(e, rows, stride=experts), :] = ye[:, t * 128:(t + 1) * 128]
        for k, off, wd in chunks:
            if not base <= off < base + WIDE:
                continue
            for t in range(wd // 128):
                rows8 = ys_f[t + (off - base) // 128].reshape(4, 2, chip_rows, 128)
                yx[k][:, :, :, t * 128:(t + 1) * 128] = rows8.astype(BF16)
            for h in range(2):
                for f in range(7):
                    y_copy(k, h, f).start()
                g_in[k][src_at(h), h] = yx[k][core * 2 + h]

    for k, _, wd in chunks:
        _drain(g_in[k].at[pl.ds(0, 7)], yr_sem.at[k])
        for q in range(GROUPS):
            for u in range(2):
                for v in range(2):
                    s0 = g_in[k][2 * u + v, q // 2, q % 2].astype(F32)
                    s1 = g_in[k][4 + 2 * u + v, q // 2, q % 2].astype(F32)
                    at = at_rest(q, u, v)
                    b = own0 + q * gsz
                    gath[k][(b,) + at] = jnp.where(low(wd), s0, pltpu.roll(s1, experts, 0)).astype(BF16)
                    gath[k][(b + 1,) + at] = jnp.where(low(wd), pltpu.roll(s0, experts, 0), s1).astype(BF16)
        for q in range(GROUPS):
            g_copy(k, q, 1).start()
    for k in range(NK):
        _drain(r1[k], gr_sem.at[2 * k + 1])
        for q in range(GROUPS):
            g_copy(k, q, 0).start()
    for k in range(NK):
        _drain(r0[k], gr_sem.at[2 * k])
        gd_copy(k).start()
        go_copy(k).start()
    c_copy.wait()
    zh_bytes = x_v.at[pl.ds(0, hrows)]
    r0_bytes = x_v.at[pl.ds(0, hrows // 2)]
    r1_bytes = x_v.at[pl.ds(0, hrows // 4)]
    q_bytes = x_v.at[pl.ds(0, 7), pl.ds(0, 32)]
    z_copy(0).wait_send()
    z_copy(1).wait_send()
    _drain(zq, zs_sem.at[2])
    _drain(zh_bytes, hs_sem)
    _drain(r0_bytes, rs_sem.at[0])
    _drain(r1_bytes, rs_sem.at[1])
    _drain(q_bytes, qs_sem)
    _drain(q_bytes, ys_sem)
    _drain(r0_bytes, gs_sem.at[0])
    _drain(r1_bytes, gs_sem.at[1])
    _drain(zh_bytes, gds_sem)
    _drain(zh_bytes, go_sem)
    _drain(zh_bytes, gdr_sem)


def _mix_kernel(*refs):
    len_ref = refs[0]
    g_hbm = refs[1:1 + NK]
    c_hbm, y_hbm, g_v, c_v, y_v, g_sem, c_sem, y_sem = refs[1 + NK:]
    rows, tok_count, width = y_v.shape
    step = rows // 4

    def c_copy(b):
        at = pl.ds(b, step)
        return pltpu.make_async_copy(c_hbm.at[at], c_v.at[at], c_sem.at[b // step])

    def g_copies(b):
        at = pl.ds(b, step)
        return [
            pltpu.make_async_copy(
                g_hbm[k].at[at], g_v.at[at, :, pl.ds(OFFS[k], WIDTHS[k])], g_sem.at[b // step])
            for k in range(NK)
        ]

    def y_copy(b):
        at = pl.ds(b, step)
        return pltpu.make_async_copy(y_v.at[at], y_hbm.at[at], y_sem)

    for b in range(0, rows, step):
        c_copy(b).start()
        for cp in g_copies(b):
            cp.start()
    row_pos = lax.axis_index("seq") * tok_count + lax.broadcasted_iota(jnp.int32, (tok_count, WIDE), 0)
    for b0 in range(0, rows, step):
        c_copy(b0).wait()
        _drain(g_v.at[pl.ds(b0, step)], g_sem.at[b0 // step])
        for b in range(b0, b0 + step):
            for off in range(0, width, WIDE):
                yk = jnp.where(row_pos < len_ref[b], _nn(c_v[b], g_v[b, :, off:off + WIDE]), 0.0)
                y_v[b, :, off:off + WIDE] = yk.astype(BF16)
        y_copy(b0).start()
    _drain(y_v, y_sem)


def solution(mesh):
    def shard_body(tok, lens, phi, gain, w_in, w_out):
        rows, tok_count, width = tok.shape
        experts, _, ff = w_in.shape
        nslots = phi.shape[1]
        hrows = rows // 2
        cr = 2 * experts
        cube = (2, 2, 2, 2)
        lanes = WIDE // 128
        vm = pltpu.VMEM
        dma = pltpu.SemaphoreType.DMA
        anyspace = pl.BlockSpec(memory_space=pl.ANY)
        smem = pl.BlockSpec(memory_space=pltpu.SMEM)

        def per_chunk(*lead):
            return [vm(lead + (cr, wd), BF16) for wd in WIDTHS]

        scratch = [
            vm((rows, tok_count, width), BF16),
            vm((rows, tok_count, width), BF16),
            vm((rows, nslots, tok_count), BF16),
            vm((width, nslots), BF16),
            vm((nslots, width), BF16),
            vm(w_in.shape, BF16),
            vm(w_out.shape, BF16),
            vm((rows, nslots, tok_count), BF16),
            vm((rows, tok_count, nslots), BF16),
            *per_chunk(rows, *cube),
            *per_chunk(hrows, *cube),
            *per_chunk(hrows, 2, 2, 2),
            *per_chunk(hrows, 2, 2),
            *per_chunk(2, 8, 2),
            *per_chunk(8, 2, 2),
            *per_chunk(4, 2),
            *per_chunk(8, 2, 2),
            *per_chunk(rows, *cube),
            vm(cube + (cr, tok_count), F32),
            vm(cube + (cr, tok_count), F32),
            vm((2, 2, 2, cr, tok_count), F32),
            vm((2, 2, cr, tok_count), F32),
            vm((3, cr, tok_count), F32),
            vm((lanes, rows * experts, 128), F32),
            vm((experts, rows, ff), F32),
            vm((experts, rows, ff), BF16),
            vm((lanes, rows * experts, 128), F32),
            dma, dma((4,)), dma, dma, dma, dma, dma((NK,)), dma, dma, dma((3,)), dma((3,)),
            dma((2,)), dma((2 * NK,)), dma, dma((NK,)), dma, dma((NK,)), dma((2,)), dma((2 * NK,)), dma, dma, dma,
        ]
        gshapes = [jax.ShapeDtypeStruct((rows,) + cube + (cr, wd), BF16) for wd in WIDTHS]
        *gath, comb = pl.pallas_call(
            _exchange_kernel,
            out_shape=(*gshapes, jax.ShapeDtypeStruct((rows, tok_count, nslots), BF16)),
            in_specs=[smem, smem, anyspace, anyspace, anyspace, anyspace],
            out_specs=(anyspace,) * (NK + 1),
            scratch_shapes=scratch,
            compiler_params=pltpu.CompilerParams(
                collective_id=0, has_side_effects=True, vmem_limit_bytes=67043328),
        )(lens, gain, tok, phi, w_in, w_out)
        return pl.pallas_call(
            _mix_kernel,
            out_shape=jax.ShapeDtypeStruct(tok.shape, BF16),
            in_specs=[smem] + [anyspace] * (NK + 1),
            out_specs=anyspace,
            scratch_shapes=[
                vm((rows, nslots, width), BF16),
                vm((rows, tok_count, nslots), BF16),
                vm(tok.shape, BF16),
                dma((4,)), dma((4,)), dma,
            ],
        )(lens, *[g.reshape(rows, nslots, wd) for g, wd in zip(gath, WIDTHS)], comb)

    return jax.shard_map(
        shard_body,
        mesh=mesh,
        in_specs=(P("data", "seq", None), P("data"), P(None, None), P(None), P("seq", None, None), P("seq", None, None)),
        out_specs=P("data", "seq", None),
        check_vma=False,
    )
```

```python
import functools

import jax
import jax.numpy as jnp
from jax import lax
from jax.experimental import pallas as pl
from jax.experimental.pallas import tpu as pltpu
from jax.sharding import PartitionSpec as P

WIDE = 256
WIDTHS = (256, 256, 128, 128)
OFFS = tuple(sum(WIDTHS[:k]) for k in range(len(WIDTHS)))
NK = len(WIDTHS)
GROUPS = 4
F32 = jnp.float32
BF16 = jnp.bfloat16
MESH = pl.DeviceIdType.MESH
ORDERS = ((3, 1, 2, 0), (1, 3, 2, 0), (2, 0, 3, 1), (0, 2, 3, 1))
FLIPS = tuple((f & 1, (f >> 1) & 1, (f >> 2) & 1) for f in range(1, 8))


def _nt(a, b):
    return lax.dot_general(a, b, (((1,), (1,)), ((), ())), preferred_element_type=F32)


def _nn(a, b):
    return jnp.dot(a, b, preferred_element_type=F32)


def _drain(ref, sem):
    pltpu.make_async_copy(ref, ref, sem).wait()


def _exchange_kernel(*refs):
    it = iter(refs)

    def take(n=NK):
        return [next(it) for _ in range(n)]

    len_ref, gain_ref, tok_hbm, phi_hbm, wi_hbm, wo_hbm = take(6)
    g_hbm = take()
    c_hbm = next(it)
    x_v, xn_v, w_v, phi_v, phit_v, wi_v, wo_v, ct_v, c_v = take(9)
    part, half_in, r0, r1, q_out, q_in, yx, g_in, gath = [take() for _ in range(9)]
    z_part, z_half, z0, z1, zq, xs_f, hid, hid_b, ys_f = take(9)
    (phi_sem, tok_sem, wi_sem, wo_sem, c_sem, hs_sem, hr_sem, zhs_sem, zhr_sem, zs_sem, zr_sem,
     rs_sem, rr_sem, qs_sem, qr_sem, ys_sem, yr_sem, gs_sem, gr_sem, gds_sem, gdr_sem, go_sem) = take(22)
    rows, tok_count, width = x_v.shape
    experts = wi_v.shape[0]
    hrows = rows // 2
    gsz = hrows // GROUPS
    nslots = phit_v.shape[0]
    chip_rows = 2 * experts
    chunks = tuple(zip(range(NK), OFFS, WIDTHS))
    me = lax.axis_index("seq")
    core = lax.rem(me, 2)
    chip = me // 2
    x = lax.rem(chip, 4)
    y = chip // 4
    xb = x // 2
    xa = lax.rem(x + xb, 2)
    yb = y // 2
    ya = lax.rem(y + yb, 2)
    bits = (yb, ya, xb, xa)

    def peer(dims, flip_core=0):
        b = [1 - v if d in dims else v for d, v in enumerate(bits)]
        yy = 2 * b[0] + lax.rem(b[0] + b[1], 2)
        xx = 2 * b[2] + lax.rem(b[2] + b[3], 2)
        return {"seq": (yy * 4 + xx) * 2 + (1 - core if flip_core else core)}

    def group_peer(q, f):
        fu, fv, fc = FLIPS[f]
        dims = tuple(d for d, on in zip(ORDERS[q][2:], (fu, fv)) if on)
        return peer(dims, fc)

    mate = peer((), 1)
    steps = tuple(peer((d,)) for d in range(4))
    own0 = core * hrows
    oth0 = (1 - core) * hrows

    tok_step = rows // 4

    def batch(i):
        return oth0 + i if i < hrows else own0 + i - hrows

    def tok_copy(i):
        at = pl.ds(batch(i), tok_step)
        return pltpu.make_async_copy(tok_hbm.at[at], x_v.at[at], tok_sem.at[i // tok_step])

    phi_copy = pltpu.make_async_copy(phi_hbm, phi_v, phi_sem)
    wi_copies = [pltpu.make_async_copy(wi_hbm.at[e], wi_v.at[e], wi_sem) for e in range(experts)]
    wo_copies = [pltpu.make_async_copy(wo_hbm.at[e], wo_v.at[e], wo_sem) for e in range(experts)]
    tok_copy(0).start()
    phi_copy.start()
    tok_copy(tok_step).start()

    pairs = sorted({tuple(sorted(o[2:])) for o in ORDERS})
    greet = [mate]
    for fc in (0, 1):
        greet += [peer((d,), fc) for d in range(4)]
        greet += [peer(dims, fc) for dims in pairs]
    barrier = pltpu.get_barrier_semaphore()
    for d in greet:
        pl.semaphore_signal(barrier, inc=1, device_id=d, device_id_type=MESH)

    z_part[...] = jnp.zeros_like(z_part)
    gain = gain_ref[0]
    shift = gain * (1.0 + 2.0 ** -7)
    lane = lax.broadcasted_iota(jnp.int32, (nslots, tok_count), 1)
    pos = me * tok_count + lane

    def normalise(i):
        xf = x_v[batch(i)].astype(F32)
        xn_v[i] = (xf * lax.rsqrt(jnp.sum(xf * xf, axis=1, keepdims=True) + 1e-6)).astype(BF16)

    def weigh(i):
        b = batch(i)
        ex = jnp.exp(_nt(phit_v[...], xn_v[i]) - shift)
        ct_v[b] = (ex * (1.0 / jnp.sum(ex, axis=0, keepdims=True))).astype(BF16)
        exm = jnp.where(pos < len_ref[b], ex, 0.0)
        w_v[i] = exm.astype(BF16)
        zs = jnp.where(lane == b, jnp.sum(exm, axis=1, keepdims=True), 0.0)
        z_part[...] += zs.reshape(z_part.shape)

    def collect(i):
        b = batch(i)
        for base in range(0, width, WIDE):
            pk = _nn(w_v[i], x_v[b, :, base:base + WIDE])
            for k, off, wd in chunks:
                if base <= off < base + WIDE:
                    piece = pk[:, off - base:off - base + wd]
                    part[k][b] = piece.reshape(2, 2, 2, 2, chip_rows, wd).astype(BF16)

    def half_copy(k, h):
        n = hrows // 2
        return pltpu.make_async_remote_copy(
            part[k].at[pl.ds(oth0 + h * n, n)], half_in[k].at[pl.ds(h * n, n)],
            hs_sem, hr_sem.at[k], device_id=mate, device_id_type=MESH)

    def region(order, fixed, flip=None):
        idx = [slice(None)] * 4
        for t in range(fixed):
            idx[order[t]] = bits[order[t]]
        if flip is not None:
            idx[flip] = 1 - bits[flip]
        return tuple(idx)

    rbuf = (r0, r1)
    zbuf = (z0, z1)

    def rs_copy(k, q, s):
        order = ORDERS[q]
        return pltpu.make_async_remote_copy(
            part[k].at[(pl.ds(own0 + q * gsz, gsz),) + region(order, s, order[s])],
            rbuf[s][k].at[pl.ds(q * gsz, gsz)],
            rs_sem.at[k if s == 0 else NK], rr_sem.at[2 * k + s], device_id=steps[order[s]], device_id_type=MESH)

    def z_copy(s):
        order = ORDERS[0]
        return pltpu.make_async_remote_copy(
            z_part.at[region(order, s, order[s])], zbuf[s],
            zs_sem.at[s], zr_sem.at[s], device_id=steps[order[s]], device_id_type=MESH)

    def zq_copy(f):
        fu, fv, _ = FLIPS[f]
        order = ORDERS[0]
        idx = list(bits)
        for d, on in zip(order[2:], (fu, fv)):
            if on:
                idx[d] = 1 - idx[d]
        return pltpu.make_async_remote_copy(
            z_part.at[tuple(idx)], zq.at[f], zs_sem.at[2], zr_sem.at[2],
            device_id=group_peer(0, f), device_id_type=MESH)

    zh_copy = pltpu.make_async_remote_copy(
        z_part, z_half, zhs_sem, zhr_sem, device_id=mate, device_id_type=MESH)

    tok_copy(0).wait()
    tok_copy(2 * tok_step).start()
    tok_copy(3 * tok_step).start()
    for i in range(tok_step):
        normalise(i)
    phi_copy.wait()
    pf = phi_v[...].astype(F32)
    pn = (pf * (gain * lax.rsqrt(jnp.sum(pf * pf, axis=0, keepdims=True) + 1e-6))).astype(BF16)
    new = lax.broadcasted_iota(jnp.int32, (nslots, nslots), 0)
    old = lax.broadcasted_iota(jnp.int32, (nslots, nslots), 1)
    nchip = new // chip_rows
    nxa, nxb, nya, nyb = nchip & 1, (nchip >> 1) & 1, (nchip >> 2) & 1, (nchip >> 3) & 1
    src = ((2 * nyb + (nya ^ nyb)) * 4 + 2 * nxb + (nxa ^ nxb)) * chip_rows + (new & (chip_rows - 1))
    perm = jnp.where(src == old, 1.0, 0.0).astype(BF16)
    phit_v[...] = _nt(perm, pn).astype(BF16)
    for cp in wi_copies + wo_copies:
        cp.start()

    def front(lo, hi, norm):
        norm = iter(norm)
        for i in range(lo, hi + 1):
            if i < hi:
                weigh(i)
            j = next(norm, None)
            if j is not None:
                normalise(j)
            if i > lo:
                collect(i - 1)

    tok_copy(tok_step).wait()
    front(0, tok_step, range(tok_step, 2 * tok_step))
    pl.semaphore_wait(barrier, len(greet))
    for k in range(NK):
        half_copy(k, 0).start()
    tok_copy(2 * tok_step).wait()
    front(tok_step, 2 * tok_step, range(2 * tok_step, 3 * tok_step))
    for k in range(NK):
        half_copy(k, 1).start()
    tok_copy(3 * tok_step).wait()
    front(2 * tok_step, rows, range(3 * tok_step, rows))
    zh_copy.start()

    def halve(k):
        _drain(half_in[k], hr_sem.at[k])
        for j in range(hrows):
            part[k][own0 + j] = part[k][own0 + j] + half_in[k][j]
        for q in range(GROUPS):
            rs_copy(k, q, 0).start()

    def flip_c(i, carry):
        for u in range(4):
            c_v[4 * i + u] = ct_v[4 * i + u].astype(F32).T.astype(BF16)
        return carry

    halve(0)
    lax.fori_loop(0, rows // 4, flip_c, 0)
    c_copy = pltpu.make_async_copy(c_v, c_hbm, c_sem)
    c_copy.start()
    halve(1)
    zh_copy.wait()
    z_part[...] += z_half[...]
    z_copy(0).start()
    _drain(r0[0], rs_sem.at[0])
    for k in range(2, NK):
        halve(k)

    def src_at(h):
        o = ORDERS[2 * h]
        return 4 * core + 2 * bits[o[2]] + bits[o[3]]

    def dst_at(h, f):
        fu, fv, fc = FLIPS[f]
        o = ORDERS[2 * h]
        mu, mv = bits[o[2]], bits[o[3]]
        return (1 - core if fc else core), (1 - mu if fu else mu), (1 - mv if fv else mv)

    def q_copy(k, h, f):
        dc, du, dv = dst_at(h, f)
        return pltpu.make_async_remote_copy(
            q_out[k].at[h, 4 * dc + 2 * du + dv], q_in[k].at[src_at(h), h],
            qs_sem, qr_sem.at[k], device_id=group_peer(2 * h, f), device_id_type=MESH)

    def low(wd):
        return lax.broadcasted_iota(jnp.int32, (chip_rows, wd), 0) < experts

    def at_rest(q, u, v):
        o = ORDERS[q]
        idx = list(bits)
        idx[o[2]] = u
        idx[o[3]] = v
        return tuple(idx)

    def at_recv(q, u, v):
        o = ORDERS[q]
        free = sorted(o[2:])
        val = {o[2]: u, o[3]: v}
        return tuple(val[d] for d in free)

    for k in range(NK):
        _drain(r0[k], rr_sem.at[2 * k])
        for q in range(GROUPS):
            for u in range(gsz):
                at = (own0 + q * gsz + u,) + region(ORDERS[q], 1)
                part[k][at] = part[k][at] + r0[k][q * gsz + u]
            rs_copy(k, q, 1).start()
        if k == 0:
            z_copy(0).wait_recv()
            at = region(ORDERS[0], 1)
            z_part[at] = z_part[at] + z0[...]
            z_copy(1).start()

    for k, _, wd in chunks:
        _drain(r1[k], rr_sem.at[2 * k + 1])
        for q in range(GROUPS):
            h, g = divmod(q, 2)
            for u in range(2):
                for v in range(2):
                    ev, od = [
                        part[k][(own0 + q * gsz + w,) + at_rest(q, u, v)].astype(F32)
                        + r1[k][(q * gsz + w,) + at_recv(q, u, v)].astype(F32)
                        for w in range(gsz)
                    ]
                    d = 2 * u + v
                    q_out[k][h, d, g] = jnp.where(low(wd), ev, pltpu.roll(od, experts, 0)).astype(BF16)
                    q_out[k][h, 4 + d, g] = jnp.where(low(wd), pltpu.roll(ev, experts, 0), od).astype(BF16)
        for h in range(2):
            for f in range(7):
                q_copy(k, h, f).start()
            q_in[k][src_at(h), h] = q_out[k][h, src_at(h)]
        if k == 0:
            z_copy(1).wait_recv()
            at = region(ORDERS[0], 2)
            z_part[at] = z_part[at] + z1[...]
            for f in range(3):
                zq_copy(f).start()
    _drain(zq, zr_sem.at[2])
    z_own = z_part[bits] + (zq[0] + (zq[1] + zq[2]))
    zrow = lax.broadcasted_iota(jnp.int32, z_own.shape, 0)
    eye = lax.broadcasted_iota(jnp.int32, (rows, z_own.shape[1]), 0) == lax.broadcasted_iota(
        jnp.int32, (rows, z_own.shape[1]), 1)
    z_inv = []
    for e in range(experts):
        zr = jnp.sum(jnp.where(zrow == core * experts + e, z_own, 0.0), axis=0, keepdims=True)
        z_inv.append(1.0 / jnp.sum(jnp.where(eye, zr, 0.0), axis=1, keepdims=True))

    _drain(wi_v, wi_sem)
    _drain(wo_v, wo_sem)
    for k, off, wd in chunks:
        _drain(q_in[k].at[pl.ds(0, 7)], qr_sem.at[k])
        for cs in range(2):
            for q in range(GROUPS):
                p = cs * GROUPS + q
                s = [q_in[k][4 * cs + j, q // 2, q % 2].astype(F32) for j in range(4)]
                s = (s[0] + s[1]) + (s[2] + s[3])
                for t in range(wd // 128):
                    xs_f[t, p * chip_rows:(p + 1) * chip_rows, :] = s[:, t * 128:(t + 1) * 128]
        for e in range(experts):
            pick = pl.ds(e, rows, stride=experts)
            xe = [(xs_f[t, pick, :] * z_inv[e]).astype(BF16) for t in range(wd // 128)]
            xe = xe[0] if len(xe) == 1 else jnp.concatenate(xe, axis=1)
            h = _nn(xe, wi_v[e, off:off + wd, :])
            hid[e] = h if k == 0 else hid[e] + h
    for e in range(experts):
        hid_b[e] = jax.nn.gelu(hid[e], approximate=True).astype(BF16)

    def y_copy(k, h, f):
        dc = dst_at(h, f)[0]
        return pltpu.make_async_remote_copy(
            yx[k].at[dc * 2 + h], g_in[k].at[src_at(h), h],
            ys_sem, yr_sem.at[k], device_id=group_peer(2 * h, f), device_id_type=MESH)

    def g_copy(k, q, s):
        ref = gath[k].at[(pl.ds(own0 + q * gsz, gsz),) + region(ORDERS[q], s + 1)]
        return pltpu.make_async_remote_copy(
            ref, ref, gs_sem.at[s], gr_sem.at[2 * k + s], device_id=steps[ORDERS[q][s]], device_id_type=MESH)

    def gd_copy(k):
        at = pl.ds(own0, hrows)
        return pltpu.make_async_remote_copy(
            gath[k].at[at], g_hbm[k].at[at], gds_sem, gdr_sem, device_id=mate, device_id_type=MESH)

    def go_copy(k):
        at = pl.ds(own0, hrows)
        return pltpu.make_async_copy(gath[k].at[at], g_hbm[k].at[at], go_sem)

    for base in range(0, width, WIDE):
        for e in range(experts):
            ye = _nn(hid_b[e], wo_v[e, :, base:base + WIDE])
            for t in range(WIDE // 128):
                ys_f[t, pl.ds(e, rows, stride=experts), :] = ye[:, t * 128:(t + 1) * 128]
        for k, off, wd in chunks:
            if not base <= off < base + WIDE:
                continue
            for t in range(wd // 128):
                rows8 = ys_f[t + (off - base) // 128].reshape(4, 2, chip_rows, 128)
                yx[k][:, :, :, t * 128:(t + 1) * 128] = rows8.astype(BF16)
            for h in range(2):
                for f in range(7):
                    y_copy(k, h, f).start()
                g_in[k][src_at(h), h] = yx[k][core * 2 + h]

    for k, _, wd in chunks:
        _drain(g_in[k].at[pl.ds(0, 7)], yr_sem.at[k])
        for q in range(GROUPS):
            for u in range(2):
                for v in range(2):
                    s0 = g_in[k][2 * u + v, q // 2, q % 2].astype(F32)
                    s1 = g_in[k][4 + 2 * u + v, q // 2, q % 2].astype(F32)
                    at = at_rest(q, u, v)
                    b = own0 + q * gsz
                    gath[k][(b,) + at] = jnp.where(low(wd), s0, pltpu.roll(s1, experts, 0)).astype(BF16)
                    gath[k][(b + 1,) + at] = jnp.where(low(wd), pltpu.roll(s0, experts, 0), s1).astype(BF16)
        for q in range(GROUPS):
            g_copy(k, q, 1).start()
    for k in range(NK):
        _drain(r1[k], gr_sem.at[2 * k + 1])
        for q in range(GROUPS):
            g_copy(k, q, 0).start()
    for k in range(NK):
        _drain(r0[k], gr_sem.at[2 * k])
        gd_copy(k).start()
        go_copy(k).start()
    c_copy.wait()
    zh_bytes = x_v.at[pl.ds(0, hrows)]
    r0_bytes = x_v.at[pl.ds(0, hrows // 2)]
    r1_bytes = x_v.at[pl.ds(0, hrows // 4)]
    q_bytes = x_v.at[pl.ds(0, 7), pl.ds(0, 32)]
    z_copy(0).wait_send()
    z_copy(1).wait_send()
    _drain(zq, zs_sem.at[2])
    _drain(zh_bytes, hs_sem)
    for k in range(1, NK):
        _drain(r0[k], rs_sem.at[k])
    _drain(r1_bytes, rs_sem.at[NK])
    _drain(q_bytes, qs_sem)
    _drain(q_bytes, ys_sem)
    _drain(r0_bytes, gs_sem.at[0])
    _drain(r1_bytes, gs_sem.at[1])
    _drain(zh_bytes, gds_sem)
    _drain(zh_bytes, go_sem)
    _drain(zh_bytes, gdr_sem)


def _mix_kernel(*refs):
    len_ref = refs[0]
    g_hbm = refs[1:1 + NK]
    c_hbm, y_hbm, g_v, c_v, y_v, g_sem, c_sem, y_sem = refs[1 + NK:]
    rows, tok_count, width = y_v.shape
    step = rows // 4

    def c_copy(b):
        at = pl.ds(b, step)
        return pltpu.make_async_copy(c_hbm.at[at], c_v.at[at], c_sem.at[b // step])

    def g_copies(b):
        at = pl.ds(b, step)
        return [
            pltpu.make_async_copy(
                g_hbm[k].at[at], g_v.at[at, :, pl.ds(OFFS[k], WIDTHS[k])], g_sem.at[b // step])
            for k in range(NK)
        ]

    def y_copy(b):
        at = pl.ds(b, step)
        return pltpu.make_async_copy(y_v.at[at], y_hbm.at[at], y_sem)

    for b in range(0, rows, step):
        c_copy(b).start()
        for cp in g_copies(b):
            cp.start()
    row_pos = lax.axis_index("seq") * tok_count + lax.broadcasted_iota(jnp.int32, (tok_count, WIDE), 0)
    for b0 in range(0, rows, step):
        c_copy(b0).wait()
        _drain(g_v.at[pl.ds(b0, step)], g_sem.at[b0 // step])
        for b in range(b0, b0 + step):
            for off in range(0, width, WIDE):
                yk = jnp.where(row_pos < len_ref[b], _nn(c_v[b], g_v[b, :, off:off + WIDE]), 0.0)
                y_v[b, :, off:off + WIDE] = yk.astype(BF16)
        y_copy(b0).start()
    _drain(y_v, y_sem)


def solution(mesh):
    def shard_body(tok, lens, phi, gain, w_in, w_out):
        rows, tok_count, width = tok.shape
        experts, _, ff = w_in.shape
        nslots = phi.shape[1]
        hrows = rows // 2
        cr = 2 * experts
        cube = (2, 2, 2, 2)
        lanes = WIDE // 128
        vm = pltpu.VMEM
        dma = pltpu.SemaphoreType.DMA
        anyspace = pl.BlockSpec(memory_space=pl.ANY)
        smem = pl.BlockSpec(memory_space=pltpu.SMEM)

        def per_chunk(*lead):
            return [vm(lead + (cr, wd), BF16) for wd in WIDTHS]

        scratch = [
            vm((rows, tok_count, width), BF16),
            vm((rows, tok_count, width), BF16),
            vm((rows, nslots, tok_count), BF16),
            vm((width, nslots), BF16),
            vm((nslots, width), BF16),
            vm(w_in.shape, BF16),
            vm(w_out.shape, BF16),
            vm((rows, nslots, tok_count), BF16),
            vm((rows, tok_count, nslots), BF16),
            *per_chunk(rows, *cube),
            *per_chunk(hrows, *cube),
            *per_chunk(hrows, 2, 2, 2),
            *per_chunk(hrows, 2, 2),
            *per_chunk(2, 8, 2),
            *per_chunk(8, 2, 2),
            *per_chunk(4, 2),
            *per_chunk(8, 2, 2),
            *per_chunk(rows, *cube),
            vm(cube + (cr, tok_count), F32),
            vm(cube + (cr, tok_count), F32),
            vm((2, 2, 2, cr, tok_count), F32),
            vm((2, 2, cr, tok_count), F32),
            vm((3, cr, tok_count), F32),
            vm((lanes, rows * experts, 128), F32),
            vm((experts, rows, ff), F32),
            vm((experts, rows, ff), BF16),
            vm((lanes, rows * experts, 128), F32),
            dma, dma((4,)), dma, dma, dma, dma, dma((NK,)), dma, dma, dma((3,)), dma((3,)),
            dma((NK + 1,)), dma((2 * NK,)), dma, dma((NK,)), dma, dma((NK,)), dma((2,)), dma((2 * NK,)), dma, dma, dma,
        ]
        gshapes = [jax.ShapeDtypeStruct((rows,) + cube + (cr, wd), BF16) for wd in WIDTHS]
        *gath, comb = pl.pallas_call(
            _exchange_kernel,
            out_shape=(*gshapes, jax.ShapeDtypeStruct((rows, tok_count, nslots), BF16)),
            in_specs=[smem, smem, anyspace, anyspace, anyspace, anyspace],
            out_specs=(anyspace,) * (NK + 1),
            scratch_shapes=scratch,
            compiler_params=pltpu.CompilerParams(
                collective_id=0, has_side_effects=True, vmem_limit_bytes=67043328),
        )(lens, gain, tok, phi, w_in, w_out)
        return pl.pallas_call(
            _mix_kernel,
            out_shape=jax.ShapeDtypeStruct(tok.shape, BF16),
            in_specs=[smem] + [anyspace] * (NK + 1),
            out_specs=anyspace,
            scratch_shapes=[
                vm((rows, nslots, width), BF16),
                vm((rows, tok_count, nslots), BF16),
                vm(tok.shape, BF16),
                dma((4,)), dma((4,)), dma,
            ],
        )(lens, *[g.reshape(rows, nslots, wd) for g, wd in zip(gath, WIDTHS)], comb)

    return jax.shard_map(
        shard_body,
        mesh=mesh,
        in_specs=(P("data", "seq", None), P("data"), P(None, None), P(None), P("seq", None, None), P("seq", None, None)),
        out_specs=P("data", "seq", None),
        check_vma=False,
    )
```

```python
import functools

import jax
import jax.numpy as jnp
from jax import lax
from jax.experimental import pallas as pl
from jax.experimental.pallas import tpu as pltpu
from jax.sharding import PartitionSpec as P

WIDE = 256
WIDTHS = (256, 256, 128, 128)
OFFS = tuple(sum(WIDTHS[:k]) for k in range(len(WIDTHS)))
NK = len(WIDTHS)
GROUPS = 4
F32 = jnp.float32
BF16 = jnp.bfloat16
MESH = pl.DeviceIdType.MESH
ORDERS = ((3, 1, 2, 0), (1, 3, 2, 0), (2, 0, 3, 1), (0, 2, 3, 1))
FLIPS = tuple((f & 1, (f >> 1) & 1, (f >> 2) & 1) for f in range(1, 8))


def _nt(a, b):
    return lax.dot_general(a, b, (((1,), (1,)), ((), ())), preferred_element_type=F32)


def _nn(a, b):
    return jnp.dot(a, b, preferred_element_type=F32)


def _drain(ref, sem):
    pltpu.make_async_copy(ref, ref, sem).wait()


def _exchange_kernel(*refs):
    it = iter(refs)

    def take(n=NK):
        return [next(it) for _ in range(n)]

    len_ref, gain_ref, tok_hbm, phi_hbm, wi_hbm, wo_hbm = take(6)
    g_hbm = take()
    c_hbm = next(it)
    x_v, xn_v, w_v, phi_v, phit_v, wi_v, wo_v, ct_v, c_v = take(9)
    part, half_in, r0, r1, q_out, q_in, yx, g_in, gath = [take() for _ in range(9)]
    z_part, z_half, z0, z1, zq, xs_f, hid, hid_b, ys_f = take(9)
    (phi_sem, tok_sem, wi_sem, wo_sem, c_sem, hs_sem, hr_sem, zhs_sem, zhr_sem, zs_sem, zr_sem,
     rs_sem, rr_sem, qs_sem, qr_sem, ys_sem, yr_sem, gs_sem, gr_sem, gds_sem, gdr_sem, go_sem, fl_sem, fs_sem, fr_sem) = take(25)
    rows, tok_count, width = x_v.shape
    experts = wi_v.shape[0]
    hrows = rows // 2
    gsz = hrows // GROUPS
    nslots = phit_v.shape[1]
    chip_rows = 2 * experts
    chunks = tuple(zip(range(NK), OFFS, WIDTHS))
    me = lax.axis_index("seq")
    core = lax.rem(me, 2)
    chip = me // 2
    x = lax.rem(chip, 4)
    y = chip // 4
    xb = x // 2
    xa = lax.rem(x + xb, 2)
    yb = y // 2
    ya = lax.rem(y + yb, 2)
    bits = (yb, ya, xb, xa)

    def peer(dims, flip_core=0):
        b = [1 - v if d in dims else v for d, v in enumerate(bits)]
        yy = 2 * b[0] + lax.rem(b[0] + b[1], 2)
        xx = 2 * b[2] + lax.rem(b[2] + b[3], 2)
        return {"seq": (yy * 4 + xx) * 2 + (1 - core if flip_core else core)}

    def group_peer(q, f):
        fu, fv, fc = FLIPS[f]
        dims = tuple(d for d, on in zip(ORDERS[q][2:], (fu, fv)) if on)
        return peer(dims, fc)

    mate = peer((), 1)
    steps = tuple(peer((d,)) for d in range(4))
    own0 = core * hrows
    oth0 = (1 - core) * hrows

    tok_step = rows // 4

    def batch(i):
        return oth0 + i if i < hrows else own0 + i - hrows

    def tok_copy(i):
        at = pl.ds(batch(i), tok_step)
        return pltpu.make_async_copy(tok_hbm.at[at], x_v.at[at], tok_sem.at[i // tok_step])

    phi_copy = pltpu.make_async_copy(phi_hbm, phi_v, phi_sem)
    wi_copies = [pltpu.make_async_copy(wi_hbm.at[e], wi_v.at[e], wi_sem) for e in range(experts)]
    wo_copies = [pltpu.make_async_copy(wo_hbm.at[e], wo_v.at[e], wo_sem) for e in range(experts)]
    tok_copy(0).start()
    phi_copy.start()
    tok_copy(tok_step).start()

    pairs = sorted({tuple(sorted(o[2:])) for o in ORDERS})
    greet = [mate]
    for fc in (0, 1):
        greet += [peer((d,), fc) for d in range(4)]
        greet += [peer(dims, fc) for dims in pairs]
    barrier = pltpu.get_barrier_semaphore()
    for d in greet:
        pl.semaphore_signal(barrier, inc=1, device_id=d, device_id_type=MESH)

    z_part[...] = jnp.zeros_like(z_part)
    gain = gain_ref[0]
    shift = gain * (1.0 + 2.0 ** -7)
    lane = lax.broadcasted_iota(jnp.int32, (nslots, tok_count), 1)
    pos = me * tok_count + lane

    def normalise(i):
        xf = x_v[batch(i)].astype(F32)
        xn_v[i] = (xf * lax.rsqrt(jnp.sum(xf * xf, axis=1, keepdims=True) + 1e-6)).astype(BF16)

    def weigh(i):
        b = batch(i)
        ex = jnp.exp(_nt(phit_v[i % 2], xn_v[i]) - shift)
        ct_v[b] = (ex * (1.0 / jnp.sum(ex, axis=0, keepdims=True))).astype(BF16)
        exm = jnp.where(pos < len_ref[b], ex, 0.0)
        w_v[i] = exm.astype(BF16)
        zs = jnp.where(lane == b, jnp.sum(exm, axis=1, keepdims=True), 0.0)
        z_part[...] += zs.reshape(z_part.shape)

    def collect(i):
        b = batch(i)
        for base in range(0, width, WIDE):
            pk = _nn(w_v[i], x_v[b, :, base:base + WIDE])
            for k, off, wd in chunks:
                if base <= off < base + WIDE:
                    piece = pk[:, off - base:off - base + wd]
                    part[k][b] = piece.reshape(2, 2, 2, 2, chip_rows, wd).astype(BF16)

    def half_copy(k, h):
        n = hrows // 2
        return pltpu.make_async_remote_copy(
            part[k].at[pl.ds(oth0 + h * n, n)], half_in[k].at[pl.ds(h * n, n)],
            hs_sem, hr_sem.at[k], device_id=mate, device_id_type=MESH)

    def region(order, fixed, flip=None):
        idx = [slice(None)] * 4
        for t in range(fixed):
            idx[order[t]] = bits[order[t]]
        if flip is not None:
            idx[flip] = 1 - bits[flip]
        return tuple(idx)

    rbuf = (r0, r1)
    zbuf = (z0, z1)

    def rs_copy(k, q, s):
        order = ORDERS[q]
        return pltpu.make_async_remote_copy(
            part[k].at[(pl.ds(own0 + q * gsz, gsz),) + region(order, s, order[s])],
            rbuf[s][k].at[pl.ds(q * gsz, gsz)],
            rs_sem.at[k if s == 0 else NK], rr_sem.at[2 * k + s], device_id=steps[order[s]], device_id_type=MESH)

    def z_copy(s):
        order = ORDERS[0]
        return pltpu.make_async_remote_copy(
            z_part.at[region(order, s, order[s])], zbuf[s],
            zs_sem.at[s], zr_sem.at[s], device_id=steps[order[s]], device_id_type=MESH)

    def zq_copy(f):
        fu, fv, _ = FLIPS[f]
        order = ORDERS[0]
        idx = list(bits)
        for d, on in zip(order[2:], (fu, fv)):
            if on:
                idx[d] = 1 - idx[d]
        return pltpu.make_async_remote_copy(
            z_part.at[tuple(idx)], zq.at[f], zs_sem.at[2], zr_sem.at[2],
            device_id=group_peer(0, f), device_id_type=MESH)

    zh_copy = pltpu.make_async_remote_copy(
        z_part, z_half, zhs_sem, zhr_sem, device_id=mate, device_id_type=MESH)

    tok_copy(0).wait()
    tok_copy(2 * tok_step).start()
    tok_copy(3 * tok_step).start()
    for i in range(tok_step):
        normalise(i)
    phi_copy.wait()
    pf = phi_v[...].astype(F32)
    pn = (pf * (gain * lax.rsqrt(jnp.sum(pf * pf, axis=0, keepdims=True) + 1e-6))).astype(BF16)
    new = lax.broadcasted_iota(jnp.int32, (nslots, nslots), 0)
    old = lax.broadcasted_iota(jnp.int32, (nslots, nslots), 1)
    nchip = new // chip_rows
    nxa, nxb, nya, nyb = nchip & 1, (nchip >> 1) & 1, (nchip >> 2) & 1, (nchip >> 3) & 1
    src = ((2 * nyb + (nya ^ nyb)) * 4 + 2 * nxb + (nxa ^ nxb)) * chip_rows + (new & (chip_rows - 1))
    for odd in range(2):
        perm = jnp.where((src ^ (odd * experts)) == old, 1.0, 0.0).astype(BF16)
        phit_v[odd] = _nt(perm, pn).astype(BF16)
    for cp in wi_copies + wo_copies:
        cp.start()

    def front(lo, hi, norm):
        norm = iter(norm)
        for i in range(lo, hi + 1):
            if i < hi:
                weigh(i)
            j = next(norm, None)
            if j is not None:
                normalise(j)
            if i > lo:
                collect(i - 1)

    tok_copy(tok_step).wait()
    front(0, tok_step, range(tok_step, 2 * tok_step))
    pl.semaphore_wait(barrier, len(greet))
    for k in range(NK):
        half_copy(k, 0).start()
    tok_copy(2 * tok_step).wait()
    front(tok_step, 2 * tok_step, range(2 * tok_step, 3 * tok_step))
    for k in range(NK):
        half_copy(k, 1).start()
    tok_copy(3 * tok_step).wait()
    front(2 * tok_step, rows, range(3 * tok_step, rows))
    zh_copy.start()

    def halve(k):
        _drain(half_in[k], hr_sem.at[k])
        for j in range(hrows):
            part[k][own0 + j] = part[k][own0 + j] + half_in[k][j]
        for q in range(GROUPS):
            rs_copy(k, q, 0).start()

    def flip_c(i, carry):
        for u in range(4):
            c_v[4 * i + u] = ct_v[4 * i + u].astype(F32).T.astype(BF16)
        return carry

    halve(0)
    lax.fori_loop(0, rows // 4, flip_c, 0)
    c_copy = pltpu.make_async_copy(c_v, c_hbm, c_sem)
    c_copy.start()
    halve(1)
    zh_copy.wait()
    z_part[...] += z_half[...]
    z_copy(0).start()
    _drain(r0[0], rs_sem.at[0])
    for k in range(2, NK):
        halve(k)

    def src_at(h):
        o = ORDERS[2 * h]
        return 4 * core + 2 * bits[o[2]] + bits[o[3]]

    def dst_at(h, f):
        fu, fv, fc = FLIPS[f]
        o = ORDERS[2 * h]
        mu, mv = bits[o[2]], bits[o[3]]
        return (1 - core if fc else core), (1 - mu if fu else mu), (1 - mv if fv else mv)

    def q_copy(k, h, f):
        dc, du, dv = dst_at(h, f)
        return pltpu.make_async_remote_copy(
            q_out[k].at[h, 4 * dc + 2 * du + dv], q_in[k].at[src_at(h), h],
            qs_sem, qr_sem.at[k], device_id=group_peer(2 * h, f), device_id_type=MESH)

    def low(wd):
        return lax.broadcasted_iota(jnp.int32, (chip_rows, wd), 0) < experts

    def at_rest(q, u, v):
        o = ORDERS[q]
        idx = list(bits)
        idx[o[2]] = u
        idx[o[3]] = v
        return tuple(idx)

    def at_recv(q, u, v):
        o = ORDERS[q]
        free = sorted(o[2:])
        val = {o[2]: u, o[3]: v}
        return tuple(val[d] for d in free)

    for k in range(NK):
        _drain(r0[k], rr_sem.at[2 * k])
        for q in range(GROUPS):
            for u in range(gsz):
                at = (own0 + q * gsz + u,) + region(ORDERS[q], 1)
                part[k][at] = part[k][at] + r0[k][q * gsz + u]
            rs_copy(k, q, 1).start()
        if k == 0:
            z_copy(0).wait_recv()
            at = region(ORDERS[0], 1)
            z_part[at] = z_part[at] + z0[...]
            z_copy(1).start()

    for k, _, wd in chunks:
        _drain(r1[k], rr_sem.at[2 * k + 1])
        for q in range(GROUPS):
            h, g = divmod(q, 2)
            for u in range(2):
                for v in range(2):
                    ev, od = [
                        part[k][(own0 + q * gsz + w,) + at_rest(q, u, v)].astype(F32)
                        + r1[k][(q * gsz + w,) + at_recv(q, u, v)].astype(F32)
                        for w in range(gsz)
                    ]
                    d = 2 * u + v
                    q_out[k][h, d, g] = jnp.where(low(wd), ev, od).astype(BF16)
                    q_out[k][h, 4 + d, g] = jnp.where(low(wd), od, ev).astype(BF16)
        for h in range(2):
            for f in range(7):
                q_copy(k, h, f).start()
            q_in[k][src_at(h), h] = q_out[k][h, src_at(h)]
        if k == 0:
            z_copy(1).wait_recv()
            at = region(ORDERS[0], 2)
            z_part[at] = z_part[at] + z1[...]
            for f in range(3):
                zq_copy(f).start()
    _drain(zq, zr_sem.at[2])
    z_own = z_part[bits] + (zq[0] + (zq[1] + zq[2]))
    zrow = lax.broadcasted_iota(jnp.int32, z_own.shape, 0)
    zcol = lax.broadcasted_iota(jnp.int32, z_own.shape, 1)
    zbase = (core ^ (zcol & 1)) * experts
    erow = lax.broadcasted_iota(jnp.int32, (rows, z_own.shape[1]), 0)
    eye = (erow ^ core) == lax.broadcasted_iota(jnp.int32, (rows, z_own.shape[1]), 1)
    z_inv = []
    for e in range(experts):
        zr = jnp.sum(jnp.where(zrow == zbase + e, z_own, 0.0), axis=0, keepdims=True)
        z_inv.append(1.0 / jnp.sum(jnp.where(eye, zr, 0.0), axis=1, keepdims=True))

    _drain(wi_v, wi_sem)
    _drain(wo_v, wo_sem)
    for k, off, wd in chunks:
        _drain(q_in[k].at[pl.ds(0, 7)], qr_sem.at[k])
        for cs in range(2):
            for q in range(GROUPS):
                p = cs * GROUPS + q
                s = [q_in[k][4 * cs + j, q // 2, q % 2].astype(F32) for j in range(4)]
                s = (s[0] + s[1]) + (s[2] + s[3])
                for t in range(wd // 128):
                    xs_f[t, p * chip_rows:(p + 1) * chip_rows, :] = s[:, t * 128:(t + 1) * 128]
        for e in range(experts):
            pick = pl.ds(e, rows, stride=experts)
            xe = [(xs_f[t, pick, :] * z_inv[e]).astype(BF16) for t in range(wd // 128)]
            xe = xe[0] if len(xe) == 1 else jnp.concatenate(xe, axis=1)
            h = _nn(xe, wi_v[e, off:off + wd, :])
            hid[e] = h if k == 0 else hid[e] + h
    for e in range(experts):
        hid_b[e] = jax.nn.gelu(hid[e], approximate=True).astype(BF16)

    def y_copy(k, h, f):
        dc = dst_at(h, f)[0]
        return pltpu.make_async_remote_copy(
            yx[k].at[dc * 2 + h], g_in[k].at[src_at(h), h],
            ys_sem, yr_sem.at[k], device_id=group_peer(2 * h, f), device_id_type=MESH)

    def g_copy(k, q, s):
        ref = gath[k].at[(pl.ds(own0 + q * gsz, gsz),) + region(ORDERS[q], s + 1)]
        return pltpu.make_async_remote_copy(
            ref, ref, gs_sem.at[s], gr_sem.at[2 * k + s], device_id=steps[ORDERS[q][s]], device_id_type=MESH)

    def gd_copy(k):
        at = pl.ds(own0, hrows)
        return pltpu.make_async_remote_copy(
            gath[k].at[at], g_hbm[k].at[at], gds_sem, gdr_sem, device_id=mate, device_id_type=MESH)

    def last_copies(q):
        dim = ORDERS[q][0]
        at = (pl.ds(own0 + q * gsz, gsz),) + region(ORDERS[q], 1)
        src, dst = gath[NK - 1].at[at], g_hbm[NK - 1].at[at]
        return [pltpu.make_async_copy(src, dst, fl_sem)] + [
            pltpu.make_async_remote_copy(
                src, dst, fs_sem.at[t], fr_sem.at[t], device_id=d, device_id_type=MESH)
            for t, d in enumerate((peer((dim,), 1), steps[dim], mate))
        ]

    def go_copy(k):
        at = pl.ds(own0, hrows)
        return pltpu.make_async_copy(gath[k].at[at], g_hbm[k].at[at], go_sem)

    for base in range(0, width, WIDE):
        for e in range(experts):
            ye = _nn(hid_b[e], wo_v[e, :, base:base + WIDE])
            for t in range(WIDE // 128):
                ys_f[t, pl.ds(e, rows, stride=experts), :] = ye[:, t * 128:(t + 1) * 128]
        for k, off, wd in chunks:
            if not base <= off < base + WIDE:
                continue
            for t in range(wd // 128):
                rows8 = ys_f[t + (off - base) // 128].reshape(4, 2, chip_rows, 128)
                yx[k][:, :, :, t * 128:(t + 1) * 128] = rows8.astype(BF16)
            for h in range(2):
                for f in range(7):
                    y_copy(k, h, f).start()
                g_in[k][src_at(h), h] = yx[k][core * 2 + h]

    for k, _, wd in chunks:
        _drain(g_in[k].at[pl.ds(0, 7)], yr_sem.at[k])
        for q in range(GROUPS):
            for u in range(2):
                for v in range(2):
                    s0 = g_in[k][2 * u + v, q // 2, q % 2].astype(F32)
                    s1 = g_in[k][4 + 2 * u + v, q // 2, q % 2].astype(F32)
                    at = at_rest(q, u, v)
                    b = own0 + q * gsz
                    gath[k][(b,) + at] = jnp.where(low(wd), s0, s1).astype(BF16)
                    gath[k][(b + 1,) + at] = jnp.where(low(wd), s1, s0).astype(BF16)
        for q in range(GROUPS):
            g_copy(k, q, 1).start()
    for k in range(NK):
        _drain(r1[k], gr_sem.at[2 * k + 1])

        @pl.when(core == 1)
        def _():
            pl.delay((300, 350, 550, 600)[k])

        for q in range(GROUPS):
            if k < NK - 1:
                g_copy(k, q, 0).start()
            else:
                for cp in last_copies(q):
                    cp.start()
    for k in range(NK - 1):
        _drain(r0[k], gr_sem.at[2 * k])
        gd_copy(k).start()
        go_copy(k).start()
    c_copy.wait()
    zh_bytes = x_v.at[pl.ds(0, hrows)]
    r0_bytes = x_v.at[pl.ds(0, hrows // 2)]
    r1_bytes = x_v.at[pl.ds(0, hrows // 4)]
    q_bytes = x_v.at[pl.ds(0, 7), pl.ds(0, 32)]
    z_copy(0).wait_send()
    z_copy(1).wait_send()
    _drain(zq, zs_sem.at[2])
    _drain(zh_bytes, hs_sem)
    for k in range(1, NK):
        _drain(r0[k], rs_sem.at[k])
    _drain(r1_bytes, rs_sem.at[NK])
    _drain(q_bytes, qs_sem)
    _drain(q_bytes, ys_sem)
    most = pl.ds(0, width - WIDTHS[-1])
    g_bytes = x_v.at[pl.ds(0, hrows), :, most]
    _drain(x_v.at[pl.ds(0, hrows // 2), :, most], gs_sem.at[0])
    _drain(r1_bytes, gs_sem.at[1])
    _drain(g_bytes, gds_sem)
    _drain(g_bytes, go_sem)
    _drain(g_bytes, gdr_sem)
    _drain(r0[NK - 1], fl_sem)
    for t in range(3):
        _drain(r0[NK - 1], fs_sem.at[t])
        _drain(r0[NK - 1], fr_sem.at[t])


def _mix_kernel(*refs):
    len_ref = refs[0]
    g_hbm = refs[1:1 + NK]
    c_hbm, y_hbm, g_v, c_v, y_v, g_sem, c_sem, y_sem = refs[1 + NK:]
    rows, tok_count, width = y_v.shape
    step = rows // 4

    def c_copy(b):
        at = pl.ds(b, step)
        return pltpu.make_async_copy(c_hbm.at[at], c_v.at[at], c_sem.at[b // step])

    def g_copies(b):
        at = pl.ds(b, step)
        return [
            pltpu.make_async_copy(
                g_hbm[k].at[at], g_v.at[at, :, pl.ds(OFFS[k], WIDTHS[k])], g_sem.at[b // step])
            for k in range(NK)
        ]

    def y_copy(b):
        at = pl.ds(b, step)
        return pltpu.make_async_copy(y_v.at[at], y_hbm.at[at], y_sem)

    for b in range(0, rows, step):
        if b:
            pl.delay(250)
        c_copy(b).start()
        for cp in g_copies(b):
            cp.start()
    row_pos = lax.axis_index("seq") * tok_count + lax.broadcasted_iota(jnp.int32, (tok_count, WIDE), 0)
    for b0 in range(0, rows, step):
        c_copy(b0).wait()
        _drain(g_v.at[pl.ds(b0, step)], g_sem.at[b0 // step])
        for b in range(b0, b0 + step):
            for off in range(0, width, WIDE):
                yk = jnp.where(row_pos < len_ref[b], _nn(c_v[b], g_v[b, :, off:off + WIDE]), 0.0)
                y_v[b, :, off:off + WIDE] = yk.astype(BF16)
        y_copy(b0).start()
    _drain(y_v, y_sem)


def solution(mesh):
    def shard_body(tok, lens, phi, gain, w_in, w_out):
        rows, tok_count, width = tok.shape
        experts, _, ff = w_in.shape
        nslots = phi.shape[1]
        hrows = rows // 2
        cr = 2 * experts
        cube = (2, 2, 2, 2)
        lanes = WIDE // 128
        vm = pltpu.VMEM
        dma = pltpu.SemaphoreType.DMA
        anyspace = pl.BlockSpec(memory_space=pl.ANY)
        smem = pl.BlockSpec(memory_space=pltpu.SMEM)

        def per_chunk(*lead):
            return [vm(lead + (cr, wd), BF16) for wd in WIDTHS]

        scratch = [
            vm((rows, tok_count, width), BF16),
            vm((rows, tok_count, width), BF16),
            vm((rows, nslots, tok_count), BF16),
            vm((width, nslots), BF16),
            vm((2, nslots, width), BF16),
            vm(w_in.shape, BF16),
            vm(w_out.shape, BF16),
            vm((rows, nslots, tok_count), BF16),
            vm((rows, tok_count, nslots), BF16),
            *per_chunk(rows, *cube),
            *per_chunk(hrows, *cube),
            *per_chunk(hrows, 2, 2, 2),
            *per_chunk(hrows, 2, 2),
            *per_chunk(2, 8, 2),
            *per_chunk(8, 2, 2),
            *per_chunk(4, 2),
            *per_chunk(8, 2, 2),
            *per_chunk(rows, *cube),
            vm(cube + (cr, tok_count), F32),
            vm(cube + (cr, tok_count), F32),
            vm((2, 2, 2, cr, tok_count), F32),
            vm((2, 2, cr, tok_count), F32),
            vm((3, cr, tok_count), F32),
            vm((lanes, rows * experts, 128), F32),
            vm((experts, rows, ff), F32),
            vm((experts, rows, ff), BF16),
            vm((lanes, rows * experts, 128), F32),
            dma, dma((4,)), dma, dma, dma, dma, dma((NK,)), dma, dma, dma((3,)), dma((3,)),
            dma((NK + 1,)), dma((2 * NK,)), dma, dma((NK,)), dma, dma((NK,)), dma((2,)), dma((2 * NK,)), dma, dma, dma,
            dma, dma((3,)), dma((3,)),
        ]
        gshapes = [jax.ShapeDtypeStruct((rows,) + cube + (cr, wd), BF16) for wd in WIDTHS]
        *gath, comb = pl.pallas_call(
            _exchange_kernel,
            out_shape=(*gshapes, jax.ShapeDtypeStruct((rows, tok_count, nslots), BF16)),
            in_specs=[smem, smem, anyspace, anyspace, anyspace, anyspace],
            out_specs=(anyspace,) * (NK + 1),
            scratch_shapes=scratch,
            compiler_params=pltpu.CompilerParams(
                collective_id=0, has_side_effects=True, vmem_limit_bytes=67043328),
        )(lens, gain, tok, phi, w_in, w_out)
        return pl.pallas_call(
            _mix_kernel,
            out_shape=jax.ShapeDtypeStruct(tok.shape, BF16),
            in_specs=[smem] + [anyspace] * (NK + 1),
            out_specs=anyspace,
            scratch_shapes=[
                vm((rows, nslots, width), BF16),
                vm((rows, tok_count, nslots), BF16),
                vm(tok.shape, BF16),
                dma((4,)), dma((4,)), dma,
            ],
        )(lens, *[g.reshape(rows, nslots, wd) for g, wd in zip(gath, WIDTHS)], comb)

    return jax.shard_map(
        shard_body,
        mesh=mesh,
        in_specs=(P("data", "seq", None), P("data"), P(None, None), P(None), P("seq", None, None), P("seq", None, None)),
        out_specs=P("data", "seq", None),
        check_vma=False,
    )
```

```python
import functools

import jax
import jax.numpy as jnp
from jax import lax
from jax.experimental import pallas as pl
from jax.experimental.pallas import tpu as pltpu
from jax.sharding import PartitionSpec as P

WIDE = 256
WIDTHS = (256, 256, 128, 128)
OFFS = tuple(sum(WIDTHS[:k]) for k in range(len(WIDTHS)))
NK = len(WIDTHS)
GROUPS = 4
F32 = jnp.float32
BF16 = jnp.bfloat16
MESH = pl.DeviceIdType.MESH
ORDERS = ((3, 1, 2, 0), (1, 3, 2, 0), (2, 0, 3, 1), (0, 2, 3, 1))
FLIPS = tuple((f & 1, (f >> 1) & 1, (f >> 2) & 1) for f in range(1, 8))


def _nt(a, b):
    return lax.dot_general(a, b, (((1,), (1,)), ((), ())), preferred_element_type=F32)


def _nn(a, b):
    return jnp.dot(a, b, preferred_element_type=F32)


def _drain(ref, sem):
    pltpu.make_async_copy(ref, ref, sem).wait()


def _exchange_kernel(*refs):
    it = iter(refs)

    def take(n=NK):
        return [next(it) for _ in range(n)]

    len_ref, gain_ref, tok_hbm, phi_hbm, wi_hbm, wo_hbm = take(6)
    g_hbm = take()
    c_hbm = next(it)
    x_v, xn_v, w_v, phi_v, phit_v, wi_v, wo_v, ct_v, c_v = take(9)
    part, half_in, r0, r1, q_out, q_in, yx, g_in, gath = [take() for _ in range(9)]
    z_part, z_half, z0, z1, zq, xs_f, hid, hid_b, ys_f = take(9)
    (phi_sem, tok_sem, wi_sem, wo_sem, c_sem, hs_sem, hr_sem, zhs_sem, zhr_sem, zs_sem, zr_sem,
     rs_sem, rr_sem, qs_sem, qr_sem, ys_sem, yr_sem, gs_sem, gr_sem, gds_sem, gdr_sem, go_sem, fl_sem, fs_sem, fr_sem) = take(25)
    rows, tok_count, width = x_v.shape
    experts = wi_v.shape[0]
    hrows = rows // 2
    gsz = hrows // GROUPS
    nslots = phit_v.shape[1]
    chip_rows = 2 * experts
    chunks = tuple(zip(range(NK), OFFS, WIDTHS))
    me = lax.axis_index("seq")
    core = lax.rem(me, 2)
    chip = me // 2
    x = lax.rem(chip, 4)
    y = chip // 4
    xb = x // 2
    xa = lax.rem(x + xb, 2)
    yb = y // 2
    ya = lax.rem(y + yb, 2)
    bits = (yb, ya, xb, xa)

    def peer(dims, flip_core=0):
        b = [1 - v if d in dims else v for d, v in enumerate(bits)]
        yy = 2 * b[0] + lax.rem(b[0] + b[1], 2)
        xx = 2 * b[2] + lax.rem(b[2] + b[3], 2)
        return {"seq": (yy * 4 + xx) * 2 + (1 - core if flip_core else core)}

    def group_peer(q, f):
        fu, fv, fc = FLIPS[f]
        dims = tuple(d for d, on in zip(ORDERS[q][2:], (fu, fv)) if on)
        return peer(dims, fc)

    mate = peer((), 1)
    steps = tuple(peer((d,)) for d in range(4))
    own0 = core * hrows
    oth0 = (1 - core) * hrows

    tok_step = rows // 4

    def batch(i):
        return oth0 + i if i < hrows else own0 + i - hrows

    def tok_copy(i):
        at = pl.ds(batch(i), tok_step)
        return pltpu.make_async_copy(tok_hbm.at[at], x_v.at[at], tok_sem.at[i // tok_step])

    phi_copy = pltpu.make_async_copy(phi_hbm, phi_v, phi_sem)
    wi_copies = [pltpu.make_async_copy(wi_hbm.at[e], wi_v.at[e], wi_sem) for e in range(experts)]
    wo_copies = [pltpu.make_async_copy(wo_hbm.at[e], wo_v.at[e], wo_sem) for e in range(experts)]
    tok_copy(0).start()
    phi_copy.start()
    tok_copy(tok_step).start()

    pairs = sorted({tuple(sorted(o[2:])) for o in ORDERS})
    greet = [mate]
    for fc in (0, 1):
        greet += [peer((d,), fc) for d in range(4)]
        greet += [peer(dims, fc) for dims in pairs]
    barrier = pltpu.get_barrier_semaphore()
    for d in greet:
        pl.semaphore_signal(barrier, inc=1, device_id=d, device_id_type=MESH)

    z_part[...] = jnp.zeros_like(z_part)
    gain = gain_ref[0]
    shift = gain * (1.0 + 2.0 ** -7)
    lane = lax.broadcasted_iota(jnp.int32, (nslots, tok_count), 1)
    pos = me * tok_count + lane

    def normalise(i):
        xf = x_v[batch(i)].astype(F32)
        xn_v[i] = (xf * lax.rsqrt(jnp.sum(xf * xf, axis=1, keepdims=True) + 1e-6)).astype(BF16)

    def weigh(i):
        b = batch(i)
        ex = jnp.exp(_nt(phit_v[i % 2], xn_v[i]) - shift)
        ct_v[b] = (ex * (1.0 / jnp.sum(ex, axis=0, keepdims=True))).astype(BF16)
        exm = jnp.where(pos < len_ref[b], ex, 0.0)
        w_v[i] = exm.astype(BF16)
        zs = jnp.where(lane == b, jnp.sum(exm, axis=1, keepdims=True), 0.0)
        z_part[...] += zs.reshape(z_part.shape)

    def collect(i):
        b = batch(i)
        for base in range(0, width, WIDE):
            pk = _nn(w_v[i], x_v[b, :, base:base + WIDE])
            for k, off, wd in chunks:
                if base <= off < base + WIDE:
                    piece = pk[:, off - base:off - base + wd]
                    part[k][b] = piece.reshape(2, 2, 2, 2, chip_rows, wd).astype(BF16)

    def half_copy(k, h):
        n = hrows // 2
        return pltpu.make_async_remote_copy(
            part[k].at[pl.ds(oth0 + h * n, n)], half_in[k].at[pl.ds(h * n, n)],
            hs_sem, hr_sem.at[k], device_id=mate, device_id_type=MESH)

    def region(order, fixed, flip=None):
        idx = [slice(None)] * 4
        for t in range(fixed):
            idx[order[t]] = bits[order[t]]
        if flip is not None:
            idx[flip] = 1 - bits[flip]
        return tuple(idx)

    rbuf = (r0, r1)
    zbuf = (z0, z1)

    def rs_copy(k, q, s):
        order = ORDERS[q]
        return pltpu.make_async_remote_copy(
            part[k].at[(pl.ds(own0 + q * gsz, gsz),) + region(order, s, order[s])],
            rbuf[s][k].at[pl.ds(q * gsz, gsz)],
            rs_sem.at[k if s == 0 else NK], rr_sem.at[2 * k + s], device_id=steps[order[s]], device_id_type=MESH)

    def z_copy(s):
        order = ORDERS[0]
        return pltpu.make_async_remote_copy(
            z_part.at[region(order, s, order[s])], zbuf[s],
            zs_sem.at[s], zr_sem.at[s], device_id=steps[order[s]], device_id_type=MESH)

    def zq_copy(f):
        fu, fv, _ = FLIPS[f]
        order = ORDERS[0]
        idx = list(bits)
        for d, on in zip(order[2:], (fu, fv)):
            if on:
                idx[d] = 1 - idx[d]
        return pltpu.make_async_remote_copy(
            z_part.at[tuple(idx)], zq.at[f], zs_sem.at[2], zr_sem.at[2],
            device_id=group_peer(0, f), device_id_type=MESH)

    zh_copy = pltpu.make_async_remote_copy(
        z_part, z_half, zhs_sem, zhr_sem, device_id=mate, device_id_type=MESH)

    tok_copy(0).wait()
    tok_copy(2 * tok_step).start()
    tok_copy(3 * tok_step).start()
    for i in range(tok_step):
        normalise(i)
    phi_copy.wait()
    pf = phi_v[...].astype(F32)
    pn = (pf * (gain * lax.rsqrt(jnp.sum(pf * pf, axis=0, keepdims=True) + 1e-6))).astype(BF16)
    new = lax.broadcasted_iota(jnp.int32, (nslots, nslots), 0)
    old = lax.broadcasted_iota(jnp.int32, (nslots, nslots), 1)
    nchip = new // chip_rows
    nxa, nxb, nya, nyb = nchip & 1, (nchip >> 1) & 1, (nchip >> 2) & 1, (nchip >> 3) & 1
    src = ((2 * nyb + (nya ^ nyb)) * 4 + 2 * nxb + (nxa ^ nxb)) * chip_rows + (new & (chip_rows - 1))
    for odd in range(2):
        perm = jnp.where((src ^ (odd * experts)) == old, 1.0, 0.0).astype(BF16)
        phit_v[odd] = _nt(perm, pn).astype(BF16)
    for cp in wi_copies + wo_copies:
        cp.start()

    def front(lo, hi, norm):
        norm = iter(norm)
        for i in range(lo, hi + 1):
            if i < hi:
                weigh(i)
            j = next(norm, None)
            if j is not None:
                normalise(j)
            if i > lo:
                collect(i - 1)

    tok_copy(tok_step).wait()
    front(0, tok_step, range(tok_step, 2 * tok_step))
    pl.semaphore_wait(barrier, len(greet))
    for k in range(NK):
        half_copy(k, 0).start()
    tok_copy(2 * tok_step).wait()
    front(tok_step, 2 * tok_step, range(2 * tok_step, 3 * tok_step))
    for k in range(NK):
        half_copy(k, 1).start()
    tok_copy(3 * tok_step).wait()
    front(2 * tok_step, rows, range(3 * tok_step, rows))
    zh_copy.start()

    def halve(k):
        _drain(half_in[k], hr_sem.at[k])
        for j in range(hrows):
            part[k][own0 + j] = part[k][own0 + j] + half_in[k][j]

        @pl.when(core == 1)
        def _():
            pl.delay(250)

        for q in range(GROUPS):
            rs_copy(k, q, 0).start()

    def flip_c(i, carry):
        for u in range(4):
            c_v[4 * i + u] = ct_v[4 * i + u].astype(F32).T.astype(BF16)
        return carry

    halve(0)
    lax.fori_loop(0, rows // 4, flip_c, 0)
    c_copy = pltpu.make_async_copy(c_v, c_hbm, c_sem)
    c_copy.start()
    halve(1)
    zh_copy.wait()
    z_part[...] += z_half[...]
    z_copy(0).start()
    _drain(r0[0], rs_sem.at[0])
    for k in range(2, NK):
        halve(k)

    def src_at(h):
        o = ORDERS[2 * h]
        return 4 * core + 2 * bits[o[2]] + bits[o[3]]

    def dst_at(h, f):
        fu, fv, fc = FLIPS[f]
        o = ORDERS[2 * h]
        mu, mv = bits[o[2]], bits[o[3]]
        return (1 - core if fc else core), (1 - mu if fu else mu), (1 - mv if fv else mv)

    def q_copy(k, h, f):
        dc, du, dv = dst_at(h, f)
        return pltpu.make_async_remote_copy(
            q_out[k].at[h, 4 * dc + 2 * du + dv], q_in[k].at[src_at(h), h],
            qs_sem, qr_sem.at[k], device_id=group_peer(2 * h, f), device_id_type=MESH)

    def low(wd):
        return lax.broadcasted_iota(jnp.int32, (chip_rows, wd), 0) < experts

    def at_rest(q, u, v):
        o = ORDERS[q]
        idx = list(bits)
        idx[o[2]] = u
        idx[o[3]] = v
        return tuple(idx)

    def at_recv(q, u, v):
        o = ORDERS[q]
        free = sorted(o[2:])
        val = {o[2]: u, o[3]: v}
        return tuple(val[d] for d in free)

    for k in range(NK):
        _drain(r0[k], rr_sem.at[2 * k])
        for q in range(GROUPS):
            for u in range(gsz):
                at = (own0 + q * gsz + u,) + region(ORDERS[q], 1)
                part[k][at] = part[k][at] + r0[k][q * gsz + u]
            rs_copy(k, q, 1).start()
        if k == 0:
            z_copy(0).wait_recv()
            at = region(ORDERS[0], 1)
            z_part[at] = z_part[at] + z0[...]
            z_copy(1).start()

    for k, _, wd in chunks:
        _drain(r1[k], rr_sem.at[2 * k + 1])
        for q in range(GROUPS):
            h, g = divmod(q, 2)
            for u in range(2):
                for v in range(2):
                    ev, od = [
                        part[k][(own0 + q * gsz + w,) + at_rest(q, u, v)].astype(F32)
                        + r1[k][(q * gsz + w,) + at_recv(q, u, v)].astype(F32)
                        for w in range(gsz)
                    ]
                    d = 2 * u + v
                    q_out[k][h, d, g] = jnp.where(low(wd), ev, od).astype(BF16)
                    q_out[k][h, 4 + d, g] = jnp.where(low(wd), od, ev).astype(BF16)
        for h in range(2):
            for f in range(7):
                q_copy(k, h, f).start()
            q_in[k][src_at(h), h] = q_out[k][h, src_at(h)]
        if k == 0:
            z_copy(1).wait_recv()
            at = region(ORDERS[0], 2)
            z_part[at] = z_part[at] + z1[...]
            for f in range(3):
                zq_copy(f).start()
    _drain(zq, zr_sem.at[2])
    z_own = z_part[bits] + (zq[0] + (zq[1] + zq[2]))
    zrow = lax.broadcasted_iota(jnp.int32, z_own.shape, 0)
    zcol = lax.broadcasted_iota(jnp.int32, z_own.shape, 1)
    zbase = (core ^ (zcol & 1)) * experts
    erow = lax.broadcasted_iota(jnp.int32, (rows, z_own.shape[1]), 0)
    eye = (erow ^ core) == lax.broadcasted_iota(jnp.int32, (rows, z_own.shape[1]), 1)
    z_inv = []
    for e in range(experts):
        zr = jnp.sum(jnp.where(zrow == zbase + e, z_own, 0.0), axis=0, keepdims=True)
        z_inv.append(1.0 / jnp.sum(jnp.where(eye, zr, 0.0), axis=1, keepdims=True))

    _drain(wi_v, wi_sem)
    _drain(wo_v, wo_sem)
    for k, off, wd in chunks:
        _drain(q_in[k].at[pl.ds(0, 7)], qr_sem.at[k])
        for cs in range(2):
            for q in range(GROUPS):
                p = cs * GROUPS + q
                s = [q_in[k][4 * cs + j, q // 2, q % 2].astype(F32) for j in range(4)]
                s = (s[0] + s[1]) + (s[2] + s[3])
                for t in range(wd // 128):
                    xs_f[t, p * chip_rows:(p + 1) * chip_rows, :] = s[:, t * 128:(t + 1) * 128]
        for e in range(experts):
            pick = pl.ds(e, rows, stride=experts)
            xe = [(xs_f[t, pick, :] * z_inv[e]).astype(BF16) for t in range(wd // 128)]
            xe = xe[0] if len(xe) == 1 else jnp.concatenate(xe, axis=1)
            h = _nn(xe, wi_v[e, off:off + wd, :])
            hid[e] = h if k == 0 else hid[e] + h
    for e in range(experts):
        hid_b[e] = jax.nn.gelu(hid[e], approximate=True).astype(BF16)

    def y_copy(k, h, f):
        dc = dst_at(h, f)[0]
        return pltpu.make_async_remote_copy(
            yx[k].at[dc * 2 + h], g_in[k].at[src_at(h), h],
            ys_sem, yr_sem.at[k], device_id=group_peer(2 * h, f), device_id_type=MESH)

    def g_copy(k, q, s):
        ref = gath[k].at[(pl.ds(own0 + q * gsz, gsz),) + region(ORDERS[q], s + 1)]
        return pltpu.make_async_remote_copy(
            ref, ref, gs_sem.at[s], gr_sem.at[2 * k + s], device_id=steps[ORDERS[q][s]], device_id_type=MESH)

    def gd_copy(k):
        at = pl.ds(own0, hrows)
        return pltpu.make_async_remote_copy(
            gath[k].at[at], g_hbm[k].at[at], gds_sem, gdr_sem, device_id=mate, device_id_type=MESH)

    def last_copies(q):
        dim = ORDERS[q][0]
        at = (pl.ds(own0 + q * gsz, gsz),) + region(ORDERS[q], 1)
        src, dst = gath[NK - 1].at[at], g_hbm[NK - 1].at[at]
        return [pltpu.make_async_copy(src, dst, fl_sem)] + [
            pltpu.make_async_remote_copy(
                src, dst, fs_sem.at[t], fr_sem.at[t], device_id=d, device_id_type=MESH)
            for t, d in enumerate((peer((dim,), 1), steps[dim], mate))
        ]

    def go_copy(k):
        at = pl.ds(own0, hrows)
        return pltpu.make_async_copy(gath[k].at[at], g_hbm[k].at[at], go_sem)

    for base in range(0, width, WIDE):
        for e in range(experts):
            ye = _nn(hid_b[e], wo_v[e, :, base:base + WIDE])
            for t in range(WIDE // 128):
                ys_f[t, pl.ds(e, rows, stride=experts), :] = ye[:, t * 128:(t + 1) * 128]
        for k, off, wd in chunks:
            if not base <= off < base + WIDE:
                continue
            for t in range(wd // 128):
                rows8 = ys_f[t + (off - base) // 128].reshape(4, 2, chip_rows, 128)
                yx[k][:, :, :, t * 128:(t + 1) * 128] = rows8.astype(BF16)
            for h in range(2):
                for f in range(7):
                    y_copy(k, h, f).start()
                g_in[k][src_at(h), h] = yx[k][core * 2 + h]

    for k, _, wd in chunks:
        _drain(g_in[k].at[pl.ds(0, 7)], yr_sem.at[k])
        for q in range(GROUPS):
            for u in range(2):
                for v in range(2):
                    s0 = g_in[k][2 * u + v, q // 2, q % 2].astype(F32)
                    s1 = g_in[k][4 + 2 * u + v, q // 2, q % 2].astype(F32)
                    at = at_rest(q, u, v)
                    b = own0 + q * gsz
                    gath[k][(b,) + at] = jnp.where(low(wd), s0, s1).astype(BF16)
                    gath[k][(b + 1,) + at] = jnp.where(low(wd), s1, s0).astype(BF16)

        @pl.when(core == 1)
        def _():
            pl.delay(200)

        for q in range(GROUPS):
            g_copy(k, q, 1).start()
    for k in range(NK):
        _drain(r1[k], gr_sem.at[2 * k + 1])

        @pl.when(core == 1)
        def _():
            pl.delay((300, 350, 550, 600)[k])

        for q in range(GROUPS):
            if k < NK - 1:
                g_copy(k, q, 0).start()
            else:
                for cp in last_copies(q):
                    cp.start()
    for k in range(NK - 1):
        _drain(r0[k], gr_sem.at[2 * k])
        gd_copy(k).start()
        go_copy(k).start()
    c_copy.wait()
    zh_bytes = x_v.at[pl.ds(0, hrows)]
    r0_bytes = x_v.at[pl.ds(0, hrows // 2)]
    r1_bytes = x_v.at[pl.ds(0, hrows // 4)]
    q_bytes = x_v.at[pl.ds(0, 7), pl.ds(0, 32)]
    z_copy(0).wait_send()
    z_copy(1).wait_send()
    _drain(zq, zs_sem.at[2])
    _drain(zh_bytes, hs_sem)
    for k in range(1, NK):
        _drain(r0[k], rs_sem.at[k])
    _drain(r1_bytes, rs_sem.at[NK])
    _drain(q_bytes, qs_sem)
    _drain(q_bytes, ys_sem)
    most = pl.ds(0, width - WIDTHS[-1])
    g_bytes = x_v.at[pl.ds(0, hrows), :, most]
    _drain(x_v.at[pl.ds(0, hrows // 2), :, most], gs_sem.at[0])
    _drain(r1_bytes, gs_sem.at[1])
    _drain(g_bytes, gds_sem)
    _drain(g_bytes, go_sem)
    _drain(g_bytes, gdr_sem)
    _drain(r0[NK - 1], fl_sem)
    for t in range(3):
        _drain(r0[NK - 1], fs_sem.at[t])
        _drain(r0[NK - 1], fr_sem.at[t])


def _mix_kernel(*refs):
    len_ref = refs[0]
    g_hbm = refs[1:1 + NK]
    c_hbm, y_hbm, g_v, c_v, y_v, g_sem, c_sem, y_sem = refs[1 + NK:]
    rows, tok_count, width = y_v.shape
    step = rows // 4

    def c_copy(b):
        at = pl.ds(b, step)
        return pltpu.make_async_copy(c_hbm.at[at], c_v.at[at], c_sem.at[b // step])

    def g_copies(b):
        at = pl.ds(b, step)
        return [
            pltpu.make_async_copy(
                g_hbm[k].at[at], g_v.at[at, :, pl.ds(OFFS[k], WIDTHS[k])], g_sem.at[b // step])
            for k in range(NK)
        ]

    def y_copy(b):
        at = pl.ds(b, step)
        return pltpu.make_async_copy(y_v.at[at], y_hbm.at[at], y_sem)

    for b in range(0, rows, step):
        if b:
            pl.delay(250)
        c_copy(b).start()
        for cp in g_copies(b):
            cp.start()
    row_pos = lax.axis_index("seq") * tok_count + lax.broadcasted_iota(jnp.int32, (tok_count, WIDE), 0)
    for b0 in range(0, rows, step):
        c_copy(b0).wait()
        _drain(g_v.at[pl.ds(b0, step)], g_sem.at[b0 // step])
        for b in range(b0, b0 + step):
            for off in range(0, width, WIDE):
                yk = jnp.where(row_pos < len_ref[b], _nn(c_v[b], g_v[b, :, off:off + WIDE]), 0.0)
                y_v[b, :, off:off + WIDE] = yk.astype(BF16)
        y_copy(b0).start()
    _drain(y_v, y_sem)


def solution(mesh):
    def shard_body(tok, lens, phi, gain, w_in, w_out):
        rows, tok_count, width = tok.shape
        experts, _, ff = w_in.shape
        nslots = phi.shape[1]
        hrows = rows // 2
        cr = 2 * experts
        cube = (2, 2, 2, 2)
        lanes = WIDE // 128
        vm = pltpu.VMEM
        dma = pltpu.SemaphoreType.DMA
        anyspace = pl.BlockSpec(memory_space=pl.ANY)
        smem = pl.BlockSpec(memory_space=pltpu.SMEM)

        def per_chunk(*lead):
            return [vm(lead + (cr, wd), BF16) for wd in WIDTHS]

        scratch = [
            vm((rows, tok_count, width), BF16),
            vm((rows, tok_count, width), BF16),
            vm((rows, nslots, tok_count), BF16),
            vm((width, nslots), BF16),
            vm((2, nslots, width), BF16),
            vm(w_in.shape, BF16),
            vm(w_out.shape, BF16),
            vm((rows, nslots, tok_count), BF16),
            vm((rows, tok_count, nslots), BF16),
            *per_chunk(rows, *cube),
            *per_chunk(hrows, *cube),
            *per_chunk(hrows, 2, 2, 2),
            *per_chunk(hrows, 2, 2),
            *per_chunk(2, 8, 2),
            *per_chunk(8, 2, 2),
            *per_chunk(4, 2),
            *per_chunk(8, 2, 2),
            *per_chunk(rows, *cube),
            vm(cube + (cr, tok_count), F32),
            vm(cube + (cr, tok_count), F32),
            vm((2, 2, 2, cr, tok_count), F32),
            vm((2, 2, cr, tok_count), F32),
            vm((3, cr, tok_count), F32),
            vm((lanes, rows * experts, 128), F32),
            vm((experts, rows, ff), F32),
            vm((experts, rows, ff), BF16),
            vm((lanes, rows * experts, 128), F32),
            dma, dma((4,)), dma, dma, dma, dma, dma((NK,)), dma, dma, dma((3,)), dma((3,)),
            dma((NK + 1,)), dma((2 * NK,)), dma, dma((NK,)), dma, dma((NK,)), dma((2,)), dma((2 * NK,)), dma, dma, dma,
            dma, dma((3,)), dma((3,)),
        ]
        gshapes = [jax.ShapeDtypeStruct((rows,) + cube + (cr, wd), BF16) for wd in WIDTHS]
        *gath, comb = pl.pallas_call(
            _exchange_kernel,
            out_shape=(*gshapes, jax.ShapeDtypeStruct((rows, tok_count, nslots), BF16)),
            in_specs=[smem, smem, anyspace, anyspace, anyspace, anyspace],
            out_specs=(anyspace,) * (NK + 1),
            scratch_shapes=scratch,
            compiler_params=pltpu.CompilerParams(
                collective_id=0, has_side_effects=True, vmem_limit_bytes=67043328),
        )(lens, gain, tok, phi, w_in, w_out)
        return pl.pallas_call(
            _mix_kernel,
            out_shape=jax.ShapeDtypeStruct(tok.shape, BF16),
            in_specs=[smem] + [anyspace] * (NK + 1),
            out_specs=anyspace,
            scratch_shapes=[
                vm((rows, nslots, width), BF16),
                vm((rows, tok_count, nslots), BF16),
                vm(tok.shape, BF16),
                dma((4,)), dma((4,)), dma,
            ],
        )(lens, *[g.reshape(rows, nslots, wd) for g, wd in zip(gath, WIDTHS)], comb)

    return jax.shard_map(
        shard_body,
        mesh=mesh,
        in_specs=(P("data", "seq", None), P("data"), P(None, None), P(None), P("seq", None, None), P("seq", None, None)),
        out_specs=P("data", "seq", None),
        check_vma=False,
    )
```

```python
import functools

import jax
import jax.numpy as jnp
from jax import lax
from jax.experimental import pallas as pl
from jax.experimental.pallas import tpu as pltpu
from jax.sharding import PartitionSpec as P

WIDE = 256
WIDTHS = (256, 256, 128, 128)
OFFS = tuple(sum(WIDTHS[:k]) for k in range(len(WIDTHS)))
NK = len(WIDTHS)
GROUPS = 4
F32 = jnp.float32
BF16 = jnp.bfloat16
MESH = pl.DeviceIdType.MESH
ORDERS = ((3, 1, 2, 0), (1, 3, 2, 0), (2, 0, 3, 1), (0, 2, 3, 1))
FLIPS = tuple((f & 1, (f >> 1) & 1, (f >> 2) & 1) for f in range(1, 8))


def _nt(a, b):
    return lax.dot_general(a, b, (((1,), (1,)), ((), ())), preferred_element_type=F32)


def _nn(a, b):
    return jnp.dot(a, b, preferred_element_type=F32)


def _drain(ref, sem):
    pltpu.make_async_copy(ref, ref, sem).wait()


def _exchange_kernel(*refs):
    it = iter(refs)

    def take(n=NK):
        return [next(it) for _ in range(n)]

    len_ref, gain_ref, tok_hbm, phi_hbm, wi_hbm, wo_hbm = take(6)
    g_hbm = take()
    c_hbm = next(it)
    x_v, xn_v, w_v, phi_v, phit_v, wi_v, wo_v, ct_v, c_v = take(9)
    part, half_in, r0, r1, q_out, q_in, yx, g_in, gath = [take() for _ in range(9)]
    z_part, z_half, z0, z1, zq, xs_f, hid, hid_b, ys_f = take(9)
    (phi_sem, tok_sem, wi_sem, wo_sem, c_sem, hs_sem, hr_sem, zhs_sem, zhr_sem, zs_sem, zr_sem,
     rs_sem, rr_sem, qs_sem, qr_sem, ys_sem, yr_sem, gs_sem, gr_sem, gds_sem, gdr_sem, go_sem, fl_sem, fs_sem, fr_sem) = take(25)
    rows, tok_count, width = x_v.shape
    experts = wi_v.shape[0]
    hrows = rows // 2
    gsz = hrows // GROUPS
    nslots = phit_v.shape[1]
    chip_rows = 2 * experts
    chunks = tuple(zip(range(NK), OFFS, WIDTHS))
    me = lax.axis_index("seq")
    core = lax.rem(me, 2)
    chip = me // 2
    x = lax.rem(chip, 4)
    y = chip // 4
    xb = x // 2
    xa = lax.rem(x + xb, 2)
    yb = y // 2
    ya = lax.rem(y + yb, 2)
    bits = (yb, ya, xb, xa)

    def peer(dims, flip_core=0):
        b = [1 - v if d in dims else v for d, v in enumerate(bits)]
        yy = 2 * b[0] + lax.rem(b[0] + b[1], 2)
        xx = 2 * b[2] + lax.rem(b[2] + b[3], 2)
        return {"seq": (yy * 4 + xx) * 2 + (1 - core if flip_core else core)}

    def group_peer(q, f):
        fu, fv, fc = FLIPS[f]
        dims = tuple(d for d, on in zip(ORDERS[q][2:], (fu, fv)) if on)
        return peer(dims, fc)

    mate = peer((), 1)
    steps = tuple(peer((d,)) for d in range(4))
    own0 = core * hrows
    oth0 = (1 - core) * hrows

    tok_step = rows // 4

    def batch(i):
        return oth0 + i if i < hrows else own0 + i - hrows

    def tok_copy(i):
        at = pl.ds(batch(i), tok_step)
        return pltpu.make_async_copy(tok_hbm.at[at], x_v.at[at], tok_sem.at[i // tok_step])

    phi_copy = pltpu.make_async_copy(phi_hbm, phi_v, phi_sem)
    wi_copies = [pltpu.make_async_copy(wi_hbm.at[e], wi_v.at[e], wi_sem) for e in range(experts)]
    wo_copies = [pltpu.make_async_copy(wo_hbm.at[e], wo_v.at[e], wo_sem) for e in range(experts)]
    tok_copy(0).start()
    phi_copy.start()
    tok_copy(tok_step).start()

    pairs = sorted({tuple(sorted(o[2:])) for o in ORDERS})
    greet = [mate]
    for fc in (0, 1):
        greet += [peer((d,), fc) for d in range(4)]
        greet += [peer(dims, fc) for dims in pairs]
    barrier = pltpu.get_barrier_semaphore()
    for d in greet:
        pl.semaphore_signal(barrier, inc=1, device_id=d, device_id_type=MESH)

    z_part[...] = jnp.zeros_like(z_part)
    gain = gain_ref[0]
    shift = gain * (1.0 + 2.0 ** -7)
    lane = lax.broadcasted_iota(jnp.int32, (nslots, tok_count), 1)
    pos = me * tok_count + lane

    def normalise(i):
        xf = x_v[batch(i)].astype(F32)
        xn_v[i] = (xf * lax.rsqrt(jnp.sum(xf * xf, axis=1, keepdims=True) + 1e-6)).astype(BF16)

    def weigh(i):
        b = batch(i)
        ex = jnp.exp(_nt(phit_v[i % 2], xn_v[i]) - shift)
        ct_v[b] = (ex * (1.0 / jnp.sum(ex, axis=0, keepdims=True))).astype(BF16)
        exm = jnp.where(pos < len_ref[b], ex, 0.0)
        w_v[i] = exm.astype(BF16)
        zs = jnp.where(lane == b, jnp.sum(exm, axis=1, keepdims=True), 0.0)
        z_part[...] += zs.reshape(z_part.shape)

    def collect(i):
        b = batch(i)
        for base in range(0, width, WIDE):
            pk = _nn(w_v[i], x_v[b, :, base:base + WIDE])
            for k, off, wd in chunks:
                if base <= off < base + WIDE:
                    piece = pk[:, off - base:off - base + wd]
                    part[k][b] = piece.reshape(2, 2, 2, 2, chip_rows, wd).astype(BF16)

    def half_copy(k, h):
        n = hrows // 2
        return pltpu.make_async_remote_copy(
            part[k].at[pl.ds(oth0 + h * n, n)], half_in[k].at[pl.ds(h * n, n)],
            hs_sem, hr_sem.at[k], device_id=mate, device_id_type=MESH)

    def region(order, fixed, flip=None):
        idx = [slice(None)] * 4
        for t in range(fixed):
            idx[order[t]] = bits[order[t]]
        if flip is not None:
            idx[flip] = 1 - bits[flip]
        return tuple(idx)

    rbuf = (r0, r1)
    zbuf = (z0, z1)

    def rs_copy(k, q, s):
        order = ORDERS[q]
        return pltpu.make_async_remote_copy(
            part[k].at[(pl.ds(own0 + q * gsz, gsz),) + region(order, s, order[s])],
            rbuf[s][k].at[pl.ds(q * gsz, gsz)],
            rs_sem.at[k if s == 0 else NK], rr_sem.at[2 * k + s], device_id=steps[order[s]], device_id_type=MESH)

    def z_copy(s):
        order = ORDERS[0]
        return pltpu.make_async_remote_copy(
            z_part.at[region(order, s, order[s])], zbuf[s],
            zs_sem.at[s], zr_sem.at[s], device_id=steps[order[s]], device_id_type=MESH)

    def zq_copy(f):
        fu, fv, _ = FLIPS[f]
        order = ORDERS[0]
        idx = list(bits)
        for d, on in zip(order[2:], (fu, fv)):
            if on:
                idx[d] = 1 - idx[d]
        return pltpu.make_async_remote_copy(
            z_part.at[tuple(idx)], zq.at[f], zs_sem.at[2], zr_sem.at[2],
            device_id=group_peer(0, f), device_id_type=MESH)

    zh_copy = pltpu.make_async_remote_copy(
        z_part, z_half, zhs_sem, zhr_sem, device_id=mate, device_id_type=MESH)

    tok_copy(0).wait()
    tok_copy(2 * tok_step).start()
    tok_copy(3 * tok_step).start()
    for i in range(tok_step):
        normalise(i)
    phi_copy.wait()
    pf = phi_v[...].astype(F32)
    pn = (pf * (gain * lax.rsqrt(jnp.sum(pf * pf, axis=0, keepdims=True) + 1e-6))).astype(BF16)
    new = lax.broadcasted_iota(jnp.int32, (nslots, nslots), 0)
    old = lax.broadcasted_iota(jnp.int32, (nslots, nslots), 1)
    nchip = new // chip_rows
    nxa, nxb, nya, nyb = nchip & 1, (nchip >> 1) & 1, (nchip >> 2) & 1, (nchip >> 3) & 1
    src = ((2 * nyb + (nya ^ nyb)) * 4 + 2 * nxb + (nxa ^ nxb)) * chip_rows + (new & (chip_rows - 1))
    for odd in range(2):
        perm = jnp.where((src ^ (odd * experts)) == old, 1.0, 0.0).astype(BF16)
        phit_v[odd] = _nt(perm, pn).astype(BF16)
    for cp in wi_copies + wo_copies:
        cp.start()

    def front(lo, hi, norm):
        norm = iter(norm)
        for i in range(lo, hi + 1):
            if i < hi:
                weigh(i)
            j = next(norm, None)
            if j is not None:
                normalise(j)
            if i > lo:
                collect(i - 1)

    tok_copy(tok_step).wait()
    front(0, tok_step, range(tok_step, 2 * tok_step))
    pl.semaphore_wait(barrier, len(greet))
    for k in range(NK):
        half_copy(k, 0).start()
    tok_copy(2 * tok_step).wait()
    front(tok_step, 2 * tok_step, range(2 * tok_step, 3 * tok_step))
    for k in range(NK):
        half_copy(k, 1).start()
    tok_copy(3 * tok_step).wait()
    front(2 * tok_step, rows, range(3 * tok_step, rows))
    zh_copy.start()

    def halve(k):
        _drain(half_in[k], hr_sem.at[k])
        for j in range(hrows):
            part[k][own0 + j] = part[k][own0 + j] + half_in[k][j]

        @pl.when(core == 1)
        def _():
            pl.delay(250)

        for q in range(GROUPS):
            rs_copy(k, q, 0).start()

    def flip_c(i, carry):
        for u in range(4):
            c_v[4 * i + u] = ct_v[4 * i + u].astype(F32).T.astype(BF16)
        return carry

    halve(0)
    lax.fori_loop(0, rows // 4, flip_c, 0)
    c_copy = pltpu.make_async_copy(c_v, c_hbm, c_sem)
    c_copy.start()
    halve(1)
    zh_copy.wait()
    z_part[...] += z_half[...]
    z_copy(0).start()
    _drain(r0[0], rs_sem.at[0])
    for k in range(2, NK):
        halve(k)

    def src_at(h):
        o = ORDERS[2 * h]
        return 4 * core + 2 * bits[o[2]] + bits[o[3]]

    def dst_at(h, f):
        fu, fv, fc = FLIPS[f]
        o = ORDERS[2 * h]
        mu, mv = bits[o[2]], bits[o[3]]
        return (1 - core if fc else core), (1 - mu if fu else mu), (1 - mv if fv else mv)

    def q_copy(k, h, f):
        dc, du, dv = dst_at(h, f)
        return pltpu.make_async_remote_copy(
            q_out[k].at[h, 4 * dc + 2 * du + dv], q_in[k].at[src_at(h), h],
            qs_sem, qr_sem.at[k], device_id=group_peer(2 * h, f), device_id_type=MESH)

    def low(wd):
        return lax.broadcasted_iota(jnp.int32, (chip_rows, wd), 0) < experts

    def at_rest(q, u, v):
        o = ORDERS[q]
        idx = list(bits)
        idx[o[2]] = u
        idx[o[3]] = v
        return tuple(idx)

    def at_recv(q, u, v):
        o = ORDERS[q]
        free = sorted(o[2:])
        val = {o[2]: u, o[3]: v}
        return tuple(val[d] for d in free)

    for k in range(NK):
        _drain(r0[k], rr_sem.at[2 * k])
        for q in range(GROUPS):
            for u in range(gsz):
                at = (own0 + q * gsz + u,) + region(ORDERS[q], 1)
                part[k][at] = part[k][at] + r0[k][q * gsz + u]
            rs_copy(k, q, 1).start()
        if k == 0:
            z_copy(0).wait_recv()
            at = region(ORDERS[0], 1)
            z_part[at] = z_part[at] + z0[...]
            z_copy(1).start()

    for k, _, wd in chunks:
        _drain(r1[k], rr_sem.at[2 * k + 1])
        for q in range(GROUPS):
            h, g = divmod(q, 2)
            for u in range(2):
                for v in range(2):
                    ev, od = [
                        part[k][(own0 + q * gsz + w,) + at_rest(q, u, v)].astype(F32)
                        + r1[k][(q * gsz + w,) + at_recv(q, u, v)].astype(F32)
                        for w in range(gsz)
                    ]
                    d = 2 * u + v
                    q_out[k][h, d, g] = jnp.where(low(wd), ev, od).astype(BF16)
                    q_out[k][h, 4 + d, g] = jnp.where(low(wd), od, ev).astype(BF16)
        for h in range(2):
            for f in range(7):
                q_copy(k, h, f).start()
            q_in[k][src_at(h), h] = q_out[k][h, src_at(h)]
        if k == 0:
            z_copy(1).wait_recv()
            at = region(ORDERS[0], 2)
            z_part[at] = z_part[at] + z1[...]
            for f in range(3):
                zq_copy(f).start()
    _drain(zq, zr_sem.at[2])
    z_own = z_part[bits] + (zq[0] + (zq[1] + zq[2]))
    zrow = lax.broadcasted_iota(jnp.int32, z_own.shape, 0)
    zcol = lax.broadcasted_iota(jnp.int32, z_own.shape, 1)
    zbase = (core ^ (zcol & 1)) * experts
    erow = lax.broadcasted_iota(jnp.int32, (rows, z_own.shape[1]), 0)
    eye = (erow ^ core) == lax.broadcasted_iota(jnp.int32, (rows, z_own.shape[1]), 1)
    z_inv = []
    for e in range(experts):
        zr = jnp.sum(jnp.where(zrow == zbase + e, z_own, 0.0), axis=0, keepdims=True)
        z_inv.append(1.0 / jnp.sum(jnp.where(eye, zr, 0.0), axis=1, keepdims=True))

    _drain(wi_v, wi_sem)
    _drain(wo_v, wo_sem)
    for k, off, wd in chunks:
        _drain(q_in[k].at[pl.ds(0, 7)], qr_sem.at[k])
        for cs in range(2):
            for q in range(GROUPS):
                p = cs * GROUPS + q
                s = [q_in[k][4 * cs + j, q // 2, q % 2].astype(F32) for j in range(4)]
                s = (s[0] + s[1]) + (s[2] + s[3])
                for t in range(wd // 128):
                    xs_f[t, p * chip_rows:(p + 1) * chip_rows, :] = s[:, t * 128:(t + 1) * 128]
        for e in range(experts):
            pick = pl.ds(e, rows, stride=experts)
            xe = [(xs_f[t, pick, :] * z_inv[e]).astype(BF16) for t in range(wd // 128)]
            xe = xe[0] if len(xe) == 1 else jnp.concatenate(xe, axis=1)
            h = _nn(xe, wi_v[e, off:off + wd, :])
            hid[e] = h if k == 0 else hid[e] + h
    for e in range(experts):
        hid_b[e] = jax.nn.gelu(hid[e], approximate=True).astype(BF16)

    def y_copy(k, h, f):
        dc = dst_at(h, f)[0]
        return pltpu.make_async_remote_copy(
            yx[k].at[dc * 2 + h], g_in[k].at[src_at(h), h],
            ys_sem, yr_sem.at[k], device_id=group_peer(2 * h, f), device_id_type=MESH)

    def g_copy(k, q, s):
        ref = gath[k].at[(pl.ds(own0 + q * gsz, gsz),) + region(ORDERS[q], s + 1)]
        return pltpu.make_async_remote_copy(
            ref, ref, gs_sem.at[s], gr_sem.at[2 * k + s], device_id=steps[ORDERS[q][s]], device_id_type=MESH)

    def gd_copy(k):
        at = pl.ds(own0, hrows)
        return pltpu.make_async_remote_copy(
            gath[k].at[at], g_hbm[k].at[at], gds_sem, gdr_sem, device_id=mate, device_id_type=MESH)

    def last_copies(q):
        dim = ORDERS[q][0]
        at = (pl.ds(own0 + q * gsz, gsz),) + region(ORDERS[q], 1)
        src, dst = gath[NK - 1].at[at], g_hbm[NK - 1].at[at]
        return [pltpu.make_async_copy(src, dst, fl_sem)] + [
            pltpu.make_async_remote_copy(
                src, dst, fs_sem.at[t], fr_sem.at[t], device_id=d, device_id_type=MESH)
            for t, d in enumerate((peer((dim,), 1), steps[dim], mate))
        ]

    def go_copy(k):
        at = pl.ds(own0, hrows)
        return pltpu.make_async_copy(gath[k].at[at], g_hbm[k].at[at], go_sem)

    for base in range(0, width, WIDE):
        for e in range(experts):
            ye = _nn(hid_b[e], wo_v[e, :, base:base + WIDE])
            for t in range(WIDE // 128):
                ys_f[t, pl.ds(e, rows, stride=experts), :] = ye[:, t * 128:(t + 1) * 128]
        for k, off, wd in chunks:
            if not base <= off < base + WIDE:
                continue
            for t in range(wd // 128):
                rows8 = ys_f[t + (off - base) // 128].reshape(4, 2, chip_rows, 128)
                yx[k][:, :, :, t * 128:(t + 1) * 128] = rows8.astype(BF16)
            for h in range(2):
                for f in range(7):
                    y_copy(k, h, f).start()
                g_in[k][src_at(h), h] = yx[k][core * 2 + h]

    for k, _, wd in chunks:
        _drain(g_in[k].at[pl.ds(0, 7)], yr_sem.at[k])
        for q in range(GROUPS):
            for u in range(2):
                for v in range(2):
                    s0 = g_in[k][2 * u + v, q // 2, q % 2].astype(F32)
                    s1 = g_in[k][4 + 2 * u + v, q // 2, q % 2].astype(F32)
                    at = at_rest(q, u, v)
                    b = own0 + q * gsz
                    gath[k][(b,) + at] = jnp.where(low(wd), s0, s1).astype(BF16)
                    gath[k][(b + 1,) + at] = jnp.where(low(wd), s1, s0).astype(BF16)

        @pl.when(core == 1)
        def _():
            pl.delay(350)

        for q in range(GROUPS):
            g_copy(k, q, 1).start()
    for k in range(NK):
        _drain(r1[k], gr_sem.at[2 * k + 1])

        @pl.when(core == 1)
        def _():
            pl.delay((300, 350, 550, 600)[k])

        for q in range(GROUPS):
            if k < NK - 1:
                g_copy(k, q, 0).start()
            else:
                for cp in last_copies(q):
                    cp.start()
    for k in range(NK - 1):
        _drain(r0[k], gr_sem.at[2 * k])
        gd_copy(k).start()
        go_copy(k).start()
    c_copy.wait()
    zh_bytes = x_v.at[pl.ds(0, hrows)]
    r0_bytes = x_v.at[pl.ds(0, hrows // 2)]
    r1_bytes = x_v.at[pl.ds(0, hrows // 4)]
    q_bytes = x_v.at[pl.ds(0, 7), pl.ds(0, 32)]
    z_copy(0).wait_send()
    z_copy(1).wait_send()
    _drain(zq, zs_sem.at[2])
    _drain(zh_bytes, hs_sem)
    for k in range(1, NK):
        _drain(r0[k], rs_sem.at[k])
    _drain(r1_bytes, rs_sem.at[NK])
    _drain(q_bytes, qs_sem)
    _drain(q_bytes, ys_sem)
    most = pl.ds(0, width - WIDTHS[-1])
    g_bytes = x_v.at[pl.ds(0, hrows), :, most]
    _drain(x_v.at[pl.ds(0, hrows // 2), :, most], gs_sem.at[0])
    _drain(r1_bytes, gs_sem.at[1])
    _drain(g_bytes, gds_sem)
    _drain(g_bytes, go_sem)
    _drain(g_bytes, gdr_sem)
    _drain(r0[NK - 1], fl_sem)
    for t in range(3):
        _drain(r0[NK - 1], fs_sem.at[t])
        _drain(r0[NK - 1], fr_sem.at[t])


def _mix_kernel(*refs):
    len_ref = refs[0]
    g_hbm = refs[1:1 + NK]
    c_hbm, y_hbm, g_v, c_v, y_v, g_sem, c_sem, y_sem = refs[1 + NK:]
    rows, tok_count, width = y_v.shape
    step = rows // 4

    def c_copy(b):
        at = pl.ds(b, step)
        return pltpu.make_async_copy(c_hbm.at[at], c_v.at[at], c_sem.at[b // step])

    def g_copies(b):
        at = pl.ds(b, step)
        return [
            pltpu.make_async_copy(
                g_hbm[k].at[at], g_v.at[at, :, pl.ds(OFFS[k], WIDTHS[k])], g_sem.at[b // step])
            for k in range(NK)
        ]

    def y_copy(b):
        at = pl.ds(b, step)
        return pltpu.make_async_copy(y_v.at[at], y_hbm.at[at], y_sem)

    for b in range(0, rows, step):
        if b:
            pl.delay(250)
        c_copy(b).start()
        for cp in g_copies(b):
            cp.start()
    row_pos = lax.axis_index("seq") * tok_count + lax.broadcasted_iota(jnp.int32, (tok_count, WIDE), 0)
    for b0 in range(0, rows, step):
        c_copy(b0).wait()
        _drain(g_v.at[pl.ds(b0, step)], g_sem.at[b0 // step])
        for b in range(b0, b0 + step):
            for off in range(0, width, WIDE):
                yk = jnp.where(row_pos < len_ref[b], _nn(c_v[b], g_v[b, :, off:off + WIDE]), 0.0)
                y_v[b, :, off:off + WIDE] = yk.astype(BF16)
        y_copy(b0).start()
    _drain(y_v, y_sem)


def solution(mesh):
    def shard_body(tok, lens, phi, gain, w_in, w_out):
        rows, tok_count, width = tok.shape
        experts, _, ff = w_in.shape
        nslots = phi.shape[1]
        hrows = rows // 2
        cr = 2 * experts
        cube = (2, 2, 2, 2)
        lanes = WIDE // 128
        vm = pltpu.VMEM
        dma = pltpu.SemaphoreType.DMA
        anyspace = pl.BlockSpec(memory_space=pl.ANY)
        smem = pl.BlockSpec(memory_space=pltpu.SMEM)

        def per_chunk(*lead):
            return [vm(lead + (cr, wd), BF16) for wd in WIDTHS]

        scratch = [
            vm((rows, tok_count, width), BF16),
            vm((rows, tok_count, width), BF16),
            vm((rows, nslots, tok_count), BF16),
            vm((width, nslots), BF16),
            vm((2, nslots, width), BF16),
            vm(w_in.shape, BF16),
            vm(w_out.shape, BF16),
            vm((rows, nslots, tok_count), BF16),
            vm((rows, tok_count, nslots), BF16),
            *per_chunk(rows, *cube),
            *per_chunk(hrows, *cube),
            *per_chunk(hrows, 2, 2, 2),
            *per_chunk(hrows, 2, 2),
            *per_chunk(2, 8, 2),
            *per_chunk(8, 2, 2),
            *per_chunk(4, 2),
            *per_chunk(8, 2, 2),
            *per_chunk(rows, *cube),
            vm(cube + (cr, tok_count), F32),
            vm(cube + (cr, tok_count), F32),
            vm((2, 2, 2, cr, tok_count), F32),
            vm((2, 2, cr, tok_count), F32),
            vm((3, cr, tok_count), F32),
            vm((lanes, rows * experts, 128), F32),
            vm((experts, rows, ff), F32),
            vm((experts, rows, ff), BF16),
            vm((lanes, rows * experts, 128), F32),
            dma, dma((4,)), dma, dma, dma, dma, dma((NK,)), dma, dma, dma((3,)), dma((3,)),
            dma((NK + 1,)), dma((2 * NK,)), dma, dma((NK,)), dma, dma((NK,)), dma((2,)), dma((2 * NK,)), dma, dma, dma,
            dma, dma((3,)), dma((3,)),
        ]
        gshapes = [jax.ShapeDtypeStruct((rows,) + cube + (cr, wd), BF16) for wd in WIDTHS]
        *gath, comb = pl.pallas_call(
            _exchange_kernel,
            out_shape=(*gshapes, jax.ShapeDtypeStruct((rows, tok_count, nslots), BF16)),
            in_specs=[smem, smem, anyspace, anyspace, anyspace, anyspace],
            out_specs=(anyspace,) * (NK + 1),
            scratch_shapes=scratch,
            compiler_params=pltpu.CompilerParams(
                collective_id=0, has_side_effects=True, vmem_limit_bytes=67043328),
        )(lens, gain, tok, phi, w_in, w_out)
        return pl.pallas_call(
            _mix_kernel,
            out_shape=jax.ShapeDtypeStruct(tok.shape, BF16),
            in_specs=[smem] + [anyspace] * (NK + 1),
            out_specs=anyspace,
            scratch_shapes=[
                vm((rows, nslots, width), BF16),
                vm((rows, tok_count, nslots), BF16),
                vm(tok.shape, BF16),
                dma((4,)), dma((4,)), dma,
            ],
        )(lens, *[g.reshape(rows, nslots, wd) for g, wd in zip(gath, WIDTHS)], comb)

    return jax.shard_map(
        shard_body,
        mesh=mesh,
        in_specs=(P("data", "seq", None), P("data"), P(None, None), P(None), P("seq", None, None), P("seq", None, None)),
        out_specs=P("data", "seq", None),
        check_vma=False,
    )
```
